8 devices in a mesh: dp: 1 (over z), tp: 2 (over y), ep: 4 (over x, core).
Axes of the slice: x: 2, y: 2, z: 1, core: 2. Of those that a mesh axis runs over, the one named last changes fastest.
Arguments:
- hidden: bfloat16 [512, 768], P(('dp', 'ep'))
- write_pos: int32 [512], P(('dp', 'ep'))
- enc_mask: int32 [512, 32], P(('dp', 'ep'))
- expert_idx: int32 [512], P(('dp', 'ep'))
- self_keys: bfloat16 [2, 512, 12, 32, 64], P(None, ('dp', 'ep'), 'tp')
- self_values: bfloat16 [2, 512, 12, 32, 64], P(None, ('dp', 'ep'), 'tp')
- cross_keys: bfloat16 [2, 512, 12, 32, 64], P(None, ('dp', 'ep'), 'tp')
- cross_values: bfloat16 [2, 512, 12, 32, 64], P(None, ('dp', 'ep'), 'tp')
- rel_bias: float32 [12, 32], P('tp')
- norm_scale: float32 [2, 3, 768], replicated
- w_query: bfloat16 [2, 768, 768], P(None, None, 'tp')
- w_key: bfloat16 [2, 768, 768], P(None, None, 'tp')
- w_value: bfloat16 [2, 768, 768], P(None, None, 'tp')
- w_out: bfloat16 [2, 768, 768], P(None, 'tp')
- w_cross_query: bfloat16 [2, 768, 768], P(None, None, 'tp')
- w_cross_out: bfloat16 [2, 768, 768], P(None, 'tp')
- dense_gate: bfloat16 [768, 3072], P(None, 'tp')
- dense_up: bfloat16 [768, 3072], P(None, 'tp')
- dense_down: bfloat16 [3072, 768], P('tp')
- router: float32 [768, 64], replicated
- exp_gate: bfloat16 [64, 768, 3072], P('ep', None, 'tp')
- exp_up: bfloat16 [64, 768, 3072], P('ep', None, 'tp')
- exp_down: bfloat16 [64, 3072, 768], P('ep', 'tp')
Outputs:
- output 1: bfloat16 [512, 768], P(('dp', 'ep'))
- output 2: bfloat16 [2, 512, 12, 32, 64], P(None, ('dp', 'ep'), 'tp')
- output 3: bfloat16 [2, 512, 12, 32, 64], P(None, ('dp', 'ep'), 'tp')
All inputs are finite; a program needn't handle non-finite values.
Results may differ from the reference program's by a relative error of at most 0.02.
Values are sent between devices in bfloat16 or wider.
A program may use at most 1 GiB of HBM per device.

```python
import jax
import jax.numpy as jnp
from jax import lax

D = 768
HEADS = 12
HEAD = 64
FF = 3072
EXPERTS = 64
TOK_DEV = 128
GROUPS = 4
CACHE = 32
SRC = 32
TOKENS = TOK_DEV * GROUPS
WIDTH = HEADS * HEAD
CAPACITY = (2 * TOK_DEV + EXPERTS - 1) // EXPERTS
EPS = 1e-6
NEG_BIG = -1e9


def setup_inputs(seed: int = 0, part: int = 0) -> dict:
    root = jax.random.key(seed)
    shared_root, part_root = jax.random.split(root)
    local = jax.random.fold_in(part_root, part)
    local_keys = jax.random.split(local, 10)
    shared_keys = jax.random.split(shared_root, 16)

    def normal(key, shape, scale):
        return jax.random.normal(key, shape, jnp.float32) * scale

    row_ids = jnp.arange(TOKENS)
    hidden = normal(local_keys[0], (TOKENS, D), 1.0).astype(jnp.bfloat16)
    pos_draw = jax.random.randint(local_keys[1], (TOKENS,), 0, CACHE)
    write_pos = jnp.where(row_ids == 0, CACHE - 1, pos_draw).astype(jnp.int32)
    src_len = jax.random.randint(local_keys[2], (TOKENS,), max(SRC // 4, 1), SRC + 1)
    src_len = jnp.where(row_ids == 1, SRC, src_len)
    enc_mask = (jnp.arange(SRC)[None, :] < src_len[:, None]).astype(jnp.int32)
    spread = jax.random.permutation(local_keys[3], TOKENS) % EXPERTS
    hot_expert = jax.random.randint(local_keys[4], (), 0, EXPERTS)
    to_hot = jax.random.randint(local_keys[5], (TOKENS,), 0, 4) == 0
    expert_idx = jnp.where(to_hot, hot_expert, spread).astype(jnp.int32)
    self_shape = (2, TOKENS, HEADS, CACHE, HEAD)
    cross_shape = (2, TOKENS, HEADS, SRC, HEAD)
    return {
        'hidden': hidden,
        'write_pos': write_pos,
        'enc_mask': enc_mask,
        'expert_idx': expert_idx,
        'self_keys': normal(local_keys[6], self_shape, 1.0).astype(jnp.bfloat16),
        'self_values': normal(local_keys[7], self_shape, 1.0).astype(jnp.bfloat16),
        'cross_keys': normal(local_keys[8], cross_shape, 1.0).astype(jnp.bfloat16),
        'cross_values': normal(local_keys[9], cross_shape, 1.0).astype(jnp.bfloat16),
        'rel_bias': normal(shared_keys[0], (HEADS, CACHE), 1.0),
        'norm_scale': jax.random.uniform(shared_keys[1], (2, 3, D), jnp.float32, 0.5, 1.5),
        'w_query': normal(shared_keys[2], (2, D, WIDTH), 2.0 * (D * HEAD) ** -0.5).astype(jnp.bfloat16),
        'w_key': normal(shared_keys[3], (2, D, WIDTH), D ** -0.5).astype(jnp.bfloat16),
        'w_value': normal(shared_keys[4], (2, D, WIDTH), D ** -0.5).astype(jnp.bfloat16),
        'w_out': normal(shared_keys[5], (2, WIDTH, D), WIDTH ** -0.5).astype(jnp.bfloat16),
        'w_cross_query': normal(shared_keys[6], (2, D, WIDTH), 2.0 * (D * HEAD) ** -0.5).astype(jnp.bfloat16),
        'w_cross_out': normal(shared_keys[7], (2, WIDTH, D), WIDTH ** -0.5).astype(jnp.bfloat16),
        'dense_gate': normal(shared_keys[8], (D, FF), D ** -0.5).astype(jnp.bfloat16),
        'dense_up': normal(shared_keys[9], (D, FF), D ** -0.5).astype(jnp.bfloat16),
        'dense_down': normal(shared_keys[10], (FF, D), FF ** -0.5).astype(jnp.bfloat16),
        'router': normal(shared_keys[11], (D, EXPERTS), 2.0 * D ** -0.5),
        'exp_gate': normal(shared_keys[12], (EXPERTS, D, FF), D ** -0.5).astype(jnp.bfloat16),
        'exp_up': normal(shared_keys[13], (EXPERTS, D, FF), D ** -0.5).astype(jnp.bfloat16),
        'exp_down': normal(shared_keys[14], (EXPERTS, FF, D), 0.5 * (EXPERTS / FF) ** 0.5).astype(jnp.bfloat16),
    }


def rms_norm(h_cur, scale):
    h_float = h_cur.astype(jnp.float32)
    inv_rms = lax.rsqrt(jnp.mean(h_float * h_float, axis=-1, keepdims=True) + EPS)
    return (h_float * inv_rms * scale).astype(jnp.bfloat16)


def add_residual(h_cur, delta):
    return (h_cur.astype(jnp.float32) + delta.astype(jnp.float32)).astype(jnp.bfloat16)


def project(normed, weight):
    return jnp.dot(normed, weight, preferred_element_type=jnp.float32)


def self_attention(normed, write_pos, keys, values, w_query, w_key, w_value, w_out, rel_bias):
    tokens = normed.shape[0]
    query = project(normed, w_query).astype(jnp.bfloat16).reshape(tokens, HEADS, HEAD)
    key_new = project(normed, w_key).astype(jnp.bfloat16).reshape(tokens, HEADS, HEAD)
    value_new = project(normed, w_value).astype(jnp.bfloat16).reshape(tokens, HEADS, HEAD)
    distance = write_pos[:, None] - jnp.arange(CACHE)[None, :]
    at_slot = (distance == 0)[:, None, :, None]
    keys = jnp.where(at_slot, key_new[:, :, None, :], keys)
    values = jnp.where(at_slot, value_new[:, :, None, :], values)
    scores = jnp.einsum('thd,thld->thl', query.astype(jnp.float32), keys.astype(jnp.float32))
    bias = jnp.take(rel_bias, jnp.maximum(distance, 0), axis=1)
    scores = jnp.where((distance >= 0)[:, None, :], scores + jnp.swapaxes(bias, 0, 1), NEG_BIG)
    attn_prob = jax.nn.softmax(scores, axis=-1).astype(jnp.bfloat16)
    context = jnp.einsum('thl,thld->thd', attn_prob.astype(jnp.float32), values.astype(jnp.float32)).astype(jnp.bfloat16)
    attn_out = project(context.reshape(tokens, WIDTH), w_out).astype(jnp.bfloat16)
    return attn_out, keys, values


def cross_attention(normed, enc_mask, keys, values, w_query, w_out):
    tokens = normed.shape[0]
    query = project(normed, w_query).astype(jnp.bfloat16).reshape(tokens, HEADS, HEAD)
    scores = jnp.einsum('thd,thsd->ths', query.astype(jnp.float32), keys.astype(jnp.float32))
    scores = jnp.where((enc_mask > 0)[:, None, :], scores, NEG_BIG)
    attn_prob = jax.nn.softmax(scores, axis=-1).astype(jnp.bfloat16)
    context = jnp.einsum('ths,thsd->thd', attn_prob.astype(jnp.float32), values.astype(jnp.float32)).astype(jnp.bfloat16)
    return project(context.reshape(tokens, WIDTH), w_out).astype(jnp.bfloat16)


def gated_ffn(normed, w_gate, w_up, w_down):
    product = (jax.nn.gelu(project(normed, w_gate)) * project(normed, w_up)).astype(jnp.bfloat16)
    return project(product, w_down).astype(jnp.bfloat16)


def switch_ffn(normed, expert_idx, router, exp_gate, exp_up, exp_down):
    logits = jnp.dot(normed.astype(jnp.float32), router)
    route_prob = jax.nn.softmax(logits, axis=-1)
    gate = jnp.take_along_axis(route_prob, expert_idx[:, None], axis=1)[:, 0]
    onehot = (expert_idx[:, None] == jnp.arange(EXPERTS)[None, :]).astype(jnp.int32)
    onehot = onehot.reshape(GROUPS, TOK_DEV, EXPERTS)
    slot = jnp.sum((jnp.cumsum(onehot, axis=1) - onehot) * onehot, axis=2)
    dispatch = (onehot[..., None] * (slot[:, :, None, None] == jnp.arange(CAPACITY))).astype(jnp.float32)
    x_groups = normed.reshape(GROUPS, TOK_DEV, D).astype(jnp.float32)
    buffers = jnp.einsum('gtec,gtd->egcd', dispatch, x_groups).astype(jnp.bfloat16)
    buffers = buffers.reshape(EXPERTS, GROUPS * CAPACITY, D)

    def run_expert(expert):
        rows, w_gate, w_up, w_down = expert
        return gated_ffn(rows, w_gate, w_up, w_down)

    expert_out = lax.map(run_expert, (buffers, exp_gate, exp_up, exp_down))
    expert_out = expert_out.reshape(EXPERTS, GROUPS, CAPACITY, D).astype(jnp.float32)
    combined = jnp.einsum('gtec,egcd->gtd', dispatch, expert_out).reshape(TOKENS, D)
    return gate[:, None] * combined


def attention_block(layer, h_cur, write_pos, enc_mask, self_keys, self_values, cross_keys, cross_values, rel_bias, norm_scale, w_query, w_key, w_value, w_out, w_cross_query, w_cross_out):
    def one_group(group):
        h_grp, pos_grp, mask_grp, keys_grp, values_grp, ckeys_grp, cvalues_grp = group
        normed = rms_norm(h_grp, norm_scale[layer, 0])
        attn_out, keys_grp, values_grp = self_attention(normed, pos_grp, keys_grp, values_grp, w_query[layer], w_key[layer], w_value[layer], w_out[layer], rel_bias)
        h_grp = add_residual(h_grp, attn_out)
        normed = rms_norm(h_grp, norm_scale[layer, 1])
        cross_out = cross_attention(normed, mask_grp, ckeys_grp, cvalues_grp, w_cross_query[layer], w_cross_out[layer])
        return add_residual(h_grp, cross_out), keys_grp, values_grp

    def grouped(array_in):
        return array_in.reshape((GROUPS, TOK_DEV) + array_in.shape[1:])

    h_grp, keys_new, values_new = lax.map(one_group, (grouped(h_cur), grouped(write_pos), grouped(enc_mask), grouped(self_keys[layer]), grouped(self_values[layer]), grouped(cross_keys[layer]), grouped(cross_values[layer])))
    return h_grp.reshape(TOKENS, D), keys_new.reshape(self_keys.shape[1:]), values_new.reshape(self_values.shape[1:])


def reference(hidden, write_pos, enc_mask, expert_idx, self_keys, self_values, cross_keys, cross_values, rel_bias, norm_scale, w_query, w_key, w_value, w_out, w_cross_query, w_cross_out, dense_gate, dense_up, dense_down, router, exp_gate, exp_up, exp_down):
    h_cur, keys_a, values_a = attention_block(0, hidden, write_pos, enc_mask, self_keys, self_values, cross_keys, cross_values, rel_bias, norm_scale, w_query, w_key, w_value, w_out, w_cross_query, w_cross_out)
    normed = rms_norm(h_cur, norm_scale[0, 2])
    h_cur = add_residual(h_cur, gated_ffn(normed, dense_gate, dense_up, dense_down))
    h_cur, keys_b, values_b = attention_block(1, h_cur, write_pos, enc_mask, self_keys, self_values, cross_keys, cross_values, rel_bias, norm_scale, w_query, w_key, w_value, w_out, w_cross_query, w_cross_out)
    normed = rms_norm(h_cur, norm_scale[1, 2])
    h_cur = add_residual(h_cur, switch_ffn(normed, expert_idx, router, exp_gate, exp_up, exp_down))
    return h_cur, jnp.stack([keys_a, keys_b]), jnp.stack([values_a, values_b])
```

```python
import functools

import jax
import jax.numpy as jnp
from jax import lax
from jax.experimental import pallas as pl
from jax.experimental.pallas import tpu as pltpu
from jax.sharding import PartitionSpec as P

EPS = 1e-6
NEG_BIG = -1e9
MESH = pl.DeviceIdType.MESH
BF16 = jnp.bfloat16
F32 = jnp.float32
VMEM_LIMIT = 63 * 1024 * 1024
SLOTS = 4


def rms_norm(h_float, scale):
    inv_rms = lax.rsqrt(jnp.mean(h_float * h_float, axis=-1, keepdims=True) + EPS)
    return (h_float * inv_rms * scale).astype(BF16)


def dot(a, b):
    return jnp.dot(a, b, preferred_element_type=F32)


def dot_t(a, b):
    return lax.dot_general(a, b, (((0,), (0,)), ((), ())), preferred_element_type=F32)


def dot_nt(a, b):
    return lax.dot_general(a, b, (((1,), (1,)), ((), ())), preferred_element_type=F32)


def fold_rows(prod):
    parts = [prod[i * 8:(i + 1) * 8] for i in range(prod.shape[0] // 8)]
    while len(parts) > 1:
        parts = [a + b for a, b in zip(parts[::2], parts[1::2])]
    return parts[0]


def score_head(q_head, keys, head, acc_ref, merge=None):
    for slot in range(keys.shape[1]):
        k_slot = keys[head, slot]
        if merge is not None:
            pos_b, k_new = merge
            k_slot = jnp.where(pos_b == jnp.asarray(slot, BF16), k_new, k_slot)
            keys[head, slot] = k_slot
        acc_ref[head, slot * 8:(slot + 1) * 8, :] = fold_rows(k_slot.astype(F32) * q_head)


def gather_scores(acc_ref, head, slots):
    total = acc_ref[head, pl.ds(0, slots, stride=8), :]
    for i in range(1, 8):
        total = total + acc_ref[head, pl.ds(i, slots, stride=8), :]
    return total


def softmax_rows(scores):
    top = jnp.max(scores, axis=0, keepdims=True)
    e = jnp.exp(scores - top)
    return (e / jnp.sum(e, axis=0, keepdims=True)).astype(BF16).astype(F32)


def context_head(p_ref, values, head, merge=None):
    total = None
    for slot in range(values.shape[1]):
        v_slot = values[head, slot]
        if merge is not None:
            pos_b, v_new = merge
            v_slot = jnp.where(pos_b == jnp.asarray(slot, BF16), v_new, v_slot)
            values[head, slot] = v_slot
        term = v_slot.astype(F32) * p_ref[head, slot:slot + 1, :]
        total = term if total is None else total + term
    return total


def self_kernel(layer, first, *refs):
    if first:
        (h_ref, pos_ref, scale_ref, rel_ref, wq_hbm, wk_hbm, wv_hbm, wo_hbm, k_hbm, v_hbm,
         part_ref, bias_ref, ko_hbm, vo_hbm,
         w_in, wo_ref, keys, values, q_t, k_t, v_t, acc_ref, p_ref, ctx_t,
         w_sem, k_sem, v_sem, ko_sem, vo_sem) = refs
    else:
        (h_ref, pos_ref, scale_ref, bias_ref, wq_hbm, wk_hbm, wv_hbm, wo_hbm, k_hbm, v_hbm, _, _,
         part_ref, ko_hbm, vo_hbm,
         w_in, wo_ref, keys, values, q_t, k_t, v_t, acc_ref, p_ref, ctx_t,
         w_sem, k_sem, v_sem, ko_sem, vo_sem) = refs
    heads, slots, head_dim, tokens = keys.shape

    w_copies = [pltpu.make_async_copy(w.at[layer], w_in.at[i], w_sem.at[i]) for i, w in enumerate((wq_hbm, wk_hbm, wv_hbm))]
    w_copies.append(pltpu.make_async_copy(wo_hbm.at[layer], wo_ref, w_sem.at[3]))

    def k_in(head):
        return pltpu.make_async_copy(k_hbm.at[layer, head], keys.at[head], k_sem.at[head])

    def v_in(head):
        return pltpu.make_async_copy(v_hbm.at[layer, head], values.at[head], v_sem.at[head])

    def k_out(head):
        return pltpu.make_async_copy(keys.at[head], ko_hbm.at[layer, head], ko_sem.at[head])

    def v_out(head):
        return pltpu.make_async_copy(values.at[head], vo_hbm.at[layer, head], vo_sem.at[head])

    for c in w_copies[:3]:
        c.start()
    for head in range(heads):
        k_in(head).start()
    for head in range(heads):
        v_in(head).start()
    w_copies[3].start()

    x = rms_norm(h_ref[...].astype(F32), scale_ref[0, layer:layer + 1, :])
    pos = pos_ref[...]
    dist = pos - lax.broadcasted_iota(jnp.int32, (slots, tokens), 0)
    valid = dist >= 0
    if first:
        bias = [jnp.zeros((slots, tokens), F32)] * heads
        for d in range(slots):
            hit = dist == d
            bias = [jnp.where(hit, rel_ref[head, d], b) for head, b in enumerate(bias)]
        for head in range(heads):
            bias_ref[head] = bias[head]
    pos_b = jnp.broadcast_to(pos.astype(F32), (head_dim, tokens)).astype(BF16)

    for i, target in enumerate((q_t, k_t, v_t)):
        w_copies[i].wait()
        proj = dot(x, w_in[i]).astype(BF16).astype(F32)
        target[...] = jnp.transpose(proj).reshape(target.shape).astype(target.dtype)

    def score_step(head, carry):
        k_in(head).wait()
        score_head(q_t[head], keys, head, acc_ref, (pos_b, k_t[head]))
        k_out(head).start()
        return carry

    lax.fori_loop(0, heads, score_step, 0)
    for head in range(heads):
        scores = jnp.where(valid, gather_scores(acc_ref, head, slots) + bias_ref[head], NEG_BIG)
        p_ref[head] = softmax_rows(scores)

    def context_step(head, carry):
        v_in(head).wait()
        ctx_t[head] = context_head(p_ref, values, head, (pos_b, v_t[head]))
        v_out(head).start()
        return carry

    lax.fori_loop(0, heads, context_step, 0)
    ctx = jnp.transpose(ctx_t[...].reshape(heads * head_dim, tokens)).astype(BF16)
    w_copies[3].wait()
    part_ref[...] = dot(ctx, wo_ref[...]).astype(BF16)
    for head in range(heads):
        k_out(head).wait()
        v_out(head).wait()


def self_attention(layer, h, pos, scale, bias, w_query, w_key, w_value, w_out, keys, values, prev=None):
    first = prev is None
    _, heads, slots, head_dim, tokens = keys.shape
    width, model = w_out.shape[1:]
    vmem = pl.BlockSpec(memory_space=pltpu.VMEM)
    hbm = pl.BlockSpec(memory_space=pl.ANY)
    smem = pl.BlockSpec(memory_space=pltpu.SMEM)
    ins = [h, pos, scale, bias, w_query, w_key, w_value, w_out, keys, values]
    in_specs = [vmem, vmem, vmem, smem if first else vmem] + [hbm] * 6
    cache = jax.ShapeDtypeStruct(keys.shape, keys.dtype)
    out_shape = [jax.ShapeDtypeStruct((tokens, model), BF16)]
    out_specs = [vmem]
    aliases = {}
    if first:
        out_shape.append(jax.ShapeDtypeStruct((heads, slots, tokens), F32))
        out_specs.append(vmem)
    else:
        ins += list(prev)
        in_specs += [hbm, hbm]
        aliases = {10: 1, 11: 2}
    out_shape += [cache, cache]
    out_specs += [hbm, hbm]
    dma = pltpu.SemaphoreType.DMA
    return pl.pallas_call(
        functools.partial(self_kernel, layer, first),
        out_shape=out_shape,
        in_specs=in_specs,
        out_specs=out_specs,
        input_output_aliases=aliases,
        scratch_shapes=[
            pltpu.VMEM((3, model, width), BF16),
            pltpu.VMEM((width, model), BF16),
            pltpu.VMEM((heads, slots, head_dim, tokens), BF16),
            pltpu.VMEM((heads, slots, head_dim, tokens), BF16),
            pltpu.VMEM((heads, head_dim, tokens), F32),
            pltpu.VMEM((heads, head_dim, tokens), BF16),
            pltpu.VMEM((heads, head_dim, tokens), BF16),
            pltpu.VMEM((heads, slots * 8, tokens), F32),
            pltpu.VMEM((heads, slots, tokens), F32),
            pltpu.VMEM((heads, head_dim, tokens), F32),
            dma((4,)), dma((heads,)), dma((heads,)), dma((heads,)), dma((heads,)),
        ],
        compiler_params=pltpu.CompilerParams(vmem_limit_bytes=VMEM_LIMIT),
        name=f"self_attention_{layer}",
    )(*ins)


def tp_exchange(src, dst, send_sem, recv_sem):
    return pltpu.make_async_remote_copy(
        src_ref=src, dst_ref=dst, send_sem=send_sem, recv_sem=recv_sem,
        device_id={"tp": 1 - lax.axis_index("tp")}, device_id_type=MESH)


def add_parts(h_float, mine, other):
    delta = (mine.astype(F32) + other.astype(F32)).astype(BF16)
    return (h_float + delta.astype(F32)).astype(BF16).astype(F32)


def cross_part(layer, x, mask, wq_copy, wq_ref, wo_copy, wo_ref, k_in, keys, v_in, values, q_t, acc_ref, p_ref, ctx_t):
    heads, slots, head_dim, tokens = keys.shape
    wq_copy.wait()
    proj = dot(x, wq_ref[...]).astype(BF16).astype(F32)
    q_t[...] = jnp.transpose(proj).reshape(heads, head_dim, tokens)

    def score_step(head, carry):
        k_in(head).wait()
        score_head(q_t[head], keys, head, acc_ref)
        return carry

    lax.fori_loop(0, heads, score_step, 0)
    valid = mask > 0
    for head in range(heads):
        p_ref[head] = softmax_rows(jnp.where(valid, gather_scores(acc_ref, head, slots), NEG_BIG))

    def context_step(head, carry):
        v_in(head).wait()
        ctx_t[head] = context_head(p_ref, values, head)
        return carry

    lax.fori_loop(0, heads, context_step, 0)
    ctx = jnp.transpose(ctx_t[...].reshape(heads * head_dim, tokens)).astype(BF16)
    wo_copy.wait()
    return dot(ctx, wo_ref[...]).astype(BF16)


def middle_kernel(layer, h_ref, part_ref, mask_ref, scale_ref, wq_hbm, wo_hbm, k_hbm, v_hbm, dg_hbm, du_hbm, dd_hbm,
                  out_ref,
                  wq_ref, wo_ref, keys, values, dg_ref, du_ref, dd_ref, q_t, acc_ref, p_ref, ctx_t, mine_ref, other_ref, prod_ref,
                  w_sem, k_sem, v_sem, send_sem, recv_sem):
    heads = keys.shape[0]

    def k_in(head):
        return pltpu.make_async_copy(k_hbm.at[layer, head], keys.at[head], k_sem.at[head])

    def v_in(head):
        return pltpu.make_async_copy(v_hbm.at[layer, head], values.at[head], v_sem.at[head])

    wq_copy = pltpu.make_async_copy(wq_hbm.at[layer], wq_ref, w_sem.at[0])
    wo_copy = pltpu.make_async_copy(wo_hbm.at[layer], wo_ref, w_sem.at[1])
    dense = [pltpu.make_async_copy(s, d, w_sem.at[2 + i]) for i, (s, d) in enumerate(((dg_hbm, dg_ref), (du_hbm, du_ref), (dd_hbm, dd_ref)))]

    barrier = pltpu.get_barrier_semaphore()
    pl.semaphore_signal(barrier, inc=1, device_id={"tp": 1 - lax.axis_index("tp")}, device_id_type=MESH)
    wq_copy.start()
    for head in range(heads):
        k_in(head).start()
    for head in range(heads):
        v_in(head).start()
    wo_copy.start()
    for c in dense:
        c.start()
    pl.semaphore_wait(barrier, 1)

    copies = [tp_exchange(part_ref if i == 0 else mine_ref.at[i - 1], other_ref.at[i], send_sem.at[i], recv_sem.at[i]) for i in range(3)]
    copies[0].start()
    copies[0].wait()
    h_float = add_parts(h_ref[...].astype(F32), part_ref[...], other_ref[0])

    x = rms_norm(h_float, scale_ref[1, layer:layer + 1, :])
    mine_ref[0] = cross_part(layer, x, mask_ref[...], wq_copy, wq_ref, wo_copy, wo_ref, k_in, keys, v_in, values, q_t, acc_ref, p_ref, ctx_t)
    copies[1].start()
    copies[1].wait()
    h_float = add_parts(h_float, mine_ref[0], other_ref[1])

    x = rms_norm(h_float, scale_ref[2, layer:layer + 1, :])
    dense[0].wait()
    dense[1].wait()
    width = dg_ref.shape[1]
    step = 512
    for c in range(0, width, step):
        gate_in = dot(x, dg_ref[:, c:c + step])
        lin_in = dot(x, du_ref[:, c:c + step])
        prod_ref[:, c:c + step] = (jax.nn.gelu(gate_in) * lin_in).astype(BF16)
    dense[2].wait()
    mine_ref[1] = dot(prod_ref[...], dd_ref[...]).astype(BF16)
    copies[2].start()
    copies[2].wait()
    out_ref[...] = add_parts(h_float, mine_ref[1], other_ref[2]).astype(BF16)


def middle(layer, h, part, mask, scale, w_query, w_out, keys, values, dense_gate, dense_up, dense_down):
    _, heads, slots, head_dim, tokens = keys.shape
    width, model = w_out.shape[1:]
    ff = dense_gate.shape[1]
    vmem = pl.BlockSpec(memory_space=pltpu.VMEM)
    hbm = pl.BlockSpec(memory_space=pl.ANY)
    dma = pltpu.SemaphoreType.DMA
    return pl.pallas_call(
        functools.partial(middle_kernel, layer),
        out_shape=jax.ShapeDtypeStruct((tokens, model), BF16),
        in_specs=[vmem] * 4 + [hbm] * 7,
        out_specs=vmem,
        scratch_shapes=[
            pltpu.VMEM((model, width), BF16),
            pltpu.VMEM((width, model), BF16),
            pltpu.VMEM((heads, slots, head_dim, tokens), BF16),
            pltpu.VMEM((heads, slots, head_dim, tokens), BF16),
            pltpu.VMEM((model, ff), BF16),
            pltpu.VMEM((model, ff), BF16),
            pltpu.VMEM((ff, model), BF16),
            pltpu.VMEM((heads, head_dim, tokens), F32),
            pltpu.VMEM((heads, slots * 8, tokens), F32),
            pltpu.VMEM((heads, slots, tokens), F32),
            pltpu.VMEM((heads, head_dim, tokens), F32),
            pltpu.VMEM((2, tokens, model), BF16),
            pltpu.VMEM((3, tokens, model), BF16),
            pltpu.VMEM((tokens, ff), BF16),
            dma((5,)), dma((heads,)), dma((heads,)), dma((3,)), dma((3,)),
        ],
        compiler_params=pltpu.CompilerParams(vmem_limit_bytes=VMEM_LIMIT, collective_id=0, has_side_effects=True),
        name="middle",
    )(h, part, mask, scale, w_query, w_out, keys, values, dense_gate, dense_up, dense_down)


def last_kernel(layer, h_ref, part_ref, mask_ref, idx_ref, scale_ref, router_ref, wq_hbm, wo_hbm, k_hbm, v_hbm, eg_hbm, eu_hbm, ed_hbm,
                out_ref,
                wq_ref, wo_ref, keys, values, eg_ref, eu_ref, ed_ref, q_t, acc_ref, p_ref, ctx_t, mine_ref, other_ref,
                place_ref, send_x, recv_x, rows_ref, y_ref, send_y, recv_y, gate_ref,
                w_sem, k_sem, v_sem, e_sem, tp_send, tp_recv, x_send, x_recv, y_send, y_recv):
    heads = keys.shape[0]
    tokens, model = h_ref.shape
    experts = router_ref.shape[0]
    groups, chunks, chunk_rows, _ = recv_x.shape
    local = experts // groups
    capacity = place_ref.shape[0] // experts
    per_chunk = local // chunks
    tp = lax.axis_index("tp")
    ep = lax.axis_index("ep")

    def peer_ep(offset):
        return lax.rem(ep + offset, groups)

    def peer_tp(offset):
        return lax.rem(tp + offset, 2)

    def k_in(head):
        return pltpu.make_async_copy(k_hbm.at[layer, head], keys.at[head], k_sem.at[head])

    def v_in(head):
        return pltpu.make_async_copy(v_hbm.at[layer, head], values.at[head], v_sem.at[head])

    def weights_in(expert, slot):
        return [pltpu.make_async_copy(s.at[expert], d.at[slot], e_sem.at[slot, i])
                for i, (s, d) in enumerate(((eg_hbm, eg_ref), (eu_hbm, eu_ref), (ed_hbm, ed_ref)))]

    wq_copy = pltpu.make_async_copy(wq_hbm.at[layer], wq_ref, w_sem.at[0])
    wo_copy = pltpu.make_async_copy(wo_hbm.at[layer], wo_ref, w_sem.at[1])

    others = [(dt, de) for dt in range(2) for de in range(groups) if dt or de]
    barrier = pltpu.get_barrier_semaphore()
    for dt, de in others:
        pl.semaphore_signal(barrier, inc=1, device_id={"tp": peer_tp(dt), "ep": peer_ep(de)}, device_id_type=MESH)
    wq_copy.start()
    for head in range(heads):
        k_in(head).start()
    for head in range(heads):
        v_in(head).start()
    wo_copy.start()
    for slot in range(SLOTS):
        for c in weights_in(slot, slot):
            c.start()
    pl.semaphore_wait(barrier, len(others))

    copies = [tp_exchange(part_ref if i == 0 else mine_ref, other_ref.at[i], tp_send.at[i], tp_recv.at[i]) for i in range(2)]
    copies[0].start()

    idx = idx_ref[...]
    onehot = (lax.broadcasted_iota(jnp.int32, (experts, tokens), 0) == idx).astype(F32)
    earlier = (lax.broadcasted_iota(jnp.int32, (tokens, tokens), 0) < lax.broadcasted_iota(jnp.int32, (tokens, tokens), 1)).astype(F32)
    counts = dot(onehot.astype(BF16), earlier.astype(BF16))
    slot_of = jnp.sum(counts * onehot, axis=0, keepdims=True).astype(jnp.int32)
    row_of = jnp.where(slot_of < capacity, idx * capacity + slot_of, -1)
    place_ref[...] = (lax.broadcasted_iota(jnp.int32, (experts * capacity, tokens), 0) == row_of).astype(F32).astype(BF16)

    copies[0].wait()
    h_float = add_parts(h_ref[...].astype(F32), part_ref[...], other_ref[0])
    x = rms_norm(h_float, scale_ref[1, layer:layer + 1, :])
    mine_ref[...] = cross_part(layer, x, mask_ref[...], wq_copy, wq_ref, wo_copy, wo_ref, k_in, keys, v_in, values, q_t, acc_ref, p_ref, ctx_t)
    copies[1].start()
    copies[1].wait()
    h_float = add_parts(h_float, mine_ref[...], other_ref[1])
    x = rms_norm(h_float, scale_ref[2, layer:layer + 1, :])

    send_x[...] = dot(place_ref[...], x).astype(BF16).reshape(send_x.shape)

    def x_copy(chunk, offset):
        return pltpu.make_async_remote_copy(
            src_ref=send_x.at[peer_ep(offset), chunk], dst_ref=recv_x.at[ep, chunk],
            send_sem=x_send.at[chunk, offset - 1], recv_sem=x_recv.at[chunk, ep],
            device_id={"ep": peer_ep(offset)}, device_id_type=MESH)

    def x_arrival(chunk, offset):
        return pltpu.make_async_remote_copy(
            src_ref=send_x.at[peer_ep(offset), chunk], dst_ref=recv_x.at[peer_ep(offset), chunk],
            send_sem=x_send.at[chunk, offset - 1], recv_sem=x_recv.at[chunk, peer_ep(offset)],
            device_id={"ep": peer_ep(offset)}, device_id_type=MESH)

    for chunk in range(chunks):
        for offset in range(1, groups):
            x_copy(chunk, offset).start()
    recv_x[ep] = send_x[ep]

    router = router_ref[...]
    high = router.astype(BF16)
    rest = router - high.astype(F32)
    mid = rest.astype(BF16)
    low = (rest - mid.astype(F32)).astype(BF16)
    logits = dot_nt(high, x) + (dot_nt(mid, x) + dot_nt(low, x))
    logits_exp = jnp.exp(logits - jnp.max(logits, axis=0, keepdims=True))
    gate = jnp.sum(logits_exp * onehot, axis=0, keepdims=True) / jnp.sum(logits_exp, axis=0, keepdims=True)
    gate_ref[...] = jnp.transpose(jnp.broadcast_to(gate, (tokens, tokens)))

    block = groups * chunk_rows
    r0 = lax.broadcasted_iota(jnp.int32, (block, block), 0)
    r1 = lax.broadcasted_iota(jnp.int32, (block, block), 1)
    group_rows = groups * capacity
    source = ((r0 % group_rows) // capacity) * chunk_rows + (r0 // group_rows) * capacity + r0 % capacity
    to_experts = (r1 == source).astype(F32).astype(BF16)
    back = ((r0 % chunk_rows) // capacity) * group_rows + (r0 // chunk_rows) * capacity + r0 % capacity
    to_groups = (r1 == back).astype(F32).astype(BF16)

    def y_copy(chunk, number):
        dt, de = others[number]
        return pltpu.make_async_remote_copy(
            src_ref=send_y.at[chunk, peer_ep(de)], dst_ref=recv_y.at[tp, ep, chunk],
            send_sem=y_send.at[chunk, number], recv_sem=y_recv.at[chunk, tp, ep],
            device_id={"tp": peer_tp(dt), "ep": peer_ep(de)}, device_id_type=MESH)

    def y_arrival(chunk, number):
        dt, de = others[number]
        return pltpu.make_async_remote_copy(
            src_ref=send_y.at[chunk, peer_ep(de)], dst_ref=recv_y.at[peer_tp(dt), peer_ep(de), chunk],
            send_sem=y_send.at[chunk, number], recv_sem=y_recv.at[chunk, peer_tp(dt), peer_ep(de)],
            device_id={"tp": peer_tp(dt), "ep": peer_ep(de)}, device_id_type=MESH)

    def expert_step(expert, carry):
        slot = lax.rem(expert, SLOTS)
        first_row = pl.multiple_of(lax.rem(expert, per_chunk) * group_rows, group_rows)
        rows = rows_ref[pl.ds(first_row, group_rows), :]
        w_copies = weights_in(expert, slot)
        w_copies[0].wait()
        gate_in = dot(rows, eg_ref[slot])
        w_copies[1].wait()
        lin_in = dot(rows, eu_ref[slot])
        product = (jax.nn.gelu(gate_in) * lin_in).astype(BF16)
        w_copies[2].wait()
        y_ref[pl.ds(first_row, group_rows), :] = dot(product, ed_ref[slot]).astype(BF16)

        @pl.when(expert + SLOTS < local)
        def _():
            for c in weights_in(expert + SLOTS, slot):
                c.start()
        return carry

    def chunk_step(chunk, carry):
        for offset in range(1, groups):
            x_arrival(chunk, offset).wait_recv()
        arrived = recv_x[:, chunk].reshape(block, model)
        rows_ref[...] = dot(to_experts, arrived).astype(BF16)
        lax.fori_loop(chunk * per_chunk, (chunk + 1) * per_chunk, expert_step, 0)
        send_y[chunk] = dot(to_groups, y_ref[...]).astype(BF16).reshape(groups, chunk_rows, model)
        for number in range(len(others)):
            y_copy(chunk, number).start()
        recv_y[tp, ep, chunk] = send_y[chunk, ep]
        return carry

    lax.fori_loop(0, chunks, chunk_step, 0)

    for chunk in range(chunks):
        for number in range(len(others)):
            y_arrival(chunk, number).wait_recv()
    returned = (recv_y[0].astype(F32) + recv_y[1].astype(F32)).astype(BF16).reshape(experts * capacity, model)
    combined = dot_t(place_ref[...], returned)
    gate_col = gate_ref[...]
    for c in range(0, model, tokens):
        delta = gate_col * combined[:, c:c + tokens]
        out_ref[:, c:c + tokens] = (h_float[:, c:c + tokens] + delta).astype(BF16)
    for chunk in range(chunks):
        for offset in range(1, groups):
            x_copy(chunk, offset).wait_send()
        for number in range(len(others)):
            y_copy(chunk, number).wait_send()


def last(layer, h, part, mask, idx, scale, router, w_query, w_out, keys, values, exp_gate, exp_up, exp_down, groups):
    _, heads, slots, head_dim, tokens = keys.shape
    width, model = w_out.shape[1:]
    local, _, ff = exp_gate.shape
    experts = router.shape[0]
    capacity = (2 * tokens + experts - 1) // experts
    chunk_rows = 16
    chunks = local * capacity // chunk_rows
    vmem = pl.BlockSpec(memory_space=pltpu.VMEM)
    hbm = pl.BlockSpec(memory_space=pl.ANY)
    dma = pltpu.SemaphoreType.DMA
    return pl.pallas_call(
        functools.partial(last_kernel, layer),
        out_shape=jax.ShapeDtypeStruct((tokens, model), BF16),
        in_specs=[vmem] * 6 + [hbm] * 7,
        out_specs=vmem,
        scratch_shapes=[
            pltpu.VMEM((model, width), BF16),
            pltpu.VMEM((width, model), BF16),
            pltpu.VMEM((heads, slots, head_dim, tokens), BF16),
            pltpu.VMEM((heads, slots, head_dim, tokens), BF16),
            pltpu.VMEM((SLOTS, model, ff), BF16),
            pltpu.VMEM((SLOTS, model, ff), BF16),
            pltpu.VMEM((SLOTS, ff, model), BF16),
            pltpu.VMEM((heads, head_dim, tokens), F32),
            pltpu.VMEM((heads, slots * 8, tokens), F32),
            pltpu.VMEM((heads, slots, tokens), F32),
            pltpu.VMEM((heads, head_dim, tokens), F32),
            pltpu.VMEM((tokens, model), BF16),
            pltpu.VMEM((2, tokens, model), BF16),
            pltpu.VMEM((experts * capacity, tokens), BF16),
            pltpu.VMEM((groups, chunks, chunk_rows, model), BF16),
            pltpu.VMEM((groups, chunks, chunk_rows, model), BF16),
            pltpu.VMEM((groups * chunk_rows, model), BF16),
            pltpu.VMEM((groups * chunk_rows, model), BF16),
            pltpu.VMEM((chunks, groups, chunk_rows, model), BF16),
            pltpu.VMEM((2, groups, chunks, chunk_rows, model), BF16),
            pltpu.VMEM((tokens, tokens), F32),
            dma((2,)), dma((heads,)), dma((heads,)), dma((SLOTS, 3)), dma((2,)), dma((2,)),
            dma((chunks, groups - 1)), dma((chunks, groups)), dma((chunks, 2 * groups - 1)), dma((chunks, 2, groups)),
        ],
        compiler_params=pltpu.CompilerParams(vmem_limit_bytes=VMEM_LIMIT, collective_id=1, has_side_effects=True),
        name="last",
    )(h, part, mask, idx, scale, router, w_query, w_out, keys, values, exp_gate, exp_up, exp_down)


def decode_body(groups, hidden, write_pos, enc_mask, expert_idx, self_keys, self_values, cross_keys, cross_values, rel_bias, norm_scale, w_query, w_key, w_value, w_out, w_cross_query, w_cross_out, dense_gate, dense_up, dense_down, router, exp_gate, exp_up, exp_down):
    def lanes(cache):
        return jnp.transpose(cache, (0, 2, 3, 4, 1))

    pos = write_pos.reshape(1, -1)
    idx = expert_idx.reshape(1, -1)
    mask = jnp.transpose(enc_mask)
    scale = jnp.transpose(norm_scale, (1, 0, 2))
    keys, values, ckeys, cvalues = map(lanes, (self_keys, self_values, cross_keys, cross_values))
    part, bias, k_out, v_out = self_attention(0, hidden, pos, scale, rel_bias, w_query, w_key, w_value, w_out, keys, values)
    h = middle(0, hidden, part, mask, scale, w_cross_query, w_cross_out, ckeys, cvalues, dense_gate, dense_up, dense_down)
    part, k_out, v_out = self_attention(1, h, pos, scale, bias, w_query, w_key, w_value, w_out, keys, values, (k_out, v_out))
    h = last(1, h, part, mask, idx, scale, jnp.transpose(router), w_cross_query, w_cross_out, ckeys, cvalues, exp_gate, exp_up, exp_down, groups)
    return h, jnp.transpose(k_out, (0, 4, 1, 2, 3)), jnp.transpose(v_out, (0, 4, 1, 2, 3))


def solution(mesh):
    batch = ('dp', 'ep')
    row_spec = P(batch, None)
    vec_spec = P(batch)
    cache_spec = P(None, batch, 'tp', None, None)
    col_spec = P(None, None, 'tp')
    out_rows = P(None, 'tp', None)
    in_specs = (row_spec, vec_spec, row_spec, vec_spec, cache_spec, cache_spec, cache_spec, cache_spec, P('tp', None), P(), col_spec, col_spec, col_spec, out_rows, col_spec, out_rows, P(None, 'tp'), P(None, 'tp'), P('tp', None), P(), P('ep', None, 'tp'), P('ep', None, 'tp'), P('ep', 'tp', None))
    out_specs = (row_spec, cache_spec, cache_spec)
    body = functools.partial(decode_body, mesh.shape['ep'])
    return jax.shard_map(body, mesh=mesh, in_specs=in_specs, out_specs=out_specs, check_vma=False)
```

```python
import functools

import jax
import jax.numpy as jnp
from jax import lax
from jax.experimental import pallas as pl
from jax.experimental.pallas import tpu as pltpu
from jax.sharding import PartitionSpec as P

EPS = 1e-6
NEG_BIG = -1e9
MESH = pl.DeviceIdType.MESH
BF16 = jnp.bfloat16
F32 = jnp.float32
VMEM_LIMIT = 63 * 1024 * 1024
SLOTS = 7


def rms_norm(h_float, scale):
    inv_rms = lax.rsqrt(jnp.mean(h_float * h_float, axis=-1, keepdims=True) + EPS)
    return (h_float * inv_rms * scale).astype(BF16)


def dot(a, b):
    return jnp.dot(a, b, preferred_element_type=F32)


def dot_t(a, b):
    return lax.dot_general(a, b, (((0,), (0,)), ((), ())), preferred_element_type=F32)


def dot_nt(a, b):
    return lax.dot_general(a, b, (((1,), (1,)), ((), ())), preferred_element_type=F32)


def fold_rows(prod):
    parts = [prod[i * 8:(i + 1) * 8] for i in range(prod.shape[0] // 8)]
    while len(parts) > 1:
        parts = [a + b for a, b in zip(parts[::2], parts[1::2])]
    return parts[0]


def score_head(q_head, keys, head, acc_ref, merge=None):
    for slot in range(keys.shape[1]):
        k_slot = keys[head, slot]
        if merge is not None:
            pos_b, k_new = merge
            k_slot = jnp.where(pos_b == jnp.asarray(slot, BF16), k_new, k_slot)
            keys[head, slot] = k_slot
        acc_ref[head, slot * 8:(slot + 1) * 8, :] = fold_rows(k_slot.astype(F32) * q_head)


def gather_scores(acc_ref, head, slots):
    total = acc_ref[head, pl.ds(0, slots, stride=8), :]
    for i in range(1, 8):
        total = total + acc_ref[head, pl.ds(i, slots, stride=8), :]
    return total


def softmax_rows(scores):
    top = jnp.max(scores, axis=0, keepdims=True)
    e = jnp.exp(scores - top)
    return (e / jnp.sum(e, axis=0, keepdims=True)).astype(BF16).astype(F32)


def context_head(p_ref, values, head, merge=None):
    total = None
    for slot in range(values.shape[1]):
        v_slot = values[head, slot]
        if merge is not None:
            pos_b, v_new = merge
            v_slot = jnp.where(pos_b == jnp.asarray(slot, BF16), v_new, v_slot)
            values[head, slot] = v_slot
        term = v_slot.astype(F32) * p_ref[head, slot:slot + 1, :]
        total = term if total is None else total + term
    return total


def self_kernel(layer, first, *refs):
    if first:
        (h_ref, pos_ref, scale_ref, rel_ref, wq_hbm, wk_hbm, wv_hbm, wo_hbm, k_hbm, v_hbm,
         part_ref, bias_ref, ko_hbm, vo_hbm,
         w_in, wo_ref, keys, values, q_t, k_t, v_t, acc_ref, p_ref, ctx_t,
         w_sem, k_sem, v_sem, ko_sem, vo_sem) = refs
    else:
        (h_ref, pos_ref, scale_ref, bias_ref, wq_hbm, wk_hbm, wv_hbm, wo_hbm, k_hbm, v_hbm, _, _,
         part_ref, ko_hbm, vo_hbm,
         w_in, wo_ref, keys, values, q_t, k_t, v_t, acc_ref, p_ref, ctx_t,
         w_sem, k_sem, v_sem, ko_sem, vo_sem) = refs
    heads, slots, head_dim, tokens = keys.shape

    w_copies = [pltpu.make_async_copy(w.at[layer], w_in.at[i], w_sem.at[i]) for i, w in enumerate((wq_hbm, wk_hbm, wv_hbm))]
    w_copies.append(pltpu.make_async_copy(wo_hbm.at[layer], wo_ref, w_sem.at[3]))

    def k_in(head):
        return pltpu.make_async_copy(k_hbm.at[layer, head], keys.at[head], k_sem.at[head])

    def v_in(head):
        return pltpu.make_async_copy(v_hbm.at[layer, head], values.at[head], v_sem.at[head])

    def k_out(head):
        return pltpu.make_async_copy(keys.at[head], ko_hbm.at[layer, head], ko_sem.at[head])

    def v_out(head):
        return pltpu.make_async_copy(values.at[head], vo_hbm.at[layer, head], vo_sem.at[head])

    for c in w_copies[:3]:
        c.start()
    for head in range(heads):
        k_in(head).start()
    for head in range(heads):
        v_in(head).start()
    w_copies[3].start()

    x = rms_norm(h_ref[...].astype(F32), scale_ref[0, layer:layer + 1, :])
    pos = pos_ref[...]
    dist = pos - lax.broadcasted_iota(jnp.int32, (slots, tokens), 0)
    valid = dist >= 0
    if first:
        bias = [jnp.zeros((slots, tokens), F32)] * heads
        for d in range(slots):
            hit = dist == d
            bias = [jnp.where(hit, rel_ref[head, d], b) for head, b in enumerate(bias)]
        for head in range(heads):
            bias_ref[head] = bias[head]
    pos_b = jnp.broadcast_to(pos.astype(F32), (head_dim, tokens)).astype(BF16)

    for i, target in enumerate((q_t, k_t, v_t)):
        w_copies[i].wait()
        proj = dot(x, w_in[i]).astype(BF16).astype(F32)
        target[...] = jnp.transpose(proj).reshape(target.shape).astype(target.dtype)

    def score_step(head, carry):
        k_in(head).wait()
        score_head(q_t[head], keys, head, acc_ref, (pos_b, k_t[head]))
        k_out(head).start()
        return carry

    lax.fori_loop(0, heads, score_step, 0)
    for head in range(heads):
        scores = jnp.where(valid, gather_scores(acc_ref, head, slots) + bias_ref[head], NEG_BIG)
        p_ref[head] = softmax_rows(scores)

    def context_step(head, carry):
        v_in(head).wait()
        ctx_t[head] = context_head(p_ref, values, head, (pos_b, v_t[head]))
        v_out(head).start()
        return carry

    lax.fori_loop(0, heads, context_step, 0)
    ctx = jnp.transpose(ctx_t[...].reshape(heads * head_dim, tokens)).astype(BF16)
    w_copies[3].wait()
    part_ref[...] = dot(ctx, wo_ref[...]).astype(BF16)
    for head in range(heads):
        k_out(head).wait()
        v_out(head).wait()


def self_attention(layer, h, pos, scale, bias, w_query, w_key, w_value, w_out, keys, values, prev=None):
    first = prev is None
    _, heads, slots, head_dim, tokens = keys.shape
    width, model = w_out.shape[1:]
    vmem = pl.BlockSpec(memory_space=pltpu.VMEM)
    hbm = pl.BlockSpec(memory_space=pl.ANY)
    smem = pl.BlockSpec(memory_space=pltpu.SMEM)
    ins = [h, pos, scale, bias, w_query, w_key, w_value, w_out, keys, values]
    in_specs = [vmem, vmem, vmem, smem if first else vmem] + [hbm] * 6
    cache = jax.ShapeDtypeStruct(keys.shape, keys.dtype)
    out_shape = [jax.ShapeDtypeStruct((tokens, model), BF16)]
    out_specs = [vmem]
    aliases = {}
    if first:
        out_shape.append(jax.ShapeDtypeStruct((heads, slots, tokens), F32))
        out_specs.append(vmem)
    else:
        ins += list(prev)
        in_specs += [hbm, hbm]
        aliases = {10: 1, 11: 2}
    out_shape += [cache, cache]
    out_specs += [hbm, hbm]
    dma = pltpu.SemaphoreType.DMA
    return pl.pallas_call(
        functools.partial(self_kernel, layer, first),
        out_shape=out_shape,
        in_specs=in_specs,
        out_specs=out_specs,
        input_output_aliases=aliases,
        scratch_shapes=[
            pltpu.VMEM((3, model, width), BF16),
            pltpu.VMEM((width, model), BF16),
            pltpu.VMEM((heads, slots, head_dim, tokens), BF16),
            pltpu.VMEM((heads, slots, head_dim, tokens), BF16),
            pltpu.VMEM((heads, head_dim, tokens), F32),
            pltpu.VMEM((heads, head_dim, tokens), BF16),
            pltpu.VMEM((heads, head_dim, tokens), BF16),
            pltpu.VMEM((heads, slots * 8, tokens), F32),
            pltpu.VMEM((heads, slots, tokens), F32),
            pltpu.VMEM((heads, head_dim, tokens), F32),
            dma((4,)), dma((heads,)), dma((heads,)), dma((heads,)), dma((heads,)),
        ],
        compiler_params=pltpu.CompilerParams(vmem_limit_bytes=VMEM_LIMIT),
        name=f"self_attention_{layer}",
    )(*ins)


def tp_exchange(src, dst, send_sem, recv_sem):
    return pltpu.make_async_remote_copy(
        src_ref=src, dst_ref=dst, send_sem=send_sem, recv_sem=recv_sem,
        device_id={"tp": 1 - lax.axis_index("tp")}, device_id_type=MESH)


def add_parts(h_float, mine, other):
    delta = (mine.astype(F32) + other.astype(F32)).astype(BF16)
    return (h_float + delta.astype(F32)).astype(BF16).astype(F32)


def cross_part(layer, x, mask, wq_copy, wq_ref, wo_copy, wo_ref, k_in, keys, v_in, values, q_t, acc_ref, p_ref, ctx_t):
    heads, slots, head_dim, tokens = keys.shape
    wq_copy.wait()
    proj = dot(x, wq_ref[...]).astype(BF16).astype(F32)
    q_t[...] = jnp.transpose(proj).reshape(heads, head_dim, tokens)

    def score_step(head, carry):
        k_in(head).wait()
        score_head(q_t[head], keys, head, acc_ref)
        return carry

    lax.fori_loop(0, heads, score_step, 0)
    valid = mask > 0
    for head in range(heads):
        p_ref[head] = softmax_rows(jnp.where(valid, gather_scores(acc_ref, head, slots), NEG_BIG))

    def context_step(head, carry):
        v_in(head).wait()
        ctx_t[head] = context_head(p_ref, values, head)
        return carry

    lax.fori_loop(0, heads, context_step, 0)
    ctx = jnp.transpose(ctx_t[...].reshape(heads * head_dim, tokens)).astype(BF16)
    wo_copy.wait()
    return dot(ctx, wo_ref[...]).astype(BF16)


def middle_kernel(layer, h_ref, part_ref, mask_ref, scale_ref, wq_hbm, wo_hbm, k_hbm, v_hbm, dg_hbm, du_hbm, dd_hbm,
                  out_ref,
                  wq_ref, wo_ref, keys, values, dg_ref, du_ref, dd_ref, q_t, acc_ref, p_ref, ctx_t, mine_ref, other_ref, prod_ref,
                  w_sem, k_sem, v_sem, send_sem, recv_sem):
    heads = keys.shape[0]

    def k_in(head):
        return pltpu.make_async_copy(k_hbm.at[layer, head], keys.at[head], k_sem.at[head])

    def v_in(head):
        return pltpu.make_async_copy(v_hbm.at[layer, head], values.at[head], v_sem.at[head])

    wq_copy = pltpu.make_async_copy(wq_hbm.at[layer], wq_ref, w_sem.at[0])
    wo_copy = pltpu.make_async_copy(wo_hbm.at[layer], wo_ref, w_sem.at[1])
    dense = [pltpu.make_async_copy(s, d, w_sem.at[2 + i]) for i, (s, d) in enumerate(((dg_hbm, dg_ref), (du_hbm, du_ref), (dd_hbm, dd_ref)))]

    barrier = pltpu.get_barrier_semaphore()
    pl.semaphore_signal(barrier, inc=1, device_id={"tp": 1 - lax.axis_index("tp")}, device_id_type=MESH)
    wq_copy.start()
    for head in range(heads):
        k_in(head).start()
    for head in range(heads):
        v_in(head).start()
    wo_copy.start()
    for c in dense:
        c.start()
    pl.semaphore_wait(barrier, 1)

    copies = [tp_exchange(part_ref if i == 0 else mine_ref.at[i - 1], other_ref.at[i], send_sem.at[i], recv_sem.at[i]) for i in range(3)]
    copies[0].start()
    copies[0].wait()
    h_float = add_parts(h_ref[...].astype(F32), part_ref[...], other_ref[0])

    x = rms_norm(h_float, scale_ref[1, layer:layer + 1, :])
    mine_ref[0] = cross_part(layer, x, mask_ref[...], wq_copy, wq_ref, wo_copy, wo_ref, k_in, keys, v_in, values, q_t, acc_ref, p_ref, ctx_t)
    copies[1].start()
    copies[1].wait()
    h_float = add_parts(h_float, mine_ref[0], other_ref[1])

    x = rms_norm(h_float, scale_ref[2, layer:layer + 1, :])
    dense[0].wait()
    dense[1].wait()
    width = dg_ref.shape[1]
    step = 512
    for c in range(0, width, step):
        gate_in = dot(x, dg_ref[:, c:c + step])
        lin_in = dot(x, du_ref[:, c:c + step])
        prod_ref[:, c:c + step] = (jax.nn.gelu(gate_in) * lin_in).astype(BF16)
    dense[2].wait()
    mine_ref[1] = dot(prod_ref[...], dd_ref[...]).astype(BF16)
    copies[2].start()
    copies[2].wait()
    out_ref[...] = add_parts(h_float, mine_ref[1], other_ref[2]).astype(BF16)


def middle(layer, h, part, mask, scale, w_query, w_out, keys, values, dense_gate, dense_up, dense_down):
    _, heads, slots, head_dim, tokens = keys.shape
    width, model = w_out.shape[1:]
    ff = dense_gate.shape[1]
    vmem = pl.BlockSpec(memory_space=pltpu.VMEM)
    hbm = pl.BlockSpec(memory_space=pl.ANY)
    dma = pltpu.SemaphoreType.DMA
    return pl.pallas_call(
        functools.partial(middle_kernel, layer),
        out_shape=jax.ShapeDtypeStruct((tokens, model), BF16),
        in_specs=[vmem] * 4 + [hbm] * 7,
        out_specs=vmem,
        scratch_shapes=[
            pltpu.VMEM((model, width), BF16),
            pltpu.VMEM((width, model), BF16),
            pltpu.VMEM((heads, slots, head_dim, tokens), BF16),
            pltpu.VMEM((heads, slots, head_dim, tokens), BF16),
            pltpu.VMEM((model, ff), BF16),
            pltpu.VMEM((model, ff), BF16),
            pltpu.VMEM((ff, model), BF16),
            pltpu.VMEM((heads, head_dim, tokens), F32),
            pltpu.VMEM((heads, slots * 8, tokens), F32),
            pltpu.VMEM((heads, slots, tokens), F32),
            pltpu.VMEM((heads, head_dim, tokens), F32),
            pltpu.VMEM((2, tokens, model), BF16),
            pltpu.VMEM((3, tokens, model), BF16),
            pltpu.VMEM((tokens, ff), BF16),
            dma((5,)), dma((heads,)), dma((heads,)), dma((3,)), dma((3,)),
        ],
        compiler_params=pltpu.CompilerParams(vmem_limit_bytes=VMEM_LIMIT, collective_id=0, has_side_effects=True),
        name="middle",
    )(h, part, mask, scale, w_query, w_out, keys, values, dense_gate, dense_up, dense_down)


def last_kernel(layer, h_ref, part_ref, mask_ref, idx_ref, scale_ref, router_ref, wq_hbm, wo_hbm, k_hbm, v_hbm, eg_hbm, eu_hbm, ed_hbm,
                out_ref,
                wq_ref, wo_ref, keys, values, eg_ref, eu_ref, ed_ref, q_t, acc_ref, p_ref, ctx_t, mine_ref, other_ref,
                place_ref, send_x, recv_x, rows_ref, y_ref, send_y, recv_y, gate_ref,
                w_sem, k_sem, v_sem, e_sem, tp_send, tp_recv, x_send, x_recv, y_send, y_recv):
    heads = keys.shape[0]
    tokens, model = h_ref.shape
    experts = router_ref.shape[0]
    groups, chunks, chunk_rows, _ = recv_x.shape
    local = experts // groups
    capacity = place_ref.shape[0] // experts
    per_chunk = local // chunks
    tp = lax.axis_index("tp")
    ep = lax.axis_index("ep")

    def peer_ep(offset):
        return lax.rem(ep + offset, groups)

    def peer_tp(offset):
        return lax.rem(tp + offset, 2)

    def k_in(head):
        return pltpu.make_async_copy(k_hbm.at[layer, head], keys.at[head], k_sem.at[head])

    def v_in(head):
        return pltpu.make_async_copy(v_hbm.at[layer, head], values.at[head], v_sem.at[head])

    def weights_in(expert, slot):
        return [pltpu.make_async_copy(s.at[expert], d.at[slot], e_sem.at[slot, i])
                for i, (s, d) in enumerate(((eg_hbm, eg_ref), (eu_hbm, eu_ref), (ed_hbm, ed_ref)))]

    wq_copy = pltpu.make_async_copy(wq_hbm.at[layer], wq_ref, w_sem.at[0])
    wo_copy = pltpu.make_async_copy(wo_hbm.at[layer], wo_ref, w_sem.at[1])

    others = [(dt, de) for dt in range(2) for de in range(groups) if dt or de]
    barrier = pltpu.get_barrier_semaphore()
    for dt, de in others:
        pl.semaphore_signal(barrier, inc=1, device_id={"tp": peer_tp(dt), "ep": peer_ep(de)}, device_id_type=MESH)
    wq_copy.start()
    for head in range(heads):
        k_in(head).start()
    for head in range(heads):
        v_in(head).start()
    wo_copy.start()
    for slot in range(SLOTS):
        for c in weights_in(slot, slot):
            c.start()
    pl.semaphore_wait(barrier, len(others))

    copies = [tp_exchange(part_ref if i == 0 else mine_ref, other_ref.at[i], tp_send.at[i], tp_recv.at[i]) for i in range(2)]
    copies[0].start()

    idx = idx_ref[...]
    onehot = (lax.broadcasted_iota(jnp.int32, (experts, tokens), 0) == idx).astype(F32)
    earlier = (lax.broadcasted_iota(jnp.int32, (tokens, tokens), 0) < lax.broadcasted_iota(jnp.int32, (tokens, tokens), 1)).astype(F32)
    counts = dot(onehot.astype(BF16), earlier.astype(BF16))
    slot_of = jnp.sum(counts * onehot, axis=0, keepdims=True).astype(jnp.int32)
    row_of = jnp.where(slot_of < capacity, idx * capacity + slot_of, -1)
    place_ref[...] = (lax.broadcasted_iota(jnp.int32, (experts * capacity, tokens), 0) == row_of).astype(F32).astype(BF16)

    copies[0].wait()
    h_float = add_parts(h_ref[...].astype(F32), part_ref[...], other_ref[0])
    x = rms_norm(h_float, scale_ref[1, layer:layer + 1, :])
    mine_ref[...] = cross_part(layer, x, mask_ref[...], wq_copy, wq_ref, wo_copy, wo_ref, k_in, keys, v_in, values, q_t, acc_ref, p_ref, ctx_t)
    copies[1].start()
    copies[1].wait()
    h_float = add_parts(h_float, mine_ref[...], other_ref[1])
    x = rms_norm(h_float, scale_ref[2, layer:layer + 1, :])

    send_x[...] = dot(place_ref[...], x).astype(BF16).reshape(send_x.shape)

    def x_copy(chunk, offset):
        return pltpu.make_async_remote_copy(
            src_ref=send_x.at[peer_ep(offset), chunk], dst_ref=recv_x.at[ep, chunk],
            send_sem=x_send.at[chunk, offset - 1], recv_sem=x_recv.at[chunk, ep],
            device_id={"ep": peer_ep(offset)}, device_id_type=MESH)

    def x_arrival(chunk, offset):
        return pltpu.make_async_remote_copy(
            src_ref=send_x.at[peer_ep(offset), chunk], dst_ref=recv_x.at[peer_ep(offset), chunk],
            send_sem=x_send.at[chunk, offset - 1], recv_sem=x_recv.at[chunk, peer_ep(offset)],
            device_id={"ep": peer_ep(offset)}, device_id_type=MESH)

    for chunk in range(chunks):
        for offset in range(1, groups):
            x_copy(chunk, offset).start()
    recv_x[ep] = send_x[ep]

    router = router_ref[...]
    high = router.astype(BF16)
    rest = router - high.astype(F32)
    mid = rest.astype(BF16)
    low = (rest - mid.astype(F32)).astype(BF16)
    logits = dot_nt(high, x) + (dot_nt(mid, x) + dot_nt(low, x))
    logits_exp = jnp.exp(logits - jnp.max(logits, axis=0, keepdims=True))
    gate = jnp.sum(logits_exp * onehot, axis=0, keepdims=True) / jnp.sum(logits_exp, axis=0, keepdims=True)
    gate_ref[...] = jnp.transpose(jnp.broadcast_to(gate, (tokens, tokens)))

    block = groups * chunk_rows
    r0 = lax.broadcasted_iota(jnp.int32, (block, block), 0)
    r1 = lax.broadcasted_iota(jnp.int32, (block, block), 1)
    group_rows = groups * capacity
    source = ((r0 % group_rows) // capacity) * chunk_rows + (r0 // group_rows) * capacity + r0 % capacity
    to_experts = (r1 == source).astype(F32).astype(BF16)
    back = ((r0 % chunk_rows) // capacity) * group_rows + (r0 // chunk_rows) * capacity + r0 % capacity
    to_groups = (r1 == back).astype(F32).astype(BF16)

    def y_copy(chunk, number):
        dt, de = others[number]
        return pltpu.make_async_remote_copy(
            src_ref=send_y.at[chunk, peer_ep(de)], dst_ref=recv_y.at[tp, ep, chunk],
            send_sem=y_send.at[chunk, number], recv_sem=y_recv.at[chunk, tp, ep],
            device_id={"tp": peer_tp(dt), "ep": peer_ep(de)}, device_id_type=MESH)

    def y_arrival(chunk, number):
        dt, de = others[number]
        return pltpu.make_async_remote_copy(
            src_ref=send_y.at[chunk, peer_ep(de)], dst_ref=recv_y.at[peer_tp(dt), peer_ep(de), chunk],
            send_sem=y_send.at[chunk, number], recv_sem=y_recv.at[chunk, peer_tp(dt), peer_ep(de)],
            device_id={"tp": peer_tp(dt), "ep": peer_ep(de)}, device_id_type=MESH)

    def expert_step(expert, carry):
        slot = lax.rem(expert, SLOTS)
        first_row = pl.multiple_of(lax.rem(expert, per_chunk) * group_rows, group_rows)
        rows = rows_ref[pl.ds(first_row, group_rows), :]
        w_copies = weights_in(expert, slot)
        w_copies[0].wait()
        gate_in = dot(rows, eg_ref[slot])
        w_copies[1].wait()
        lin_in = dot(rows, eu_ref[slot])
        product = (jax.nn.gelu(gate_in) * lin_in).astype(BF16)
        w_copies[2].wait()
        y_ref[pl.ds(first_row, group_rows), :] = dot(product, ed_ref[slot]).astype(BF16)

        @pl.when(expert + SLOTS < local)
        def _():
            for c in weights_in(expert + SLOTS, slot):
                c.start()
        return carry

    def chunk_step(chunk, carry):
        for offset in range(1, groups):
            x_arrival(chunk, offset).wait_recv()
        arrived = recv_x[:, chunk].reshape(block, model)
        rows_ref[...] = dot(to_experts, arrived).astype(BF16)
        lax.fori_loop(chunk * per_chunk, (chunk + 1) * per_chunk, expert_step, 0)
        send_y[chunk] = dot(to_groups, y_ref[...]).astype(BF16).reshape(groups, chunk_rows, model)
        for number in range(len(others)):
            y_copy(chunk, number).start()
        recv_y[tp, ep, chunk] = send_y[chunk, ep]
        return carry

    lax.fori_loop(0, chunks, chunk_step, 0)

    for chunk in range(chunks):
        for number in range(len(others)):
            y_arrival(chunk, number).wait_recv()
    returned = (recv_y[0].astype(F32) + recv_y[1].astype(F32)).astype(BF16).reshape(experts * capacity, model)
    combined = dot_t(place_ref[...], returned)
    gate_col = gate_ref[...]
    for c in range(0, model, tokens):
        delta = gate_col * combined[:, c:c + tokens]
        out_ref[:, c:c + tokens] = (h_float[:, c:c + tokens] + delta).astype(BF16)
    for chunk in range(chunks):
        for offset in range(1, groups):
            x_copy(chunk, offset).wait_send()
        for number in range(len(others)):
            y_copy(chunk, number).wait_send()


def last(layer, h, part, mask, idx, scale, router, w_query, w_out, keys, values, exp_gate, exp_up, exp_down, groups):
    _, heads, slots, head_dim, tokens = keys.shape
    width, model = w_out.shape[1:]
    local, _, ff = exp_gate.shape
    experts = router.shape[0]
    capacity = (2 * tokens + experts - 1) // experts
    chunk_rows = 16
    chunks = local * capacity // chunk_rows
    vmem = pl.BlockSpec(memory_space=pltpu.VMEM)
    hbm = pl.BlockSpec(memory_space=pl.ANY)
    dma = pltpu.SemaphoreType.DMA
    return pl.pallas_call(
        functools.partial(last_kernel, layer),
        out_shape=jax.ShapeDtypeStruct((tokens, model), BF16),
        in_specs=[vmem] * 6 + [hbm] * 7,
        out_specs=vmem,
        scratch_shapes=[
            pltpu.VMEM((model, width), BF16),
            pltpu.VMEM((width, model), BF16),
            pltpu.VMEM((heads, slots, head_dim, tokens), BF16),
            pltpu.VMEM((heads, slots, head_dim, tokens), BF16),
            pltpu.VMEM((SLOTS, model, ff), BF16),
            pltpu.VMEM((SLOTS, model, ff), BF16),
            pltpu.VMEM((SLOTS, ff, model), BF16),
            pltpu.VMEM((heads, head_dim, tokens), F32),
            pltpu.VMEM((heads, slots * 8, tokens), F32),
            pltpu.VMEM((heads, slots, tokens), F32),
            pltpu.VMEM((heads, head_dim, tokens), F32),
            pltpu.VMEM((tokens, model), BF16),
            pltpu.VMEM((2, tokens, model), BF16),
            pltpu.VMEM((experts * capacity, tokens), BF16),
            pltpu.VMEM((groups, chunks, chunk_rows, model), BF16),
            pltpu.VMEM((groups, chunks, chunk_rows, model), BF16),
            pltpu.VMEM((groups * chunk_rows, model), BF16),
            pltpu.VMEM((groups * chunk_rows, model), BF16),
            pltpu.VMEM((chunks, groups, chunk_rows, model), BF16),
            pltpu.VMEM((2, groups, chunks, chunk_rows, model), BF16),
            pltpu.VMEM((tokens, tokens), F32),
            dma((2,)), dma((heads,)), dma((heads,)), dma((SLOTS, 3)), dma((2,)), dma((2,)),
            dma((chunks, groups - 1)), dma((chunks, groups)), dma((chunks, 2 * groups - 1)), dma((chunks, 2, groups)),
        ],
        compiler_params=pltpu.CompilerParams(vmem_limit_bytes=VMEM_LIMIT, collective_id=1, has_side_effects=True),
        name="last",
    )(h, part, mask, idx, scale, router, w_query, w_out, keys, values, exp_gate, exp_up, exp_down)


def decode_body(groups, hidden, write_pos, enc_mask, expert_idx, self_keys, self_values, cross_keys, cross_values, rel_bias, norm_scale, w_query, w_key, w_value, w_out, w_cross_query, w_cross_out, dense_gate, dense_up, dense_down, router, exp_gate, exp_up, exp_down):
    def lanes(cache):
        return jnp.transpose(cache, (0, 2, 3, 4, 1))

    pos = write_pos.reshape(1, -1)
    idx = expert_idx.reshape(1, -1)
    mask = jnp.transpose(enc_mask)
    scale = jnp.transpose(norm_scale, (1, 0, 2))
    keys, values, ckeys, cvalues = map(lanes, (self_keys, self_values, cross_keys, cross_values))
    part, bias, k_out, v_out = self_attention(0, hidden, pos, scale, rel_bias, w_query, w_key, w_value, w_out, keys, values)
    h = middle(0, hidden, part, mask, scale, w_cross_query, w_cross_out, ckeys, cvalues, dense_gate, dense_up, dense_down)
    part, k_out, v_out = self_attention(1, h, pos, scale, bias, w_query, w_key, w_value, w_out, keys, values, (k_out, v_out))
    h = last(1, h, part, mask, idx, scale, jnp.transpose(router), w_cross_query, w_cross_out, ckeys, cvalues, exp_gate, exp_up, exp_down, groups)
    return h, jnp.transpose(k_out, (0, 4, 1, 2, 3)), jnp.transpose(v_out, (0, 4, 1, 2, 3))


def solution(mesh):
    batch = ('dp', 'ep')
    row_spec = P(batch, None)
    vec_spec = P(batch)
    cache_spec = P(None, batch, 'tp', None, None)
    col_spec = P(None, None, 'tp')
    out_rows = P(None, 'tp', None)
    in_specs = (row_spec, vec_spec, row_spec, vec_spec, cache_spec, cache_spec, cache_spec, cache_spec, P('tp', None), P(), col_spec, col_spec, col_spec, out_rows, col_spec, out_rows, P(None, 'tp'), P(None, 'tp'), P('tp', None), P(), P('ep', None, 'tp'), P('ep', None, 'tp'), P('ep', 'tp', None))
    out_specs = (row_spec, cache_spec, cache_spec)
    body = functools.partial(decode_body, mesh.shape['ep'])
    return jax.shard_map(body, mesh=mesh, in_specs=in_specs, out_specs=out_specs, check_vma=False)
```

```python
import functools

import jax
import jax.numpy as jnp
from jax import lax
from jax.experimental import pallas as pl
from jax.experimental.pallas import tpu as pltpu
from jax.sharding import PartitionSpec as P

EPS = 1e-6
NEG_BIG = -1e9
MESH = pl.DeviceIdType.MESH
BF16 = jnp.bfloat16
F32 = jnp.float32
MIB = 1024 * 1024
SLOTS = 6


def rms_norm(h_float, scale):
    inv_rms = lax.rsqrt(jnp.mean(h_float * h_float, axis=-1, keepdims=True) + EPS)
    return (h_float * inv_rms * scale).astype(BF16)


def dot(a, b):
    return jnp.dot(a, b, preferred_element_type=F32)


def dot_t(a, b):
    return lax.dot_general(a, b, (((0,), (0,)), ((), ())), preferred_element_type=F32)


def dot_nt(a, b):
    return lax.dot_general(a, b, (((1,), (1,)), ((), ())), preferred_element_type=F32)


def fold_rows(prod):
    parts = [prod[i * 8:(i + 1) * 8] for i in range(prod.shape[0] // 8)]
    while len(parts) > 1:
        parts = [a + b for a, b in zip(parts[::2], parts[1::2])]
    return parts[0]


def score_head(q_head, keys, head, acc_ref, merge=None):
    for slot in range(keys.shape[1]):
        k_slot = keys[head, slot]
        if merge is not None:
            pos_b, k_new, merged = merge
            k_slot = jnp.where(pos_b == jnp.asarray(slot, BF16), k_new, k_slot)
            merged[head, slot] = k_slot
        acc_ref[head, slot * 8:(slot + 1) * 8, :] = fold_rows(k_slot.astype(F32) * q_head)


def gather_scores(acc_ref, head, slots):
    total = acc_ref[head, pl.ds(0, slots, stride=8), :]
    for i in range(1, 8):
        total = total + acc_ref[head, pl.ds(i, slots, stride=8), :]
    return total


def softmax_rows(scores):
    top = jnp.max(scores, axis=0, keepdims=True)
    e = jnp.exp(scores - top)
    return (e / jnp.sum(e, axis=0, keepdims=True)).astype(BF16).astype(F32)


def context_head(p_ref, values, head, merge=None):
    total = None
    for slot in range(values.shape[1]):
        v_slot = values[head, slot]
        if merge is not None:
            pos_b, v_new, merged = merge
            v_slot = jnp.where(pos_b == jnp.asarray(slot, BF16), v_new, v_slot)
            merged[head, slot] = v_slot
        term = v_slot.astype(F32) * p_ref[head, slot:slot + 1, :]
        total = term if total is None else total + term
    return total


def pinned(x):
    return pltpu.with_memory_space_constraint(x, pltpu.HBM)


def first_kernel(layer, h_hbm, pos_hbm, scale_hbm, rel_hbm, wq_hbm, wk_hbm, wv_hbm, wo_hbm, k_hbm, v_hbm,
                 part_ref, bias_ref, ko_hbm, vo_hbm,
                 h_ref, pos_ref, scale_ref, rel_ref, w_in, wo_ref, keys, values, q_t, k_t, v_t, acc_ref, p_ref, ctx_t,
                 s_sem, w_sem, k_sem, v_sem, ko_sem, vo_sem):
    heads = keys.shape[0]
    small = [pltpu.make_async_copy(s, d, s_sem.at[i]) for i, (s, d) in enumerate(
        ((h_hbm, h_ref), (scale_hbm, scale_ref), (pos_hbm, pos_ref), (rel_hbm, rel_ref)))]
    w_copies = [pltpu.make_async_copy(w.at[layer], w_in.at[i], w_sem.at[i]) for i, w in enumerate((wq_hbm, wk_hbm, wv_hbm))]
    wo_copy = pltpu.make_async_copy(wo_hbm.at[layer], wo_ref, w_sem.at[3])

    def k_in(head):
        return pltpu.make_async_copy(k_hbm.at[layer, head], keys.at[head], k_sem.at[head])

    def v_in(head):
        return pltpu.make_async_copy(v_hbm.at[layer, head], values.at[head], v_sem.at[head])

    for c in small + w_copies:
        c.start()
    for head in range(heads):
        k_in(head).start()
    for head in range(heads):
        v_in(head).start(priority=1)
    wo_copy.start(priority=1)

    slots, tokens = bias_ref.shape[1:]
    small[2].wait()
    small[3].wait()
    dist = pos_ref[...] - lax.broadcasted_iota(jnp.int32, (slots, tokens), 0)
    bias = [jnp.zeros((slots, tokens), F32)] * heads
    for d in range(slots):
        hit = dist == d
        bias = [jnp.where(hit, rel_ref[head, d], b) for head, b in enumerate(bias)]
    for head in range(heads):
        bias_ref[head] = bias[head]
    small[0].wait()
    small[1].wait()

    self_part(layer, h_ref, pos_ref, scale_ref, bias_ref, w_in, [c.wait for c in w_copies], wo_ref, wo_copy.wait,
              keys, values, lambda head: k_in(head).wait(), lambda head: v_in(head).wait(), keys, values,
              part_ref, ko_hbm, vo_hbm, q_t, k_t, v_t, acc_ref, p_ref, ctx_t, ko_sem, vo_sem)


def second_kernel(layer, h_ref, pos_ref, scale_ref, bias_ref, w_in, wo_ref, keys_in, values_in, _, __,
                  part_ref, ko_hbm, vo_hbm,
                  keys, values, q_t, k_t, v_t, acc_ref, p_ref, ctx_t, ko_sem, vo_sem):
    self_part(layer, h_ref, pos_ref, scale_ref, bias_ref, w_in, [None] * 3, wo_ref, None,
              keys_in, values_in, None, None, keys, values,
              part_ref, ko_hbm, vo_hbm, q_t, k_t, v_t, acc_ref, p_ref, ctx_t, ko_sem, vo_sem)


def self_part(layer, h_ref, pos_ref, scale_ref, bias_ref, w_in, w_waits, wo_ref, wo_wait,
              keys_in, values_in, k_wait, v_wait, keys, values,
              part_ref, ko_hbm, vo_hbm, q_t, k_t, v_t, acc_ref, p_ref, ctx_t, ko_sem, vo_sem):
    heads, slots, head_dim, tokens = keys.shape

    def k_out(head):
        return pltpu.make_async_copy(keys.at[head], ko_hbm.at[layer, head], ko_sem.at[head])

    def v_out(head):
        return pltpu.make_async_copy(values.at[head], vo_hbm.at[layer, head], vo_sem.at[head])

    x = rms_norm(h_ref[...].astype(F32), scale_ref[0, layer:layer + 1, :])
    pos = pos_ref[...]
    valid = pos >= lax.broadcasted_iota(jnp.int32, (slots, tokens), 0)
    pos_b = jnp.broadcast_to(pos.astype(F32), (head_dim, tokens)).astype(BF16)

    for i, target in enumerate((q_t, k_t, v_t)):
        if w_waits[i] is not None:
            w_waits[i]()
        proj = dot(x, w_in[i]).astype(BF16).astype(F32)
        target[...] = jnp.transpose(proj).reshape(target.shape).astype(target.dtype)

    def score_step(head, carry):
        if k_wait is not None:
            k_wait(head)
        score_head(q_t[head], keys_in, head, acc_ref, (pos_b, k_t[head], keys))
        k_out(head).start()
        return carry

    lax.fori_loop(0, heads, score_step, 0)
    for head in range(heads):
        scores = jnp.where(valid, gather_scores(acc_ref, head, slots) + bias_ref[head], NEG_BIG)
        p_ref[head] = softmax_rows(scores)

    def context_step(head, carry):
        if v_wait is not None:
            v_wait(head)
        ctx_t[head] = context_head(p_ref, values_in, head, (pos_b, v_t[head], values))
        v_out(head).start()
        return carry

    lax.fori_loop(0, heads, context_step, 0)
    ctx = jnp.transpose(ctx_t[...].reshape(heads * head_dim, tokens)).astype(BF16)
    if wo_wait is not None:
        wo_wait()
    part_ref[...] = dot(ctx, wo_ref[...]).astype(BF16)
    for head in range(heads):
        k_out(head).wait()
        v_out(head).wait()


def attention_scratch(heads, slots, head_dim, tokens):
    return [
        pltpu.VMEM((heads, slots, head_dim, tokens), BF16),
        pltpu.VMEM((heads, slots, head_dim, tokens), BF16),
        pltpu.VMEM((heads, head_dim, tokens), F32),
        pltpu.VMEM((heads, head_dim, tokens), BF16),
        pltpu.VMEM((heads, head_dim, tokens), BF16),
        pltpu.VMEM((heads, slots * 8, tokens), F32),
        pltpu.VMEM((heads, slots, tokens), F32),
        pltpu.VMEM((heads, head_dim, tokens), F32),
    ]


def self_first(layer, h, pos, scale, rel, w_query, w_key, w_value, w_out, keys, values):
    _, heads, slots, head_dim, tokens = keys.shape
    width, model = w_out.shape[1:]
    vmem = pl.BlockSpec(memory_space=pltpu.VMEM)
    hbm = pl.BlockSpec(memory_space=pltpu.HBM)
    dma = pltpu.SemaphoreType.DMA
    ins = [pinned(x) for x in (h, pos, scale, rel, w_query, w_key, w_value, w_out, keys, values)]
    cache = pltpu.HBM(keys.shape, keys.dtype)
    return pl.pallas_call(
        functools.partial(first_kernel, layer),
        out_shape=[pltpu.VMEM((tokens, model), BF16), pltpu.VMEM((heads, slots, tokens), F32), cache, cache],
        in_specs=[hbm] * 10,
        out_specs=[vmem, vmem, hbm, hbm],
        scratch_shapes=[
            pltpu.VMEM((tokens, model), BF16),
            pltpu.VMEM(pos.shape, pos.dtype),
            pltpu.VMEM(scale.shape, F32),
            pltpu.SMEM(rel.shape, F32),
            pltpu.VMEM((3, model, width), BF16),
            pltpu.VMEM((width, model), BF16),
        ] + attention_scratch(heads, slots, head_dim, tokens) + [
            dma((4,)), dma((4,)), dma((heads,)), dma((heads,)), dma((heads,)), dma((heads,)),
        ],
        compiler_params=pltpu.CompilerParams(vmem_limit_bytes=20 * MIB),
        name="self_first",
    )(*ins)


def self_second(layer, h, pos, scale, bias, w_in, w_out, keys_in, values_in, k_out, v_out):
    heads, slots, head_dim, tokens = keys_in.shape
    vmem = pl.BlockSpec(memory_space=pltpu.VMEM)
    hbm = pl.BlockSpec(memory_space=pltpu.HBM)
    dma = pltpu.SemaphoreType.DMA
    cache = pltpu.HBM(k_out.shape, k_out.dtype)
    return pl.pallas_call(
        functools.partial(second_kernel, layer),
        out_shape=[pltpu.VMEM(h.shape, BF16), cache, cache],
        in_specs=[vmem] * 8 + [hbm] * 2,
        out_specs=[vmem, hbm, hbm],
        input_output_aliases={8: 1, 9: 2},
        scratch_shapes=attention_scratch(heads, slots, head_dim, tokens) + [dma((heads,)), dma((heads,))],
        compiler_params=pltpu.CompilerParams(vmem_limit_bytes=20 * MIB),
        name="self_second",
    )(h, pos, scale, bias, w_in, w_out, keys_in, values_in, pinned(k_out), pinned(v_out))


def tp_exchange(src, dst, send_sem, recv_sem):
    return pltpu.make_async_remote_copy(
        src_ref=src, dst_ref=dst, send_sem=send_sem, recv_sem=recv_sem,
        device_id={"tp": 1 - lax.axis_index("tp")}, device_id_type=MESH)


def add_parts(h_float, mine, other):
    delta = (mine.astype(F32) + other.astype(F32)).astype(BF16)
    return (h_float + delta.astype(F32)).astype(BF16).astype(F32)


def cross_part(layer, x, mask, wq_copy, wq_ref, wo_copy, wo_ref, k_in, keys, v_in, values, q_t, acc_ref, p_ref, ctx_t):
    heads, slots, head_dim, tokens = keys.shape
    wq_copy.wait()
    proj = dot(x, wq_ref[...]).astype(BF16).astype(F32)
    q_t[...] = jnp.transpose(proj).reshape(heads, head_dim, tokens)

    def score_step(head, carry):
        k_in(head).wait()
        score_head(q_t[head], keys, head, acc_ref)
        return carry

    lax.fori_loop(0, heads, score_step, 0)
    valid = mask > 0
    for head in range(heads):
        p_ref[head] = softmax_rows(jnp.where(valid, gather_scores(acc_ref, head, slots), NEG_BIG))

    def context_step(head, carry):
        v_in(head).wait()
        ctx_t[head] = context_head(p_ref, values, head)
        return carry

    lax.fori_loop(0, heads, context_step, 0)
    ctx = jnp.transpose(ctx_t[...].reshape(heads * head_dim, tokens)).astype(BF16)
    wo_copy.wait()
    return dot(ctx, wo_ref[...]).astype(BF16)


def middle_kernel(layer, part_ref, h_hbm, mask_hbm, scale_hbm, pos_hbm, wq_hbm, wo_hbm, k_hbm, v_hbm, dg_hbm, du_hbm, dd_hbm,
                  nq_hbm, nk_hbm, nv_hbm, no_hbm, nkeys_hbm, nvalues_hbm,
                  out_ref, pos_ref, scale_ref, nw_ref, nwo_ref, nkeys_ref, nvalues_ref,
                  h_ref, mask_ref, wq_ref, wo_ref, keys, values, dg_ref, du_ref, dd_ref, q_t, acc_ref, p_ref, ctx_t, mine_ref, other_ref, prod_ref,
                  w_sem, k_sem, v_sem, send_sem, recv_sem, s_sem, n_sem):
    heads = keys.shape[0]
    small = [pltpu.make_async_copy(s, d, s_sem.at[i]) for i, (s, d) in enumerate(
        ((h_hbm, h_ref), (mask_hbm, mask_ref), (scale_hbm, scale_ref), (pos_hbm, pos_ref)))]
    following = [pltpu.make_async_copy(s, d, n_sem.at[i]) for i, (s, d) in enumerate(
        ((nq_hbm.at[layer + 1], nw_ref.at[0]), (nk_hbm.at[layer + 1], nw_ref.at[1]), (nv_hbm.at[layer + 1], nw_ref.at[2]),
         (no_hbm.at[layer + 1], nwo_ref), (nkeys_hbm.at[layer + 1], nkeys_ref), (nvalues_hbm.at[layer + 1], nvalues_ref)))]

    def k_in(head):
        return pltpu.make_async_copy(k_hbm.at[layer, head], keys.at[head], k_sem.at[head])

    def v_in(head):
        return pltpu.make_async_copy(v_hbm.at[layer, head], values.at[head], v_sem.at[head])

    wq_copy = pltpu.make_async_copy(wq_hbm.at[layer], wq_ref, w_sem.at[0])
    wo_copy = pltpu.make_async_copy(wo_hbm.at[layer], wo_ref, w_sem.at[1])
    dense = [pltpu.make_async_copy(s, d, w_sem.at[2 + i]) for i, (s, d) in enumerate(((dg_hbm, dg_ref), (du_hbm, du_ref), (dd_hbm, dd_ref)))]

    barrier = pltpu.get_barrier_semaphore()
    pl.semaphore_signal(barrier, inc=1, device_id={"tp": 1 - lax.axis_index("tp")}, device_id_type=MESH)
    for c in small:
        c.start()
    wq_copy.start()
    for head in range(heads):
        k_in(head).start()
    for head in range(heads):
        v_in(head).start(priority=1)
    wo_copy.start(priority=1)
    for c in dense + following:
        c.start(priority=1)
    pl.semaphore_wait(barrier, 1)

    copies = [tp_exchange(part_ref if i == 0 else mine_ref.at[i - 1], other_ref.at[i], send_sem.at[i], recv_sem.at[i]) for i in range(3)]
    copies[0].start()
    for c in small:
        c.wait()
    copies[0].wait()
    h_float = add_parts(h_ref[...].astype(F32), part_ref[...], other_ref[0])

    x = rms_norm(h_float, scale_ref[1, layer:layer + 1, :])
    mine_ref[0] = cross_part(layer, x, mask_ref[...], wq_copy, wq_ref, wo_copy, wo_ref, k_in, keys, v_in, values, q_t, acc_ref, p_ref, ctx_t)
    copies[1].start()
    copies[1].wait()
    h_float = add_parts(h_float, mine_ref[0], other_ref[1])

    x = rms_norm(h_float, scale_ref[2, layer:layer + 1, :])
    dense[0].wait()
    dense[1].wait()
    width = dg_ref.shape[1]
    step = 512
    for c in range(0, width, step):
        gate_in = dot(x, dg_ref[:, c:c + step])
        lin_in = dot(x, du_ref[:, c:c + step])
        prod_ref[:, c:c + step] = (jax.nn.gelu(gate_in) * lin_in).astype(BF16)
    dense[2].wait()
    mine_ref[1] = dot(prod_ref[...], dd_ref[...]).astype(BF16)
    copies[2].start()
    copies[2].wait()
    out_ref[...] = add_parts(h_float, mine_ref[1], other_ref[2]).astype(BF16)
    for c in following:
        c.wait()


def middle(layer, part, h, mask, scale, pos, w_query, w_out, keys, values, dense_gate, dense_up, dense_down, following):
    _, heads, slots, head_dim, tokens = keys.shape
    width, model = w_out.shape[1:]
    ff = dense_gate.shape[1]
    vmem = pl.BlockSpec(memory_space=pltpu.VMEM)
    hbm = pl.BlockSpec(memory_space=pltpu.HBM)
    dma = pltpu.SemaphoreType.DMA
    cache = pltpu.VMEM((heads, slots, head_dim, tokens), BF16)
    return pl.pallas_call(
        functools.partial(middle_kernel, layer),
        out_shape=[
            pltpu.VMEM((tokens, model), BF16), pltpu.VMEM(pos.shape, pos.dtype), pltpu.VMEM(scale.shape, F32),
            pltpu.VMEM((3, model, width), BF16), pltpu.VMEM((width, model), BF16), cache, cache,
        ],
        in_specs=[vmem] + [hbm] * 17,
        out_specs=[vmem] * 7,
        scratch_shapes=[
            pltpu.VMEM((tokens, model), BF16),
            pltpu.VMEM(mask.shape, mask.dtype),
            pltpu.VMEM((model, width), BF16),
            pltpu.VMEM((width, model), BF16),
            pltpu.VMEM((heads, slots, head_dim, tokens), BF16),
            pltpu.VMEM((heads, slots, head_dim, tokens), BF16),
            pltpu.VMEM((model, ff), BF16),
            pltpu.VMEM((model, ff), BF16),
            pltpu.VMEM((ff, model), BF16),
            pltpu.VMEM((heads, head_dim, tokens), F32),
            pltpu.VMEM((heads, slots * 8, tokens), F32),
            pltpu.VMEM((heads, slots, tokens), F32),
            pltpu.VMEM((heads, head_dim, tokens), F32),
            pltpu.VMEM((2, tokens, model), BF16),
            pltpu.VMEM((3, tokens, model), BF16),
            pltpu.VMEM((tokens, ff), BF16),
            dma((5,)), dma((heads,)), dma((heads,)), dma((3,)), dma((3,)), dma((4,)), dma((6,)),
        ],
        compiler_params=pltpu.CompilerParams(vmem_limit_bytes=26 * MIB, collective_id=0, has_side_effects=True),
        name="middle",
    )(part, *map(pinned, (h, mask, scale, pos, w_query, w_out, keys, values, dense_gate, dense_up, dense_down) + following))


def last_kernel(layer, h_ref, part_ref, mask_hbm, idx_hbm, scale_hbm, router_hbm, wq_hbm, wo_hbm, k_hbm, v_hbm, eg_hbm, eu_hbm, ed_hbm,
                out_ref,
                mask_ref, idx_ref, scale_ref, router_ref, wq_ref, wo_ref, keys, values, eg_ref, eu_ref, ed_ref, q_t, acc_ref, p_ref, ctx_t, mine_ref, other_ref,
                place_ref, send_x, recv_x, rows_ref, y_ref, send_y, recv_y, gate_ref,
                w_sem, k_sem, v_sem, e_sem, tp_send, tp_recv, x_send, x_recv, y_send, y_recv, s_sem):
    heads = keys.shape[0]
    tokens, model = h_ref.shape
    experts = router_ref.shape[0]
    small = [pltpu.make_async_copy(s, d, s_sem.at[i]) for i, (s, d) in enumerate(
        ((mask_hbm, mask_ref), (idx_hbm, idx_ref), (scale_hbm, scale_ref), (router_hbm, router_ref)))]
    groups, chunks, chunk_rows, _ = recv_x.shape
    local = experts // groups
    capacity = place_ref.shape[0] // experts
    per_chunk = local // chunks
    tp = lax.axis_index("tp")
    ep = lax.axis_index("ep")

    def peer_ep(offset):
        return lax.rem(ep + offset, groups)

    def peer_tp(offset):
        return lax.rem(tp + offset, 2)

    def k_in(head):
        return pltpu.make_async_copy(k_hbm.at[layer, head], keys.at[head], k_sem.at[head])

    def v_in(head):
        return pltpu.make_async_copy(v_hbm.at[layer, head], values.at[head], v_sem.at[head])

    def weights_in(expert, slot):
        return [pltpu.make_async_copy(s.at[expert], d.at[slot], e_sem.at[slot, i])
                for i, (s, d) in enumerate(((eg_hbm, eg_ref), (eu_hbm, eu_ref), (ed_hbm, ed_ref)))]

    wq_copy = pltpu.make_async_copy(wq_hbm.at[layer], wq_ref, w_sem.at[0])
    wo_copy = pltpu.make_async_copy(wo_hbm.at[layer], wo_ref, w_sem.at[1])

    others = [(dt, de) for dt in range(2) for de in range(groups) if dt or de]
    barrier = pltpu.get_barrier_semaphore()
    for dt, de in others:
        pl.semaphore_signal(barrier, inc=1, device_id={"tp": peer_tp(dt), "ep": peer_ep(de)}, device_id_type=MESH)
    for c in small:
        c.start()
    wq_copy.start()
    for head in range(heads):
        k_in(head).start()
    for head in range(heads):
        v_in(head).start()
    wo_copy.start()
    for slot in range(SLOTS):
        for c in weights_in(slot, slot):
            c.start(priority=1)
    pl.semaphore_wait(barrier, len(others))

    copies = [tp_exchange(part_ref if i == 0 else mine_ref, other_ref.at[i], tp_send.at[i], tp_recv.at[i]) for i in range(2)]
    copies[0].start()

    for c in small:
        c.wait()
    idx = idx_ref[...]
    onehot = (lax.broadcasted_iota(jnp.int32, (experts, tokens), 0) == idx).astype(F32)
    earlier = (lax.broadcasted_iota(jnp.int32, (tokens, tokens), 0) < lax.broadcasted_iota(jnp.int32, (tokens, tokens), 1)).astype(F32)
    counts = dot(onehot.astype(BF16), earlier.astype(BF16))
    slot_of = jnp.sum(counts * onehot, axis=0, keepdims=True).astype(jnp.int32)
    row_of = jnp.where(slot_of < capacity, idx * capacity + slot_of, -1)
    place_ref[...] = (lax.broadcasted_iota(jnp.int32, (experts * capacity, tokens), 0) == row_of).astype(F32).astype(BF16)

    copies[0].wait()
    h_float = add_parts(h_ref[...].astype(F32), part_ref[...], other_ref[0])
    x = rms_norm(h_float, scale_ref[1, layer:layer + 1, :])
    mine_ref[...] = cross_part(layer, x, mask_ref[...], wq_copy, wq_ref, wo_copy, wo_ref, k_in, keys, v_in, values, q_t, acc_ref, p_ref, ctx_t)
    copies[1].start()
    copies[1].wait()
    h_float = add_parts(h_float, mine_ref[...], other_ref[1])
    x = rms_norm(h_float, scale_ref[2, layer:layer + 1, :])

    send_x[...] = dot(place_ref[...], x).astype(BF16).reshape(send_x.shape)

    def x_copy(chunk, offset):
        return pltpu.make_async_remote_copy(
            src_ref=send_x.at[peer_ep(offset), chunk], dst_ref=recv_x.at[ep, chunk],
            send_sem=x_send.at[chunk, offset - 1], recv_sem=x_recv.at[chunk, ep],
            device_id={"ep": peer_ep(offset)}, device_id_type=MESH)

    def x_arrival(chunk, offset):
        return pltpu.make_async_remote_copy(
            src_ref=send_x.at[peer_ep(offset), chunk], dst_ref=recv_x.at[peer_ep(offset), chunk],
            send_sem=x_send.at[chunk, offset - 1], recv_sem=x_recv.at[chunk, peer_ep(offset)],
            device_id={"ep": peer_ep(offset)}, device_id_type=MESH)

    for chunk in range(chunks):
        for offset in range(1, groups):
            x_copy(chunk, offset).start()
    recv_x[ep] = send_x[ep]

    router = router_ref[...]
    high = router.astype(BF16)
    rest = router - high.astype(F32)
    mid = rest.astype(BF16)
    low = (rest - mid.astype(F32)).astype(BF16)
    logits = dot_nt(high, x) + (dot_nt(mid, x) + dot_nt(low, x))
    logits_exp = jnp.exp(logits - jnp.max(logits, axis=0, keepdims=True))
    gate = jnp.sum(logits_exp * onehot, axis=0, keepdims=True) / jnp.sum(logits_exp, axis=0, keepdims=True)
    gate_ref[...] = jnp.transpose(jnp.broadcast_to(gate, (tokens, tokens)))

    block = groups * chunk_rows
    r0 = lax.broadcasted_iota(jnp.int32, (block, block), 0)
    r1 = lax.broadcasted_iota(jnp.int32, (block, block), 1)
    group_rows = groups * capacity
    source = ((r0 % group_rows) // capacity) * chunk_rows + (r0 // group_rows) * capacity + r0 % capacity
    to_experts = (r1 == source).astype(F32).astype(BF16)
    back = ((r0 % chunk_rows) // capacity) * group_rows + (r0 // chunk_rows) * capacity + r0 % capacity
    to_groups = (r1 == back).astype(F32).astype(BF16)

    def y_copy(chunk, number):
        dt, de = others[number]
        return pltpu.make_async_remote_copy(
            src_ref=send_y.at[chunk, peer_ep(de)], dst_ref=recv_y.at[tp, ep, chunk],
            send_sem=y_send.at[chunk, number], recv_sem=y_recv.at[chunk, tp, ep],
            device_id={"tp": peer_tp(dt), "ep": peer_ep(de)}, device_id_type=MESH)

    def y_arrival(chunk, number):
        dt, de = others[number]
        return pltpu.make_async_remote_copy(
            src_ref=send_y.at[chunk, peer_ep(de)], dst_ref=recv_y.at[peer_tp(dt), peer_ep(de), chunk],
            send_sem=y_send.at[chunk, number], recv_sem=y_recv.at[chunk, peer_tp(dt), peer_ep(de)],
            device_id={"tp": peer_tp(dt), "ep": peer_ep(de)}, device_id_type=MESH)

    def expert_step(expert, carry):
        slot = lax.rem(expert, SLOTS)
        first_row = pl.multiple_of(lax.rem(expert, per_chunk) * group_rows, group_rows)
        rows = rows_ref[pl.ds(first_row, group_rows), :]
        w_copies = weights_in(expert, slot)
        w_copies[0].wait()
        gate_in = dot(rows, eg_ref[slot])
        w_copies[1].wait()
        lin_in = dot(rows, eu_ref[slot])
        product = (jax.nn.gelu(gate_in) * lin_in).astype(BF16)
        w_copies[2].wait()
        y_ref[pl.ds(first_row, group_rows), :] = dot(product, ed_ref[slot]).astype(BF16)

        @pl.when(expert + SLOTS < local)
        def _():
            for c in weights_in(expert + SLOTS, slot):
                c.start(priority=1)
        return carry

    def chunk_step(chunk, carry):
        for offset in range(1, groups):
            x_arrival(chunk, offset).wait_recv()
        arrived = recv_x[:, chunk].reshape(block, model)
        rows_ref[...] = dot(to_experts, arrived).astype(BF16)
        lax.fori_loop(chunk * per_chunk, (chunk + 1) * per_chunk, expert_step, 0)
        send_y[chunk] = dot(to_groups, y_ref[...]).astype(BF16).reshape(groups, chunk_rows, model)
        for number in range(len(others)):
            y_copy(chunk, number).start()
        recv_y[tp, ep, chunk] = send_y[chunk, ep]
        return carry

    lax.fori_loop(0, chunks, chunk_step, 0)

    for chunk in range(chunks):
        for number in range(len(others)):
            y_arrival(chunk, number).wait_recv()
    returned = (recv_y[0].astype(F32) + recv_y[1].astype(F32)).astype(BF16).reshape(experts * capacity, model)
    combined = dot_t(place_ref[...], returned)
    gate_col = gate_ref[...]
    for c in range(0, model, tokens):
        delta = gate_col * combined[:, c:c + tokens]
        out_ref[:, c:c + tokens] = (h_float[:, c:c + tokens] + delta).astype(BF16)
    for chunk in range(chunks):
        for offset in range(1, groups):
            x_copy(chunk, offset).wait_send()
        for number in range(len(others)):
            y_copy(chunk, number).wait_send()


def last(layer, h, part, mask, idx, scale, router, w_query, w_out, keys, values, exp_gate, exp_up, exp_down, groups):
    _, heads, slots, head_dim, tokens = keys.shape
    width, model = w_out.shape[1:]
    local, _, ff = exp_gate.shape
    experts = router.shape[0]
    capacity = (2 * tokens + experts - 1) // experts
    chunk_rows = 16
    chunks = local * capacity // chunk_rows
    vmem = pl.BlockSpec(memory_space=pltpu.VMEM)
    hbm = pl.BlockSpec(memory_space=pltpu.HBM)
    dma = pltpu.SemaphoreType.DMA
    return pl.pallas_call(
        functools.partial(last_kernel, layer),
        out_shape=pltpu.VMEM((tokens, model), BF16),
        in_specs=[vmem] * 2 + [hbm] * 11,
        out_specs=vmem,
        scratch_shapes=[
            pltpu.VMEM(mask.shape, mask.dtype),
            pltpu.VMEM(idx.shape, idx.dtype),
            pltpu.VMEM(scale.shape, F32),
            pltpu.VMEM(router.shape, F32),
            pltpu.VMEM((model, width), BF16),
            pltpu.VMEM((width, model), BF16),
            pltpu.VMEM((heads, slots, head_dim, tokens), BF16),
            pltpu.VMEM((heads, slots, head_dim, tokens), BF16),
            pltpu.VMEM((SLOTS, model, ff), BF16),
            pltpu.VMEM((SLOTS, model, ff), BF16),
            pltpu.VMEM((SLOTS, ff, model), BF16),
            pltpu.VMEM((heads, head_dim, tokens), F32),
            pltpu.VMEM((heads, slots * 8, tokens), F32),
            pltpu.VMEM((heads, slots, tokens), F32),
            pltpu.VMEM((heads, head_dim, tokens), F32),
            pltpu.VMEM((tokens, model), BF16),
            pltpu.VMEM((2, tokens, model), BF16),
            pltpu.VMEM((experts * capacity, tokens), BF16),
            pltpu.VMEM((groups, chunks, chunk_rows, model), BF16),
            pltpu.VMEM((groups, chunks, chunk_rows, model), BF16),
            pltpu.VMEM((groups * chunk_rows, model), BF16),
            pltpu.VMEM((groups * chunk_rows, model), BF16),
            pltpu.VMEM((chunks, groups, chunk_rows, model), BF16),
            pltpu.VMEM((2, groups, chunks, chunk_rows, model), BF16),
            pltpu.VMEM((tokens, tokens), F32),
            dma((2,)), dma((heads,)), dma((heads,)), dma((SLOTS, 3)), dma((2,)), dma((2,)),
            dma((chunks, groups - 1)), dma((chunks, groups)), dma((chunks, 2 * groups - 1)), dma((chunks, 2, groups)), dma((4,)),
        ],
        compiler_params=pltpu.CompilerParams(vmem_limit_bytes=58 * MIB, collective_id=1, has_side_effects=True),
        name="last",
    )(pltpu.with_memory_space_constraint(h, pltpu.VMEM), pltpu.with_memory_space_constraint(part, pltpu.VMEM), *map(pinned, (mask, idx, scale, router, w_query, w_out, keys, values, exp_gate, exp_up, exp_down)))


def decode_body(groups, hidden, write_pos, enc_mask, expert_idx, self_keys, self_values, cross_keys, cross_values, rel_bias, norm_scale, w_query, w_key, w_value, w_out, w_cross_query, w_cross_out, dense_gate, dense_up, dense_down, router, exp_gate, exp_up, exp_down):
    def lanes(cache):
        return jnp.transpose(cache, (0, 2, 3, 4, 1))

    pos = write_pos.reshape(1, -1)
    idx = expert_idx.reshape(1, -1)
    mask = jnp.transpose(enc_mask)
    scale = jnp.transpose(norm_scale, (1, 0, 2))
    keys, values, ckeys, cvalues = map(lanes, (self_keys, self_values, cross_keys, cross_values))
    part, bias, k_out, v_out = self_first(0, hidden, pos, scale, rel_bias, w_query, w_key, w_value, w_out, keys, values)
    following = (w_query, w_key, w_value, w_out, keys, values)
    h, pos, scale_in, w_in, w_o, keys, values = middle(0, part, hidden, mask, scale, pos, w_cross_query, w_cross_out, ckeys, cvalues, dense_gate, dense_up, dense_down, following)
    part, k_out, v_out = self_second(1, h, pos, scale_in, bias, w_in, w_o, keys, values, k_out, v_out)
    h = last(1, h, part, mask, idx, scale, jnp.transpose(router), w_cross_query, w_cross_out, ckeys, cvalues, exp_gate, exp_up, exp_down, groups)
    return h, jnp.transpose(k_out, (0, 4, 1, 2, 3)), jnp.transpose(v_out, (0, 4, 1, 2, 3))


def solution(mesh):
    batch = ('dp', 'ep')
    row_spec = P(batch, None)
    vec_spec = P(batch)
    cache_spec = P(None, batch, 'tp', None, None)
    col_spec = P(None, None, 'tp')
    out_rows = P(None, 'tp', None)
    in_specs = (row_spec, vec_spec, row_spec, vec_spec, cache_spec, cache_spec, cache_spec, cache_spec, P('tp', None), P(), col_spec, col_spec, col_spec, out_rows, col_spec, out_rows, P(None, 'tp'), P(None, 'tp'), P('tp', None), P(), P('ep', None, 'tp'), P('ep', None, 'tp'), P('ep', 'tp', None))
    out_specs = (row_spec, cache_spec, cache_spec)
    body = functools.partial(decode_body, mesh.shape['ep'])
    return jax.shard_map(body, mesh=mesh, in_specs=in_specs, out_specs=out_specs, check_vma=False)
```

```python
import functools

import jax
import jax.numpy as jnp
from jax import lax
from jax.experimental import pallas as pl
from jax.experimental.pallas import tpu as pltpu
from jax.sharding import PartitionSpec as P

EPS = 1e-6
NEG_BIG = -1e9
MESH = pl.DeviceIdType.MESH
BF16 = jnp.bfloat16
F32 = jnp.float32
MIB = 1024 * 1024
GATE_SLOTS = 7
DOWN_SLOTS = 7
LAST_VMEM = 62 * MIB


def rms_norm(h_float, scale):
    inv_rms = lax.rsqrt(jnp.mean(h_float * h_float, axis=-1, keepdims=True) + EPS)
    return (h_float * inv_rms * scale).astype(BF16)


def dot(a, b):
    return jnp.dot(a, b, preferred_element_type=F32)


def dot_t(a, b):
    return lax.dot_general(a, b, (((0,), (0,)), ((), ())), preferred_element_type=F32)


def dot_nt(a, b):
    return lax.dot_general(a, b, (((1,), (1,)), ((), ())), preferred_element_type=F32)


def fold_rows(prod):
    parts = [prod[i * 8:(i + 1) * 8] for i in range(prod.shape[0] // 8)]
    while len(parts) > 1:
        parts = [a + b for a, b in zip(parts[::2], parts[1::2])]
    return parts[0]


def score_head(q_head, keys, head, acc_ref, merge=None):
    for slot in range(keys.shape[1]):
        k_slot = keys[head, slot]
        if merge is not None:
            pos_b, k_new, merged = merge
            k_slot = jnp.where(pos_b == jnp.asarray(slot, BF16), k_new, k_slot)
            merged[head, slot] = k_slot
        acc_ref[head, slot * 8:(slot + 1) * 8, :] = fold_rows(k_slot.astype(F32) * q_head)


def gather_scores(acc_ref, head, slots):
    total = acc_ref[head, pl.ds(0, slots, stride=8), :]
    for i in range(1, 8):
        total = total + acc_ref[head, pl.ds(i, slots, stride=8), :]
    return total


def softmax_rows(scores):
    top = jnp.max(scores, axis=0, keepdims=True)
    e = jnp.exp(scores - top)
    return (e / jnp.sum(e, axis=0, keepdims=True)).astype(BF16).astype(F32)


def context_head(p_ref, values, head, merge=None):
    total = None
    for slot in range(values.shape[1]):
        v_slot = values[head, slot]
        if merge is not None:
            pos_b, v_new, merged = merge
            v_slot = jnp.where(pos_b == jnp.asarray(slot, BF16), v_new, v_slot)
            merged[head, slot] = v_slot
        term = v_slot.astype(F32) * p_ref[head, slot:slot + 1, :]
        total = term if total is None else total + term
    return total


def pinned(x):
    return pltpu.with_memory_space_constraint(x, pltpu.HBM)


def first_kernel(layer, h_hbm, pos_hbm, scale_hbm, rel_hbm, wq_hbm, wk_hbm, wv_hbm, wo_hbm, k_hbm, v_hbm,
                 part_ref, bias_ref, ko_hbm, vo_hbm,
                 h_ref, pos_ref, scale_ref, rel_ref, w_in, wo_ref, keys, values, q_t, k_t, v_t, acc_ref, p_ref, ctx_t,
                 s_sem, w_sem, k_sem, v_sem, ko_sem, vo_sem):
    heads = keys.shape[0]
    small = [pltpu.make_async_copy(s, d, s_sem.at[i]) for i, (s, d) in enumerate(
        ((h_hbm, h_ref), (scale_hbm, scale_ref), (pos_hbm, pos_ref), (rel_hbm, rel_ref)))]
    w_copies = [pltpu.make_async_copy(w.at[layer], w_in.at[i], w_sem.at[i]) for i, w in enumerate((wq_hbm, wk_hbm, wv_hbm))]
    wo_copy = pltpu.make_async_copy(wo_hbm.at[layer], wo_ref, w_sem.at[3])

    def k_in(head):
        return pltpu.make_async_copy(k_hbm.at[layer, head], keys.at[head], k_sem.at[head])

    def v_in(head):
        return pltpu.make_async_copy(v_hbm.at[layer, head], values.at[head], v_sem.at[head])

    for c in small + w_copies:
        c.start()
    for head in range(heads):
        k_in(head).start()
    for head in range(heads):
        v_in(head).start(priority=1)
    wo_copy.start(priority=1)

    slots, tokens = bias_ref.shape[1:]
    small[2].wait()
    small[3].wait()
    dist = pos_ref[...] - lax.broadcasted_iota(jnp.int32, (slots, tokens), 0)
    bias = [jnp.zeros((slots, tokens), F32)] * heads
    for d in range(slots):
        hit = dist == d
        bias = [jnp.where(hit, rel_ref[head, d], b) for head, b in enumerate(bias)]
    for head in range(heads):
        bias_ref[head] = bias[head]
    small[0].wait()
    small[1].wait()

    self_part(layer, h_ref, pos_ref, scale_ref, bias_ref, w_in, [c.wait for c in w_copies], wo_ref, wo_copy.wait,
              keys, values, lambda head: k_in(head).wait(), lambda head: v_in(head).wait(), keys, values,
              part_ref, ko_hbm, vo_hbm, q_t, k_t, v_t, acc_ref, p_ref, ctx_t, ko_sem, vo_sem)


def second_kernel(layer, h_ref, pos_ref, scale_ref, bias_ref, w_in, wo_ref, keys_in, values_in, _, __,
                  part_ref, ko_hbm, vo_hbm,
                  keys, values, q_t, k_t, v_t, acc_ref, p_ref, ctx_t, ko_sem, vo_sem):
    self_part(layer, h_ref, pos_ref, scale_ref, bias_ref, w_in, [None] * 3, wo_ref, None,
              keys_in, values_in, None, None, keys, values,
              part_ref, ko_hbm, vo_hbm, q_t, k_t, v_t, acc_ref, p_ref, ctx_t, ko_sem, vo_sem)


def self_part(layer, h_ref, pos_ref, scale_ref, bias_ref, w_in, w_waits, wo_ref, wo_wait,
              keys_in, values_in, k_wait, v_wait, keys, values,
              part_ref, ko_hbm, vo_hbm, q_t, k_t, v_t, acc_ref, p_ref, ctx_t, ko_sem, vo_sem):
    heads, slots, head_dim, tokens = keys.shape

    def k_out(head):
        return pltpu.make_async_copy(keys.at[head], ko_hbm.at[layer, head], ko_sem.at[head])

    def v_out(head):
        return pltpu.make_async_copy(values.at[head], vo_hbm.at[layer, head], vo_sem.at[head])

    x = rms_norm(h_ref[...].astype(F32), scale_ref[0, layer:layer + 1, :])
    pos = pos_ref[...]
    valid = pos >= lax.broadcasted_iota(jnp.int32, (slots, tokens), 0)
    pos_b = jnp.broadcast_to(pos.astype(F32), (head_dim, tokens)).astype(BF16)

    for i, target in enumerate((q_t, k_t, v_t)):
        if w_waits[i] is not None:
            w_waits[i]()
        proj = dot(x, w_in[i]).astype(BF16).astype(F32)
        target[...] = jnp.transpose(proj).reshape(target.shape).astype(target.dtype)

    def score_step(head, carry):
        if k_wait is not None:
            k_wait(head)
        score_head(q_t[head], keys_in, head, acc_ref, (pos_b, k_t[head], keys))
        k_out(head).start()
        return carry

    lax.fori_loop(0, heads, score_step, 0)
    for head in range(heads):
        scores = jnp.where(valid, gather_scores(acc_ref, head, slots) + bias_ref[head], NEG_BIG)
        p_ref[head] = softmax_rows(scores)

    def context_step(head, carry):
        if v_wait is not None:
            v_wait(head)
        ctx_t[head] = context_head(p_ref, values_in, head, (pos_b, v_t[head], values))
        v_out(head).start()
        return carry

    lax.fori_loop(0, heads, context_step, 0)
    ctx = jnp.transpose(ctx_t[...].reshape(heads * head_dim, tokens)).astype(BF16)
    if wo_wait is not None:
        wo_wait()
    part_ref[...] = dot(ctx, wo_ref[...]).astype(BF16)
    for head in range(heads):
        k_out(head).wait()
        v_out(head).wait()


def attention_scratch(heads, slots, head_dim, tokens):
    return [
        pltpu.VMEM((heads, slots, head_dim, tokens), BF16),
        pltpu.VMEM((heads, slots, head_dim, tokens), BF16),
        pltpu.VMEM((heads, head_dim, tokens), F32),
        pltpu.VMEM((heads, head_dim, tokens), BF16),
        pltpu.VMEM((heads, head_dim, tokens), BF16),
        pltpu.VMEM((heads, slots * 8, tokens), F32),
        pltpu.VMEM((heads, slots, tokens), F32),
        pltpu.VMEM((heads, head_dim, tokens), F32),
    ]


def self_first(layer, h, pos, scale, rel, w_query, w_key, w_value, w_out, keys, values):
    _, heads, slots, head_dim, tokens = keys.shape
    width, model = w_out.shape[1:]
    vmem = pl.BlockSpec(memory_space=pltpu.VMEM)
    hbm = pl.BlockSpec(memory_space=pltpu.HBM)
    dma = pltpu.SemaphoreType.DMA
    ins = [pinned(x) for x in (h, pos, scale, rel, w_query, w_key, w_value, w_out, keys, values)]
    cache = pltpu.HBM(keys.shape, keys.dtype)
    return pl.pallas_call(
        functools.partial(first_kernel, layer),
        out_shape=[pltpu.VMEM((tokens, model), BF16), pltpu.VMEM((heads, slots, tokens), F32), cache, cache],
        in_specs=[hbm] * 10,
        out_specs=[vmem, vmem, hbm, hbm],
        scratch_shapes=[
            pltpu.VMEM((tokens, model), BF16),
            pltpu.VMEM(pos.shape, pos.dtype),
            pltpu.VMEM(scale.shape, F32),
            pltpu.SMEM(rel.shape, F32),
            pltpu.VMEM((3, model, width), BF16),
            pltpu.VMEM((width, model), BF16),
        ] + attention_scratch(heads, slots, head_dim, tokens) + [
            dma((4,)), dma((4,)), dma((heads,)), dma((heads,)), dma((heads,)), dma((heads,)),
        ],
        compiler_params=pltpu.CompilerParams(vmem_limit_bytes=20 * MIB),
        name="self_first",
    )(*ins)


def self_second(layer, h, pos, scale, bias, w_in, w_out, keys_in, values_in, k_out, v_out):
    heads, slots, head_dim, tokens = keys_in.shape
    vmem = pl.BlockSpec(memory_space=pltpu.VMEM)
    hbm = pl.BlockSpec(memory_space=pltpu.HBM)
    dma = pltpu.SemaphoreType.DMA
    cache = pltpu.HBM(k_out.shape, k_out.dtype)
    return pl.pallas_call(
        functools.partial(second_kernel, layer),
        out_shape=[pltpu.VMEM(h.shape, BF16), cache, cache],
        in_specs=[vmem] * 8 + [hbm] * 2,
        out_specs=[vmem, hbm, hbm],
        input_output_aliases={8: 1, 9: 2},
        scratch_shapes=attention_scratch(heads, slots, head_dim, tokens) + [dma((heads,)), dma((heads,))],
        compiler_params=pltpu.CompilerParams(vmem_limit_bytes=20 * MIB),
        name="self_second",
    )(h, pos, scale, bias, w_in, w_out, keys_in, values_in, pinned(k_out), pinned(v_out))


def tp_exchange(src, dst, send_sem, recv_sem):
    return pltpu.make_async_remote_copy(
        src_ref=src, dst_ref=dst, send_sem=send_sem, recv_sem=recv_sem,
        device_id={"tp": 1 - lax.axis_index("tp")}, device_id_type=MESH)


def add_parts(h_float, mine, other):
    delta = (mine.astype(F32) + other.astype(F32)).astype(BF16)
    return (h_float + delta.astype(F32)).astype(BF16).astype(F32)


def cross_part(layer, x, mask, wq_copy, wq_ref, wo_copy, wo_ref, k_in, keys, v_in, values, q_t, acc_ref, p_ref, ctx_t):
    heads, slots, head_dim, tokens = keys.shape
    wq_copy.wait()
    proj = dot(x, wq_ref[...]).astype(BF16).astype(F32)
    q_t[...] = jnp.transpose(proj).reshape(heads, head_dim, tokens)

    def score_step(head, carry):
        k_in(head).wait()
        score_head(q_t[head], keys, head, acc_ref)
        return carry

    lax.fori_loop(0, heads, score_step, 0)
    valid = mask > 0
    for head in range(heads):
        p_ref[head] = softmax_rows(jnp.where(valid, gather_scores(acc_ref, head, slots), NEG_BIG))

    def context_step(head, carry):
        v_in(head).wait()
        ctx_t[head] = context_head(p_ref, values, head)
        return carry

    lax.fori_loop(0, heads, context_step, 0)
    ctx = jnp.transpose(ctx_t[...].reshape(heads * head_dim, tokens)).astype(BF16)
    wo_copy.wait()
    return dot(ctx, wo_ref[...]).astype(BF16)


def middle_kernel(layer, part_ref, h_hbm, mask_hbm, scale_hbm, pos_hbm, wq_hbm, wo_hbm, k_hbm, v_hbm, dg_hbm, du_hbm, dd_hbm,
                  nq_hbm, nk_hbm, nv_hbm, no_hbm, nkeys_hbm, nvalues_hbm,
                  out_ref, pos_ref, scale_ref, nw_ref, nwo_ref, nkeys_ref, nvalues_ref,
                  h_ref, mask_ref, wq_ref, wo_ref, keys, values, dg_ref, du_ref, dd_ref, q_t, acc_ref, p_ref, ctx_t, mine_ref, other_ref, prod_ref,
                  w_sem, k_sem, v_sem, send_sem, recv_sem, s_sem, n_sem):
    heads = keys.shape[0]
    small = [pltpu.make_async_copy(s, d, s_sem.at[i]) for i, (s, d) in enumerate(
        ((h_hbm, h_ref), (mask_hbm, mask_ref), (scale_hbm, scale_ref), (pos_hbm, pos_ref)))]
    following = [pltpu.make_async_copy(s, d, n_sem.at[i]) for i, (s, d) in enumerate(
        ((nq_hbm.at[layer + 1], nw_ref.at[0]), (nk_hbm.at[layer + 1], nw_ref.at[1]), (nv_hbm.at[layer + 1], nw_ref.at[2]),
         (no_hbm.at[layer + 1], nwo_ref), (nkeys_hbm.at[layer + 1], nkeys_ref), (nvalues_hbm.at[layer + 1], nvalues_ref)))]

    def k_in(head):
        return pltpu.make_async_copy(k_hbm.at[layer, head], keys.at[head], k_sem.at[head])

    def v_in(head):
        return pltpu.make_async_copy(v_hbm.at[layer, head], values.at[head], v_sem.at[head])

    wq_copy = pltpu.make_async_copy(wq_hbm.at[layer], wq_ref, w_sem.at[0])
    wo_copy = pltpu.make_async_copy(wo_hbm.at[layer], wo_ref, w_sem.at[1])
    dense = [pltpu.make_async_copy(s, d, w_sem.at[2 + i]) for i, (s, d) in enumerate(((dg_hbm, dg_ref), (du_hbm, du_ref), (dd_hbm, dd_ref)))]

    barrier = pltpu.get_barrier_semaphore()
    pl.semaphore_signal(barrier, inc=1, device_id={"tp": 1 - lax.axis_index("tp")}, device_id_type=MESH)
    for c in small:
        c.start()
    wq_copy.start()
    for head in range(heads):
        k_in(head).start()
    for head in range(heads):
        v_in(head).start(priority=1)
    wo_copy.start(priority=1)
    for c in dense + following:
        c.start(priority=1)
    pl.semaphore_wait(barrier, 1)

    copies = [tp_exchange(part_ref if i == 0 else mine_ref.at[i - 1], other_ref.at[i], send_sem.at[i], recv_sem.at[i]) for i in range(3)]
    copies[0].start()
    for c in small:
        c.wait()
    copies[0].wait()
    h_float = add_parts(h_ref[...].astype(F32), part_ref[...], other_ref[0])

    x = rms_norm(h_float, scale_ref[1, layer:layer + 1, :])
    mine_ref[0] = cross_part(layer, x, mask_ref[...], wq_copy, wq_ref, wo_copy, wo_ref, k_in, keys, v_in, values, q_t, acc_ref, p_ref, ctx_t)
    copies[1].start()
    copies[1].wait()
    h_float = add_parts(h_float, mine_ref[0], other_ref[1])

    x = rms_norm(h_float, scale_ref[2, layer:layer + 1, :])
    dense[0].wait()
    dense[1].wait()
    width = dg_ref.shape[1]
    step = 512
    for c in range(0, width, step):
        gate_in = dot(x, dg_ref[:, c:c + step])
        lin_in = dot(x, du_ref[:, c:c + step])
        prod_ref[:, c:c + step] = (jax.nn.gelu(gate_in) * lin_in).astype(BF16)
    dense[2].wait()
    mine_ref[1] = dot(prod_ref[...], dd_ref[...]).astype(BF16)
    copies[2].start()
    copies[2].wait()
    out_ref[...] = add_parts(h_float, mine_ref[1], other_ref[2]).astype(BF16)
    for c in following:
        c.wait()


def middle(layer, part, h, mask, scale, pos, w_query, w_out, keys, values, dense_gate, dense_up, dense_down, following):
    _, heads, slots, head_dim, tokens = keys.shape
    width, model = w_out.shape[1:]
    ff = dense_gate.shape[1]
    vmem = pl.BlockSpec(memory_space=pltpu.VMEM)
    hbm = pl.BlockSpec(memory_space=pltpu.HBM)
    dma = pltpu.SemaphoreType.DMA
    cache = pltpu.VMEM((heads, slots, head_dim, tokens), BF16)
    return pl.pallas_call(
        functools.partial(middle_kernel, layer),
        out_shape=[
            pltpu.VMEM((tokens, model), BF16), pltpu.VMEM(pos.shape, pos.dtype), pltpu.VMEM(scale.shape, F32),
            pltpu.VMEM((3, model, width), BF16), pltpu.VMEM((width, model), BF16), cache, cache,
        ],
        in_specs=[vmem] + [hbm] * 17,
        out_specs=[vmem] * 7,
        scratch_shapes=[
            pltpu.VMEM((tokens, model), BF16),
            pltpu.VMEM(mask.shape, mask.dtype),
            pltpu.VMEM((model, width), BF16),
            pltpu.VMEM((width, model), BF16),
            pltpu.VMEM((heads, slots, head_dim, tokens), BF16),
            pltpu.VMEM((heads, slots, head_dim, tokens), BF16),
            pltpu.VMEM((model, ff), BF16),
            pltpu.VMEM((model, ff), BF16),
            pltpu.VMEM((ff, model), BF16),
            pltpu.VMEM((heads, head_dim, tokens), F32),
            pltpu.VMEM((heads, slots * 8, tokens), F32),
            pltpu.VMEM((heads, slots, tokens), F32),
            pltpu.VMEM((heads, head_dim, tokens), F32),
            pltpu.VMEM((2, tokens, model), BF16),
            pltpu.VMEM((3, tokens, model), BF16),
            pltpu.VMEM((tokens, ff), BF16),
            dma((5,)), dma((heads,)), dma((heads,)), dma((3,)), dma((3,)), dma((4,)), dma((6,)),
        ],
        compiler_params=pltpu.CompilerParams(vmem_limit_bytes=26 * MIB, collective_id=0, has_side_effects=True),
        name="middle",
    )(part, *map(pinned, (h, mask, scale, pos, w_query, w_out, keys, values, dense_gate, dense_up, dense_down) + following))


def last_kernel(layer, h_ref, part_ref, mask_hbm, idx_hbm, scale_hbm, router_hbm, wq_hbm, wo_hbm, k_hbm, v_hbm, eg_hbm, eu_hbm, ed_hbm,
                out_ref,
                mask_ref, idx_ref, scale_ref, router_ref, wq_ref, wo_ref, keys, values, eg_ref, eu_ref, ed_ref, q_t, acc_ref, p_ref, ctx_t, mine_ref, other_ref,
                place_ref, send_x, recv_x, product_ref, send_y, recv_y, comb_ref, gate_ref,
                w_sem, k_sem, v_sem, g_sem, d_sem, tp_send, tp_recv, x_send, x_recv, y_send, y_recv, s_sem):
    heads = k_sem.shape[0]
    tokens, model = h_ref.shape
    experts = router_ref.shape[0]
    local, groups, capacity, _ = recv_x.shape
    rows = groups * capacity
    g_slots, d_slots = eg_ref.shape[0], ed_ref.shape[0]
    tp = lax.axis_index("tp")
    ep = lax.axis_index("ep")
    me = tp * groups + ep

    def peer_ep(offset):
        return lax.rem(ep + offset, groups)

    def peer_tp(offset):
        return lax.rem(tp + offset, 2)

    def k_in(head):
        return pltpu.make_async_copy(k_hbm.at[layer, head], keys.at[head], k_sem.at[head])

    def v_in(head):
        return pltpu.make_async_copy(v_hbm.at[layer, head], values.at[head], v_sem.at[head])

    def gate_up_in(expert):
        slot = lax.rem(expert, g_slots)
        return [pltpu.make_async_copy(s.at[expert], d.at[slot], g_sem.at[slot, i]) for i, (s, d) in enumerate(((eg_hbm, eg_ref), (eu_hbm, eu_ref)))]

    def down_in(expert):
        slot = lax.rem(expert, d_slots)
        return pltpu.make_async_copy(ed_hbm.at[expert], ed_ref.at[slot], d_sem.at[slot])

    small = [pltpu.make_async_copy(s, d, s_sem.at[i]) for i, (s, d) in enumerate(
        ((mask_hbm, mask_ref), (idx_hbm, idx_ref), (scale_hbm, scale_ref), (router_hbm, router_ref)))]
    wq_copy = pltpu.make_async_copy(wq_hbm.at[layer], wq_ref, w_sem.at[0])
    wo_copy = pltpu.make_async_copy(wo_hbm.at[layer], wo_ref, w_sem.at[1])

    others = [(dt, de) for dt in range(2) for de in range(groups) if dt or de]
    barrier = pltpu.get_barrier_semaphore()
    for dt, de in others:
        pl.semaphore_signal(barrier, inc=1, device_id={"tp": peer_tp(dt), "ep": peer_ep(de)}, device_id_type=MESH)
    for c in small:
        c.start()
    wq_copy.start()
    for head in range(heads):
        k_in(head).start()
    for head in range(heads):
        v_in(head).start()
    wo_copy.start()
    for expert in range(max(g_slots, d_slots)):
        for c in (gate_up_in(expert) if expert < g_slots else []) + ([down_in(expert)] if expert < d_slots else []):
            c.start(priority=1)
    pl.semaphore_wait(barrier, len(others))

    copies = [tp_exchange(part_ref if i == 0 else mine_ref, other_ref.at[i], tp_send.at[i], tp_recv.at[i]) for i in range(2)]
    copies[0].start()

    for c in small:
        c.wait()
    idx = idx_ref[...]
    onehot = (lax.broadcasted_iota(jnp.int32, (experts, tokens), 0) == idx).astype(F32)
    earlier = (lax.broadcasted_iota(jnp.int32, (tokens, tokens), 0) < lax.broadcasted_iota(jnp.int32, (tokens, tokens), 1)).astype(F32)
    counts = dot(onehot.astype(BF16), earlier.astype(BF16))
    slot_of = jnp.sum(counts * onehot, axis=0, keepdims=True).astype(jnp.int32)
    row_of = jnp.where(slot_of < capacity, lax.rem(idx, local) * rows + lax.div(idx, local) * capacity + slot_of, -1)
    place_ref[...] = (lax.broadcasted_iota(jnp.int32, (experts * capacity, tokens), 0) == row_of).astype(F32).astype(BF16)

    copies[0].wait()
    h_float = add_parts(h_ref[...].astype(F32), part_ref[...], other_ref[0])
    x = rms_norm(h_float, scale_ref[1, layer:layer + 1, :])
    mine_ref[...] = cross_part(layer, x, mask_ref[...], wq_copy, wq_ref, wo_copy, wo_ref, k_in, keys, v_in, values, q_t, acc_ref, p_ref, ctx_t)
    copies[1].start()
    copies[1].wait()
    h_float = add_parts(h_float, mine_ref[...], other_ref[1])
    x = rms_norm(h_float, scale_ref[2, layer:layer + 1, :])

    def x_copy(expert, offset):
        return pltpu.make_async_remote_copy(
            src_ref=send_x.at[expert, peer_ep(offset)], dst_ref=recv_x.at[expert, ep],
            send_sem=x_send.at[expert], recv_sem=x_recv.at[expert],
            device_id={"ep": peer_ep(offset)}, device_id_type=MESH)

    def x_all(expert):
        return pltpu.make_async_remote_copy(
            src_ref=send_x.at[expert, 0:groups - 1], dst_ref=recv_x.at[expert, 0:groups - 1],
            send_sem=x_send.at[expert], recv_sem=x_recv.at[expert],
            device_id={"ep": peer_ep(1)}, device_id_type=MESH)

    def y_copy(expert, number):
        dt, de = others[number]
        return pltpu.make_async_remote_copy(
            src_ref=send_y.at[expert, peer_ep(de)], dst_ref=recv_y.at[expert, me],
            send_sem=y_send.at[expert], recv_sem=y_recv.at[expert],
            device_id={"tp": peer_tp(dt), "ep": peer_ep(de)}, device_id_type=MESH)

    def y_all(expert):
        return pltpu.make_async_remote_copy(
            src_ref=recv_y.at[expert, 0:2 * groups - 1], dst_ref=recv_y.at[expert, 0:2 * groups - 1],
            send_sem=y_send.at[expert], recv_sem=y_recv.at[expert],
            device_id={"ep": peer_ep(1)}, device_id_type=MESH)

    buffers = dot(place_ref[...], x).astype(BF16)
    for expert in range(local):
        for g in range(groups):
            first = expert * rows + g * capacity
            send_x[expert, g] = buffers[first:first + capacity]
        for offset in range(1, groups):
            x_copy(expert, offset).start()
    recv_x[:, ep] = send_x[:, ep]

    router = router_ref[...]
    high = router.astype(BF16)
    rest = router - high.astype(F32)
    mid = rest.astype(BF16)
    low = (rest - mid.astype(F32)).astype(BF16)
    logits = dot_nt(high, x) + (dot_nt(mid, x) + dot_nt(low, x))
    logits_exp = jnp.exp(logits - jnp.max(logits, axis=0, keepdims=True))
    gate = jnp.sum(logits_exp * onehot, axis=0, keepdims=True) / jnp.sum(logits_exp, axis=0, keepdims=True)
    gate_ref[...] = jnp.transpose(jnp.broadcast_to(gate, (tokens, tokens)))

    def gate_up(expert):
        slot = lax.rem(expert, g_slots)
        x_rows = jnp.concatenate([recv_x[expert, g].astype(F32) for g in range(groups)], axis=0).astype(BF16)
        return (jax.nn.gelu(dot(x_rows, eg_ref[slot])) * dot(x_rows, eu_ref[slot])).astype(BF16)

    def send_result(expert, y):
        for g in range(groups):
            send_y[expert, g] = y[g * capacity:(g + 1) * capacity]
        for number in range(len(others)):
            y_copy(expert, number).start()
        recv_y[expert, me] = send_y[expert, ep]

    def wait_gate_up(expert):
        x_all(expert).wait_recv()
        for c in gate_up_in(expert):
            c.wait()

    def collect(expert):
        y_all(expert).wait_recv()
        blocks = [recv_y[expert, g].astype(F32) + recv_y[expert, groups + g].astype(F32) for g in range(groups)]
        comb_ref[pl.ds(pl.multiple_of(expert * rows, rows), rows), :] = jnp.concatenate(blocks, axis=0).astype(BF16)

    wait_gate_up(0)
    product_ref[0] = gate_up(0)
    for c in gate_up_in(g_slots):
        c.start(priority=1)
    lag = 4

    def expert_step(expert, carry):
        wait_gate_up(expert)
        down_in(expert - 1).wait()
        before = product_ref[lax.rem(expert - 1, 2)]
        y = dot(before, ed_ref[lax.rem(expert - 1, d_slots)]).astype(BF16)
        product_ref[lax.rem(expert, 2)] = gate_up(expert)
        send_result(expert - 1, y)

        @pl.when(expert + g_slots < local)
        def _():
            for c in gate_up_in(expert + g_slots):
                c.start(priority=1)

        @pl.when(expert - 1 + d_slots < local)
        def _():
            down_in(expert - 1 + d_slots).start(priority=1)

        @pl.when(expert >= lag)
        def _():
            collect(expert - lag)
        return carry

    lax.fori_loop(1, local, expert_step, 0)
    down_in(local - 1).wait()
    send_result(local - 1, dot(product_ref[(local - 1) % 2], ed_ref[(local - 1) % d_slots]).astype(BF16))
    for expert in range(local - lag, local):
        collect(expert)
    combined = dot_t(place_ref[...], comb_ref[...])
    gate_col = gate_ref[...]
    for c in range(0, model, tokens):
        delta = gate_col * combined[:, c:c + tokens]
        out_ref[:, c:c + tokens] = (h_float[:, c:c + tokens] + delta).astype(BF16)
    for expert in range(local):
        x_all(expert).wait_send()
        y_all(expert).wait_send()


def last(layer, h, part, mask, idx, scale, router, w_query, w_out, keys, values, exp_gate, exp_up, exp_down, groups):
    _, heads, slots, head_dim, tokens = keys.shape
    width, model = w_out.shape[1:]
    local, _, ff = exp_gate.shape
    experts = router.shape[0]
    capacity = (2 * tokens + experts - 1) // experts
    vmem = pl.BlockSpec(memory_space=pltpu.VMEM)
    hbm = pl.BlockSpec(memory_space=pltpu.HBM)
    dma = pltpu.SemaphoreType.DMA
    on_chip = functools.partial(pltpu.with_memory_space_constraint, memory_space=pltpu.VMEM)
    return pl.pallas_call(
        functools.partial(last_kernel, layer),
        out_shape=pltpu.VMEM((tokens, model), BF16),
        in_specs=[vmem] * 2 + [hbm] * 11,
        out_specs=vmem,
        scratch_shapes=[
            pltpu.VMEM(mask.shape, mask.dtype),
            pltpu.VMEM(idx.shape, idx.dtype),
            pltpu.VMEM(scale.shape, F32),
            pltpu.VMEM(router.shape, F32),
            pltpu.VMEM((model, width), BF16),
            pltpu.VMEM((width, model), BF16),
            pltpu.VMEM((heads, slots, head_dim, tokens), BF16),
            pltpu.VMEM((heads, slots, head_dim, tokens), BF16),
            pltpu.VMEM((GATE_SLOTS, model, ff), BF16),
            pltpu.VMEM((GATE_SLOTS, model, ff), BF16),
            pltpu.VMEM((DOWN_SLOTS, ff, model), BF16),
            pltpu.VMEM((heads, head_dim, tokens), F32),
            pltpu.VMEM((heads, slots * 8, tokens), F32),
            pltpu.VMEM((heads, slots, tokens), F32),
            pltpu.VMEM((heads, head_dim, tokens), F32),
            pltpu.VMEM((tokens, model), BF16),
            pltpu.VMEM((2, tokens, model), BF16),
            pltpu.VMEM((experts * capacity, tokens), BF16),
            pltpu.VMEM((local, groups, capacity, model), BF16),
            pltpu.VMEM((local, groups, capacity, model), BF16),
            pltpu.VMEM((2, groups * capacity, ff), BF16),
            pltpu.VMEM((local, groups, capacity, model), BF16),
            pltpu.VMEM((local, 2 * groups, capacity, model), BF16),
            pltpu.VMEM((experts * capacity, model), BF16),
            pltpu.VMEM((tokens, tokens), F32),
            dma((2,)), dma((heads,)), dma((heads,)), dma((GATE_SLOTS, 2)), dma((DOWN_SLOTS,)), dma((2,)), dma((2,)),
            dma((local,)), dma((local,)), dma((local,)), dma((local,)), dma((4,)),
        ],
        compiler_params=pltpu.CompilerParams(vmem_limit_bytes=LAST_VMEM, collective_id=1, has_side_effects=True),
        name="last",
    )(on_chip(h), on_chip(part), *map(pinned, (mask, idx, scale, router, w_query, w_out, keys, values, exp_gate, exp_up, exp_down)))


def decode_body(groups, hidden, write_pos, enc_mask, expert_idx, self_keys, self_values, cross_keys, cross_values, rel_bias, norm_scale, w_query, w_key, w_value, w_out, w_cross_query, w_cross_out, dense_gate, dense_up, dense_down, router, exp_gate, exp_up, exp_down):
    def lanes(cache):
        return jnp.transpose(cache, (0, 2, 3, 4, 1))

    pos = write_pos.reshape(1, -1)
    idx = expert_idx.reshape(1, -1)
    mask = jnp.transpose(enc_mask)
    scale = jnp.transpose(norm_scale, (1, 0, 2))
    keys, values, ckeys, cvalues = map(lanes, (self_keys, self_values, cross_keys, cross_values))
    part, bias, k_out, v_out = self_first(0, hidden, pos, scale, rel_bias, w_query, w_key, w_value, w_out, keys, values)
    following = (w_query, w_key, w_value, w_out, keys, values)
    h, pos, scale_in, w_in, w_o, keys, values = middle(0, part, hidden, mask, scale, pos, w_cross_query, w_cross_out, ckeys, cvalues, dense_gate, dense_up, dense_down, following)
    part, k_out, v_out = self_second(1, h, pos, scale_in, bias, w_in, w_o, keys, values, k_out, v_out)
    h = last(1, h, part, mask, idx, scale, jnp.transpose(router), w_cross_query, w_cross_out, ckeys, cvalues, exp_gate, exp_up, exp_down, groups)
    return h, jnp.transpose(k_out, (0, 4, 1, 2, 3)), jnp.transpose(v_out, (0, 4, 1, 2, 3))


def solution(mesh):
    batch = ('dp', 'ep')
    row_spec = P(batch, None)
    vec_spec = P(batch)
    cache_spec = P(None, batch, 'tp', None, None)
    col_spec = P(None, None, 'tp')
    out_rows = P(None, 'tp', None)
    in_specs = (row_spec, vec_spec, row_spec, vec_spec, cache_spec, cache_spec, cache_spec, cache_spec, P('tp', None), P(), col_spec, col_spec, col_spec, out_rows, col_spec, out_rows, P(None, 'tp'), P(None, 'tp'), P('tp', None), P(), P('ep', None, 'tp'), P('ep', None, 'tp'), P('ep', 'tp', None))
    out_specs = (row_spec, cache_spec, cache_spec)
    body = functools.partial(decode_body, mesh.shape['ep'])
    return jax.shard_map(body, mesh=mesh, in_specs=in_specs, out_specs=out_specs, check_vma=False)
```

```python
import functools

import jax
import jax.numpy as jnp
from jax import lax
from jax.experimental import pallas as pl
from jax.experimental.pallas import tpu as pltpu
from jax.sharding import PartitionSpec as P

EPS = 1e-6
NEG_BIG = -1e9
MESH = pl.DeviceIdType.MESH
BF16 = jnp.bfloat16
F32 = jnp.float32
MIB = 1024 * 1024
GATE_SLOTS = 8
DOWN_SLOTS = 8
LAST_VMEM = 62 * MIB


def rms_norm(h_float, scale):
    inv_rms = lax.rsqrt(jnp.mean(h_float * h_float, axis=-1, keepdims=True) + EPS)
    return (h_float * inv_rms * scale).astype(BF16)


def dot(a, b):
    return jnp.dot(a, b, preferred_element_type=F32)


def dot_t(a, b):
    return lax.dot_general(a, b, (((0,), (0,)), ((), ())), preferred_element_type=F32)


def dot_nt(a, b):
    return lax.dot_general(a, b, (((1,), (1,)), ((), ())), preferred_element_type=F32)


def fold_rows(prod):
    parts = [prod[i * 8:(i + 1) * 8] for i in range(prod.shape[0] // 8)]
    while len(parts) > 1:
        parts = [a + b for a, b in zip(parts[::2], parts[1::2])]
    return parts[0]


def score_head(q_head, keys, head, acc_ref, merge=None):
    for slot in range(acc_ref.shape[1] // 8):
        k_slot = keys(head, slot) if callable(keys) else keys[head, slot]
        if merge is not None:
            pos_b, k_new, merged = merge
            k_slot = jnp.where(pos_b == jnp.asarray(slot, BF16), k_new, k_slot)
            merged[head, slot] = k_slot
        acc_ref[head, slot * 8:(slot + 1) * 8, :] = fold_rows(k_slot.astype(F32) * q_head)


def gather_scores(acc_ref, head, slots):
    total = acc_ref[head, pl.ds(0, slots, stride=8), :]
    for i in range(1, 8):
        total = total + acc_ref[head, pl.ds(i, slots, stride=8), :]
    return total


def softmax_rows(scores):
    top = jnp.max(scores, axis=0, keepdims=True)
    e = jnp.exp(scores - top)
    return (e / jnp.sum(e, axis=0, keepdims=True)).astype(BF16).astype(F32)


def context_head(p_ref, values, head, merge=None):
    total = None
    for slot in range(p_ref.shape[1]):
        v_slot = values(head, slot) if callable(values) else values[head, slot]
        if merge is not None:
            pos_b, v_new, merged = merge
            v_slot = jnp.where(pos_b == jnp.asarray(slot, BF16), v_new, v_slot)
            merged[head, slot] = v_slot
        term = v_slot.astype(F32) * p_ref[head, slot:slot + 1, :]
        total = term if total is None else total + term
    return total


def pinned(x):
    return pltpu.with_memory_space_constraint(x, pltpu.HBM)


def first_kernel(layer, h_hbm, pos_hbm, scale_hbm, rel_hbm, wq_hbm, wk_hbm, wv_hbm, wo_hbm, k_hbm, v_hbm,
                 part_ref, bias_ref, ko_hbm, values,
                 h_ref, pos_ref, scale_ref, rel_ref, w_in, wo_ref, keys, q_t, k_t, v_t, acc_ref, p_ref, ctx_t,
                 s_sem, w_sem, k_sem, v_sem, ko_sem):
    heads = keys.shape[0]
    small = [pltpu.make_async_copy(s, d, s_sem.at[i]) for i, (s, d) in enumerate(
        ((h_hbm, h_ref), (scale_hbm, scale_ref), (pos_hbm, pos_ref), (rel_hbm, rel_ref)))]
    w_copies = [pltpu.make_async_copy(w.at[layer], w_in.at[i], w_sem.at[i]) for i, w in enumerate((wq_hbm, wk_hbm, wv_hbm))]
    wo_copy = pltpu.make_async_copy(wo_hbm.at[layer], wo_ref, w_sem.at[3])

    def k_in(head):
        return pltpu.make_async_copy(k_hbm.at[layer, head], keys.at[head], k_sem.at[head])

    def v_in(head):
        return pltpu.make_async_copy(v_hbm.at[layer, head], values.at[head], v_sem.at[head])

    for c in small + w_copies:
        c.start()
    for head in range(heads):
        k_in(head).start()
    for head in range(heads):
        v_in(head).start(priority=1)
    wo_copy.start(priority=1)

    slots, tokens = bias_ref.shape[1:]
    small[2].wait()
    small[3].wait()
    dist = pos_ref[...] - lax.broadcasted_iota(jnp.int32, (slots, tokens), 0)
    bias = [jnp.zeros((slots, tokens), F32)] * heads
    for d in range(slots):
        hit = dist == d
        bias = [jnp.where(hit, rel_ref[head, d], b) for head, b in enumerate(bias)]
    for head in range(heads):
        bias_ref[head] = bias[head]
    small[0].wait()
    small[1].wait()

    self_part(layer, h_ref, pos_ref, scale_ref, bias_ref, w_in, [c.wait for c in w_copies], wo_ref, wo_copy.wait,
              keys, values, lambda head: k_in(head).wait(), lambda head: v_in(head).wait(), keys, values,
              part_ref, ko_hbm, None, q_t, k_t, v_t, acc_ref, p_ref, ctx_t, ko_sem, None)


def second_kernel(layer, h_ref, pos_ref, scale_ref, bias_ref, w_in, wo_ref, keys_in, values_in, values_before, _,
                  part_ref, ko_hbm, vo_hbm,
                  keys, values, q_t, k_t, v_t, acc_ref, p_ref, ctx_t, ko_sem, vo_sem, before_sem):
    before = pltpu.make_async_copy(values_before, vo_hbm.at[layer - 1], before_sem)
    before.start()
    self_part(layer, h_ref, pos_ref, scale_ref, bias_ref, w_in, [None] * 3, wo_ref, None,
              keys_in, values_in, None, None, keys, values,
              part_ref, ko_hbm, vo_hbm, q_t, k_t, v_t, acc_ref, p_ref, ctx_t, ko_sem, vo_sem)
    before.wait()


def self_part(layer, h_ref, pos_ref, scale_ref, bias_ref, w_in, w_waits, wo_ref, wo_wait,
              keys_in, values_in, k_wait, v_wait, keys, values,
              part_ref, ko_hbm, vo_hbm, q_t, k_t, v_t, acc_ref, p_ref, ctx_t, ko_sem, vo_sem):
    heads, slots, head_dim, tokens = keys.shape

    def k_out(head):
        return pltpu.make_async_copy(keys.at[head], ko_hbm.at[layer, head], ko_sem.at[head])

    def v_out(head):
        return pltpu.make_async_copy(values.at[head], vo_hbm.at[layer, head], vo_sem.at[head])

    x = rms_norm(h_ref[...].astype(F32), scale_ref[0, layer:layer + 1, :])
    pos = pos_ref[...]
    valid = pos >= lax.broadcasted_iota(jnp.int32, (slots, tokens), 0)
    pos_b = jnp.broadcast_to(pos.astype(F32), (head_dim, tokens)).astype(BF16)

    for i, target in enumerate((q_t, k_t, v_t)):
        if w_waits[i] is not None:
            w_waits[i]()
        proj = dot(x, w_in[i]).astype(BF16).astype(F32)
        target[...] = jnp.transpose(proj).reshape(target.shape).astype(target.dtype)

    def score_step(head, carry):
        if k_wait is not None:
            k_wait(head)
        score_head(q_t[head], keys_in, head, acc_ref, (pos_b, k_t[head], keys))
        k_out(head).start()
        return carry

    lax.fori_loop(0, heads, score_step, 0)
    for head in range(heads):
        scores = jnp.where(valid, gather_scores(acc_ref, head, slots) + bias_ref[head], NEG_BIG)
        p_ref[head] = softmax_rows(scores)

    def context_step(head, carry):
        if v_wait is not None:
            v_wait(head)
        ctx_t[head] = context_head(p_ref, values_in, head, (pos_b, v_t[head], values))
        if vo_hbm is not None:
            v_out(head).start()
        return carry

    lax.fori_loop(0, heads, context_step, 0)
    ctx = jnp.transpose(ctx_t[...].reshape(heads * head_dim, tokens)).astype(BF16)
    if wo_wait is not None:
        wo_wait()
    part_ref[...] = dot(ctx, wo_ref[...]).astype(BF16)
    for head in range(heads):
        k_out(head).wait()
        if vo_hbm is not None:
            v_out(head).wait()


def attention_scratch(heads, slots, head_dim, tokens):
    return [
        pltpu.VMEM((heads, slots, head_dim, tokens), BF16),
        pltpu.VMEM((heads, slots, head_dim, tokens), BF16),
        pltpu.VMEM((heads, head_dim, tokens), F32),
        pltpu.VMEM((heads, head_dim, tokens), BF16),
        pltpu.VMEM((heads, head_dim, tokens), BF16),
        pltpu.VMEM((heads, slots * 8, tokens), F32),
        pltpu.VMEM((heads, slots, tokens), F32),
        pltpu.VMEM((heads, head_dim, tokens), F32),
    ]


def self_first(layer, h, pos, scale, rel, w_query, w_key, w_value, w_out, keys, values):
    _, heads, slots, head_dim, tokens = keys.shape
    width, model = w_out.shape[1:]
    vmem = pl.BlockSpec(memory_space=pltpu.VMEM)
    hbm = pl.BlockSpec(memory_space=pltpu.HBM)
    dma = pltpu.SemaphoreType.DMA
    ins = [pinned(x) for x in (h, pos, scale, rel, w_query, w_key, w_value, w_out, keys, values)]
    cache = pltpu.HBM(keys.shape, keys.dtype)
    return pl.pallas_call(
        functools.partial(first_kernel, layer),
        out_shape=[
            pltpu.VMEM((tokens, model), BF16), pltpu.VMEM((heads, slots, tokens), F32), cache,
            pltpu.VMEM((heads, slots, head_dim, tokens), BF16),
        ],
        in_specs=[hbm] * 10,
        out_specs=[vmem, vmem, hbm, vmem],
        scratch_shapes=[
            pltpu.VMEM((tokens, model), BF16),
            pltpu.VMEM(pos.shape, pos.dtype),
            pltpu.VMEM(scale.shape, F32),
            pltpu.SMEM(rel.shape, F32),
            pltpu.VMEM((3, model, width), BF16),
            pltpu.VMEM((width, model), BF16),
        ] + attention_scratch(heads, slots, head_dim, tokens)[1:] + [
            dma((4,)), dma((4,)), dma((heads,)), dma((heads,)), dma((heads,)),
        ],
        compiler_params=pltpu.CompilerParams(vmem_limit_bytes=20 * MIB),
        name="self_first",
    )(*ins)


def self_second(layer, h, pos, scale, bias, w_in, w_out, keys_in, values_in, values_before, k_out):
    heads, slots, head_dim, tokens = keys_in.shape
    vmem = pl.BlockSpec(memory_space=pltpu.VMEM)
    hbm = pl.BlockSpec(memory_space=pltpu.HBM)
    dma = pltpu.SemaphoreType.DMA
    cache = pltpu.HBM(k_out.shape, k_out.dtype)
    return pl.pallas_call(
        functools.partial(second_kernel, layer),
        out_shape=[pltpu.VMEM(h.shape, BF16), cache, cache],
        in_specs=[vmem] * 9 + [hbm],
        out_specs=[vmem, hbm, hbm],
        input_output_aliases={9: 1},
        scratch_shapes=attention_scratch(heads, slots, head_dim, tokens) + [dma((heads,)), dma((heads,)), dma],
        compiler_params=pltpu.CompilerParams(vmem_limit_bytes=20 * MIB),
        name="self_second",
    )(h, pos, scale, bias, w_in, w_out, keys_in, values_in, values_before, pinned(k_out))


def tp_exchange(src, dst, send_sem, recv_sem):
    rows = src.shape[0] // 2
    return [pltpu.make_async_remote_copy(
        src_ref=src.at[i * rows:(i + 1) * rows], dst_ref=dst.at[i * rows:(i + 1) * rows],
        send_sem=send_sem.at[i], recv_sem=recv_sem.at[i],
        device_id={"tp": 1 - lax.axis_index("tp")}, device_id_type=MESH) for i in range(2)]


def halves(ref):
    rows = ref.shape[0] // 2
    return [ref[i * rows:(i + 1) * rows] for i in range(2)]


def send_projected(ctx, wo_ref, mine_ref, copies):
    rows = ctx.shape[0] // 2
    for i, copy in enumerate(copies):
        mine_ref[i * rows:(i + 1) * rows] = dot(ctx[i * rows:(i + 1) * rows], wo_ref[...]).astype(BF16)
        copy.start()


def receive_sum(h_parts, mine_ref, other_ref, copies):
    rows = mine_ref.shape[0] // 2
    for i, copy in enumerate(copies):
        copy.wait()
        part = slice(i * rows, (i + 1) * rows)
        yield add_parts(h_parts[i], mine_ref[part], other_ref[part])


def add_parts(h_float, mine, other):
    delta = (mine.astype(F32) + other.astype(F32)).astype(BF16)
    return (h_float + delta.astype(F32)).astype(BF16).astype(F32)


def cross_context(x, mask, wq_copy, wq_ref, k_wait, keys, v_wait, values, q_t, acc_ref, p_ref, ctx_t, unrolled=False):
    heads, head_dim, tokens = q_t.shape
    slots = p_ref.shape[1]
    wq_copy.wait()
    proj = dot(x, wq_ref[...]).astype(BF16).astype(F32)
    q_t[...] = jnp.transpose(proj).reshape(heads, head_dim, tokens)

    def score_step(head, carry):
        k_wait(head)
        score_head(q_t[head], keys, head, acc_ref)
        return carry

    def context_step(head, carry):
        v_wait(head)
        ctx_t[head] = context_head(p_ref, values, head)
        return carry

    def for_heads(step):
        if unrolled:
            for head in range(heads):
                step(head, 0)
        else:
            lax.fori_loop(0, heads, step, 0)

    for_heads(score_step)
    valid = mask > 0
    for head in range(heads):
        p_ref[head] = softmax_rows(jnp.where(valid, gather_scores(acc_ref, head, slots), NEG_BIG))
    for_heads(context_step)
    return jnp.transpose(ctx_t[...].reshape(heads * head_dim, tokens)).astype(BF16)


def middle_kernel(layer, part_ref, h_hbm, mask_hbm, scale_hbm, pos_hbm, wq_hbm, wo_hbm, k_hbm, v_hbm, dg_hbm, du_hbm, dd_hbm,
                  nq_hbm, nk_hbm, nv_hbm, no_hbm, nkeys_hbm, nvalues_hbm,
                  out_ref, pos_ref, scale_ref, nw_ref, nwo_ref, nkeys_ref, nvalues_ref,
                  h_ref, mask_ref, wq_ref, wo_ref, keys, values, dg_ref, du_ref, dd_ref, q_t, acc_ref, p_ref, ctx_t, mine_ref, other_ref, prod_ref,
                  w_sem, k_sem, v_sem, send_sem, recv_sem, s_sem, n_sem):
    heads = keys.shape[0]
    small = [pltpu.make_async_copy(s, d, s_sem.at[i]) for i, (s, d) in enumerate(
        ((h_hbm, h_ref), (mask_hbm, mask_ref), (scale_hbm, scale_ref), (pos_hbm, pos_ref)))]
    following = [pltpu.make_async_copy(s, d, n_sem.at[i]) for i, (s, d) in enumerate(
        ((nq_hbm.at[layer + 1], nw_ref.at[0]), (nk_hbm.at[layer + 1], nw_ref.at[1]), (nv_hbm.at[layer + 1], nw_ref.at[2]),
         (no_hbm.at[layer + 1], nwo_ref), (nkeys_hbm.at[layer + 1], nkeys_ref), (nvalues_hbm.at[layer + 1], nvalues_ref)))]

    def k_in(head):
        return pltpu.make_async_copy(k_hbm.at[layer, head], keys.at[head], k_sem.at[head])

    def v_in(head):
        return pltpu.make_async_copy(v_hbm.at[layer, head], values.at[head], v_sem.at[head])

    wq_copy = pltpu.make_async_copy(wq_hbm.at[layer], wq_ref, w_sem.at[0])
    wo_copy = pltpu.make_async_copy(wo_hbm.at[layer], wo_ref, w_sem.at[1])
    dense = [pltpu.make_async_copy(s, d, w_sem.at[2 + i]) for i, (s, d) in enumerate(((dg_hbm, dg_ref), (du_hbm, du_ref), (dd_hbm, dd_ref)))]

    barrier = pltpu.get_barrier_semaphore()
    pl.semaphore_signal(barrier, inc=1, device_id={"tp": 1 - lax.axis_index("tp")}, device_id_type=MESH)
    for c in small:
        c.start()
    wq_copy.start()
    for head in range(heads):
        k_in(head).start()
    for head in range(heads):
        v_in(head).start(priority=1)
    wo_copy.start(priority=1)
    for c in dense + following:
        c.start(priority=1)
    pl.semaphore_wait(barrier, 1)

    copies = [tp_exchange(part_ref if i == 0 else mine_ref.at[i - 1], other_ref.at[i], send_sem.at[i], recv_sem.at[i]) for i in range(3)]
    for c in copies[0]:
        c.start()
    for c in small:
        c.wait()
    h_parts = [h.astype(F32) for h in halves(h_ref)]
    h_new, x_new = [], []
    for h in receive_sum(h_parts, part_ref, other_ref.at[0], copies[0]):
        h_new.append(h)
        x_new.append(rms_norm(h, scale_ref[1, layer:layer + 1, :]))
    x = jnp.concatenate(x_new, axis=0)
    ctx = cross_context(x, mask_ref[...], wq_copy, wq_ref, lambda head: k_in(head).wait(), keys, lambda head: v_in(head).wait(), values, q_t, acc_ref, p_ref, ctx_t)
    wo_copy.wait()
    send_projected(ctx, wo_ref, mine_ref.at[0], copies[1])

    for c in dense:
        c.wait()
    width = dg_ref.shape[1]
    step = 512
    rows = ctx.shape[0] // 2
    h_last = []
    for i, h in enumerate(receive_sum(h_new, mine_ref.at[0], other_ref.at[1], copies[1])):
        h_last.append(h)
        x = rms_norm(h, scale_ref[2, layer:layer + 1, :])
        for c in range(0, width, step):
            gate_in = dot(x, dg_ref[:, c:c + step])
            lin_in = dot(x, du_ref[:, c:c + step])
            prod_ref[i * rows:(i + 1) * rows, c:c + step] = (jax.nn.gelu(gate_in) * lin_in).astype(BF16)
        mine_ref[1, i * rows:(i + 1) * rows] = dot(prod_ref[i * rows:(i + 1) * rows], dd_ref[...]).astype(BF16)
        copies[2][i].start()
    for i, h in enumerate(receive_sum(h_last, mine_ref.at[1], other_ref.at[2], copies[2])):
        out_ref[i * rows:(i + 1) * rows] = h.astype(BF16)
    for c in following:
        c.wait()


def middle(layer, part, h, mask, scale, pos, w_query, w_out, keys, values, dense_gate, dense_up, dense_down, following):
    _, heads, slots, head_dim, tokens = keys.shape
    width, model = w_out.shape[1:]
    ff = dense_gate.shape[1]
    vmem = pl.BlockSpec(memory_space=pltpu.VMEM)
    hbm = pl.BlockSpec(memory_space=pltpu.HBM)
    dma = pltpu.SemaphoreType.DMA
    cache = pltpu.VMEM((heads, slots, head_dim, tokens), BF16)
    return pl.pallas_call(
        functools.partial(middle_kernel, layer),
        out_shape=[
            pltpu.VMEM((tokens, model), BF16), pltpu.VMEM(pos.shape, pos.dtype), pltpu.VMEM(scale.shape, F32),
            pltpu.VMEM((3, model, width), BF16), pltpu.VMEM((width, model), BF16), cache, cache,
        ],
        in_specs=[vmem] + [hbm] * 17,
        out_specs=[vmem] * 7,
        scratch_shapes=[
            pltpu.VMEM((tokens, model), BF16),
            pltpu.VMEM(mask.shape, mask.dtype),
            pltpu.VMEM((model, width), BF16),
            pltpu.VMEM((width, model), BF16),
            pltpu.VMEM((heads, slots, head_dim, tokens), BF16),
            pltpu.VMEM((heads, slots, head_dim, tokens), BF16),
            pltpu.VMEM((model, ff), BF16),
            pltpu.VMEM((model, ff), BF16),
            pltpu.VMEM((ff, model), BF16),
            pltpu.VMEM((heads, head_dim, tokens), F32),
            pltpu.VMEM((heads, slots * 8, tokens), F32),
            pltpu.VMEM((heads, slots, tokens), F32),
            pltpu.VMEM((heads, head_dim, tokens), F32),
            pltpu.VMEM((2, tokens, model), BF16),
            pltpu.VMEM((3, tokens, model), BF16),
            pltpu.VMEM((tokens, ff), BF16),
            dma((5,)), dma((heads,)), dma((heads,)), dma((3, 2)), dma((3, 2)), dma((4,)), dma((6,)),
        ],
        compiler_params=pltpu.CompilerParams(vmem_limit_bytes=26 * MIB, collective_id=0, has_side_effects=True),
        name="middle",
    )(part, *map(pinned, (h, mask, scale, pos, w_query, w_out, keys, values, dense_gate, dense_up, dense_down) + following))


def last_kernel(layer, h_ref, part_ref, mask_hbm, idx_hbm, scale_hbm, router_hbm, wq_hbm, wo_hbm, k_hbm, v_hbm, eg_hbm, eu_hbm, ed_hbm,
                out_ref,
                mask_ref, idx_ref, scale_ref, router_ref, wq_ref, wo_ref, eg_ref, eu_ref, ed_ref, q_t, acc_ref, p_ref, ctx_t, mine_ref, other_ref,
                place_ref, send_x, recv_x, product_ref, send_y, recv_y, comb_ref, gate_ref,
                w_sem, k_sem, v_sem, g_sem, d_sem, tp_send, tp_recv, x_send, x_recv, y_send, y_recv, s_sem):
    heads, head_dim, _ = q_t.shape
    slots = p_ref.shape[1]
    tokens, model = h_ref.shape
    experts = router_ref.shape[0]
    local, groups, capacity, _ = recv_x.shape
    rows = groups * capacity
    g_slots, d_slots = eg_ref.shape[0], ed_ref.shape[0]
    tp = lax.axis_index("tp")
    ep = lax.axis_index("ep")
    me = tp * groups + ep

    def peer_ep(offset):
        return lax.rem(ep + offset, groups)

    def peer_tp(offset):
        return lax.rem(tp + offset, 2)

    regions = (eg_ref.at[g_slots - 1], eu_ref.at[g_slots - 1], ed_ref.at[d_slots - 1])
    places = []
    for region in range(3):
        height, wide = regions[region].shape
        places += [(region, w, r) for w in range(wide // tokens) for r in range(height // head_dim)]

    def block(number):
        region, w, r = places[number]
        return regions[region].at[r * head_dim:(r + 1) * head_dim, w * tokens:(w + 1) * tokens]

    def cache_in(source, head, first, sems):
        out, slot = [], 0
        while slot < slots:
            region, w, r = places[first + slot]
            count = 1
            while slot + count < slots and places[first + slot + count][:2] == (region, w):
                count += 1
            dst = regions[region].at[r * head_dim:(r + count) * head_dim, w * tokens:(w + 1) * tokens]
            out.append(pltpu.make_async_copy(source.at[layer, head, slot * head_dim:(slot + count) * head_dim], dst, sems.at[head, len(out)]))
            slot += count
        return out

    def k_in(head):
        return cache_in(k_hbm, head, head * slots, k_sem)

    def v_in(head):
        return cache_in(v_hbm, head, (heads + head) * slots, v_sem)

    def wait_all(copies):
        for c in copies:
            c.wait()

    def gate_up_in(expert):
        slot = lax.rem(expert, g_slots)
        return [pltpu.make_async_copy(s.at[expert], d.at[slot], g_sem.at[slot, i]) for i, (s, d) in enumerate(((eg_hbm, eg_ref), (eu_hbm, eu_ref)))]

    def down_in(expert):
        slot = lax.rem(expert, d_slots)
        return pltpu.make_async_copy(ed_hbm.at[expert], ed_ref.at[slot], d_sem.at[slot])

    small = [pltpu.make_async_copy(s, d, s_sem.at[i]) for i, (s, d) in enumerate(
        ((mask_hbm, mask_ref), (idx_hbm, idx_ref), (scale_hbm, scale_ref), (router_hbm, router_ref)))]
    wq_copy = pltpu.make_async_copy(wq_hbm.at[layer], wq_ref, w_sem.at[0])
    wo_copy = pltpu.make_async_copy(wo_hbm.at[layer], wo_ref, w_sem.at[1])

    others = [(dt, de) for dt in range(2) for de in range(groups) if dt or de]
    barrier = pltpu.get_barrier_semaphore()
    for dt, de in others:
        pl.semaphore_signal(barrier, inc=1, device_id={"tp": peer_tp(dt), "ep": peer_ep(de)}, device_id_type=MESH)
    for c in small:
        c.start()
    wq_copy.start()
    for head in range(heads):
        for c in k_in(head):
            c.start()
    for head in range(heads):
        for c in v_in(head):
            c.start()
    wo_copy.start()
    for expert in range(max(g_slots, d_slots) - 1):
        for c in (gate_up_in(expert) if expert < g_slots - 1 else []) + ([down_in(expert)] if expert < d_slots - 1 else []):
            c.start(priority=1)
    pl.semaphore_wait(barrier, len(others))

    copies = [tp_exchange(part_ref if i == 0 else mine_ref, other_ref.at[i], tp_send.at[i], tp_recv.at[i]) for i in range(2)]
    for c in copies[0]:
        c.start()

    for c in small:
        c.wait()
    idx = idx_ref[...]
    onehot = (lax.broadcasted_iota(jnp.int32, (experts, tokens), 0) == idx).astype(F32)
    earlier = (lax.broadcasted_iota(jnp.int32, (tokens, tokens), 0) < lax.broadcasted_iota(jnp.int32, (tokens, tokens), 1)).astype(F32)
    counts = dot(onehot.astype(BF16), earlier.astype(BF16))
    slot_of = jnp.sum(counts * onehot, axis=0, keepdims=True).astype(jnp.int32)
    row_of = jnp.where(slot_of < capacity, lax.rem(idx, local) * rows + lax.div(idx, local) * capacity + slot_of, -1)
    place_ref[...] = (lax.broadcasted_iota(jnp.int32, (experts * capacity, tokens), 0) == row_of).astype(F32).astype(BF16)

    h_parts = [h.astype(F32) for h in halves(h_ref)]
    h_new, x_new = [], []
    for h in receive_sum(h_parts, part_ref, other_ref.at[0], copies[0]):
        h_new.append(h)
        x_new.append(rms_norm(h, scale_ref[1, layer:layer + 1, :]))
    x = jnp.concatenate(x_new, axis=0)
    ctx = cross_context(
        x, mask_ref[...], wq_copy, wq_ref,
        lambda head: wait_all(k_in(head)), lambda head, slot: block(head * slots + slot)[...],
        lambda head: wait_all(v_in(head)), lambda head, slot: block((heads + head) * slots + slot)[...],
        q_t, acc_ref, p_ref, ctx_t, True)
    for c in gate_up_in(g_slots - 1) + [down_in(d_slots - 1)]:
        c.start(priority=1)
    wo_copy.wait()
    send_projected(ctx, wo_ref, mine_ref, copies[1])
    h_last, x_new = [], []
    for h in receive_sum(h_new, mine_ref, other_ref.at[1], copies[1]):
        h_last.append(h)
        x_new.append(rms_norm(h, scale_ref[2, layer:layer + 1, :]))
    h_float = jnp.concatenate(h_last, axis=0)
    x = jnp.concatenate(x_new, axis=0)

    def x_copy(expert, offset):
        return pltpu.make_async_remote_copy(
            src_ref=send_x.at[expert, peer_ep(offset)], dst_ref=recv_x.at[expert, ep],
            send_sem=x_send.at[expert], recv_sem=x_recv.at[expert],
            device_id={"ep": peer_ep(offset)}, device_id_type=MESH)

    def x_all(expert):
        return pltpu.make_async_remote_copy(
            src_ref=send_x.at[expert, 0:groups - 1], dst_ref=recv_x.at[expert, 0:groups - 1],
            send_sem=x_send.at[expert], recv_sem=x_recv.at[expert],
            device_id={"ep": peer_ep(1)}, device_id_type=MESH)

    def y_copy(expert, number):
        dt, de = others[number]
        return pltpu.make_async_remote_copy(
            src_ref=send_y.at[expert, peer_ep(de)], dst_ref=recv_y.at[expert, me],
            send_sem=y_send.at[expert], recv_sem=y_recv.at[expert],
            device_id={"tp": peer_tp(dt), "ep": peer_ep(de)}, device_id_type=MESH)

    def y_all(expert):
        return pltpu.make_async_remote_copy(
            src_ref=recv_y.at[expert, 0:2 * groups - 1], dst_ref=recv_y.at[expert, 0:2 * groups - 1],
            send_sem=y_send.at[expert], recv_sem=y_recv.at[expert],
            device_id={"ep": peer_ep(1)}, device_id_type=MESH)

    buffers = dot(place_ref[...], x).astype(BF16)
    for expert in range(local):
        for g in range(groups):
            first = expert * rows + g * capacity
            send_x[expert, g] = buffers[first:first + capacity]
        for offset in range(1, groups):
            x_copy(expert, offset).start()
    recv_x[:, ep] = send_x[:, ep]

    router = router_ref[...]
    high = router.astype(BF16)
    rest = router - high.astype(F32)
    mid = rest.astype(BF16)
    low = (rest - mid.astype(F32)).astype(BF16)
    logits = dot_nt(high, x) + (dot_nt(mid, x) + dot_nt(low, x))
    logits_exp = jnp.exp(logits - jnp.max(logits, axis=0, keepdims=True))
    gate = jnp.sum(logits_exp * onehot, axis=0, keepdims=True) / jnp.sum(logits_exp, axis=0, keepdims=True)
    gate_ref[...] = jnp.transpose(jnp.broadcast_to(gate, (tokens, tokens)))

    def gate_up(expert):
        slot = lax.rem(expert, g_slots)
        x_rows = jnp.concatenate([recv_x[expert, g].astype(F32) for g in range(groups)], axis=0).astype(BF16)
        return (jax.nn.gelu(dot(x_rows, eg_ref[slot])) * dot(x_rows, eu_ref[slot])).astype(BF16)

    def send_result(expert, y):
        for g in range(groups):
            send_y[expert, g] = y[g * capacity:(g + 1) * capacity]
        for number in range(len(others)):
            y_copy(expert, number).start()
        recv_y[expert, me] = send_y[expert, ep]

    def wait_gate_up(expert):
        x_all(expert).wait_recv()
        for c in gate_up_in(expert):
            c.wait()

    def collect(expert):
        y_all(expert).wait_recv()
        blocks = [recv_y[expert, g].astype(F32) + recv_y[expert, groups + g].astype(F32) for g in range(groups)]
        comb_ref[pl.ds(pl.multiple_of(expert * rows, rows), rows), :] = jnp.concatenate(blocks, axis=0).astype(BF16)

    wait_gate_up(0)
    product_ref[0] = gate_up(0)
    for c in gate_up_in(g_slots):
        c.start(priority=1)
    lag = 4

    def expert_step(expert, carry):
        wait_gate_up(expert)
        down_in(expert - 1).wait()
        before = product_ref[lax.rem(expert - 1, 2)]
        y = dot(before, ed_ref[lax.rem(expert - 1, d_slots)]).astype(BF16)
        product_ref[lax.rem(expert, 2)] = gate_up(expert)
        send_result(expert - 1, y)

        @pl.when(expert + g_slots < local)
        def _():
            for c in gate_up_in(expert + g_slots):
                c.start(priority=1)

        @pl.when(expert - 1 + d_slots < local)
        def _():
            down_in(expert - 1 + d_slots).start(priority=1)

        @pl.when(expert >= lag)
        def _():
            collect(expert - lag)
        return carry

    lax.fori_loop(1, local, expert_step, 0)
    down_in(local - 1).wait()
    send_result(local - 1, dot(product_ref[(local - 1) % 2], ed_ref[(local - 1) % d_slots]).astype(BF16))
    for expert in range(local - lag, local):
        collect(expert)
    combined = dot_t(place_ref[...], comb_ref[...])
    gate_col = gate_ref[...]
    for c in range(0, model, tokens):
        delta = gate_col * combined[:, c:c + tokens]
        out_ref[:, c:c + tokens] = (h_float[:, c:c + tokens] + delta).astype(BF16)
    for expert in range(local):
        x_all(expert).wait_send()
        y_all(expert).wait_send()


def last(layer, h, part, mask, idx, scale, router, w_query, w_out, keys, values, exp_gate, exp_up, exp_down, groups):
    _, heads, slots, head_dim, tokens = keys.shape
    flat = keys.shape[:2] + (slots * head_dim, tokens)
    width, model = w_out.shape[1:]
    local, _, ff = exp_gate.shape
    experts = router.shape[0]
    capacity = (2 * tokens + experts - 1) // experts
    vmem = pl.BlockSpec(memory_space=pltpu.VMEM)
    hbm = pl.BlockSpec(memory_space=pltpu.HBM)
    dma = pltpu.SemaphoreType.DMA
    on_chip = functools.partial(pltpu.with_memory_space_constraint, memory_space=pltpu.VMEM)
    return pl.pallas_call(
        functools.partial(last_kernel, layer),
        out_shape=pltpu.VMEM((tokens, model), BF16),
        in_specs=[vmem] * 2 + [hbm] * 11,
        out_specs=vmem,
        scratch_shapes=[
            pltpu.VMEM(mask.shape, mask.dtype),
            pltpu.VMEM(idx.shape, idx.dtype),
            pltpu.VMEM(scale.shape, F32),
            pltpu.VMEM(router.shape, F32),
            pltpu.VMEM((model, width), BF16),
            pltpu.VMEM((width, model), BF16),
            pltpu.VMEM((GATE_SLOTS, model, ff), BF16),
            pltpu.VMEM((GATE_SLOTS, model, ff), BF16),
            pltpu.VMEM((DOWN_SLOTS, ff, model), BF16),
            pltpu.VMEM((heads, head_dim, tokens), F32),
            pltpu.VMEM((heads, slots * 8, tokens), F32),
            pltpu.VMEM((heads, slots, tokens), F32),
            pltpu.VMEM((heads, head_dim, tokens), F32),
            pltpu.VMEM((tokens, model), BF16),
            pltpu.VMEM((2, tokens, model), BF16),
            pltpu.VMEM((experts * capacity, tokens), BF16),
            pltpu.VMEM((local, groups, capacity, model), BF16),
            pltpu.VMEM((local, groups, capacity, model), BF16),
            pltpu.VMEM((2, groups * capacity, ff), BF16),
            pltpu.VMEM((local, groups, capacity, model), BF16),
            pltpu.VMEM((local, 2 * groups, capacity, model), BF16),
            pltpu.VMEM((experts * capacity, model), BF16),
            pltpu.VMEM((tokens, tokens), F32),
            dma((2,)), dma((heads, 4)), dma((heads, 4)), dma((GATE_SLOTS, 2)), dma((DOWN_SLOTS,)), dma((2, 2)), dma((2, 2)),
            dma((local,)), dma((local,)), dma((local,)), dma((local,)), dma((4,)),
        ],
        compiler_params=pltpu.CompilerParams(vmem_limit_bytes=LAST_VMEM, collective_id=1, has_side_effects=True),
        name="last",
    )(on_chip(h), on_chip(part), *map(pinned, (mask, idx, scale, router, w_query, w_out, keys.reshape(flat), values.reshape(flat), exp_gate, exp_up, exp_down)))


def decode_body(groups, hidden, write_pos, enc_mask, expert_idx, self_keys, self_values, cross_keys, cross_values, rel_bias, norm_scale, w_query, w_key, w_value, w_out, w_cross_query, w_cross_out, dense_gate, dense_up, dense_down, router, exp_gate, exp_up, exp_down):
    def lanes(cache):
        return jnp.transpose(cache, (0, 2, 3, 4, 1))

    pos = write_pos.reshape(1, -1)
    idx = expert_idx.reshape(1, -1)
    mask = jnp.transpose(enc_mask)
    scale = jnp.transpose(norm_scale, (1, 0, 2))
    keys, values, ckeys, cvalues = map(lanes, (self_keys, self_values, cross_keys, cross_values))
    part, bias, k_out, v_first = self_first(0, hidden, pos, scale, rel_bias, w_query, w_key, w_value, w_out, keys, values)
    following = (w_query, w_key, w_value, w_out, keys, values)
    h, pos, scale_in, w_in, w_o, keys, values = middle(0, part, hidden, mask, scale, pos, w_cross_query, w_cross_out, ckeys, cvalues, dense_gate, dense_up, dense_down, following)
    part, k_out, v_out = self_second(1, h, pos, scale_in, bias, w_in, w_o, keys, values, v_first, k_out)
    h = last(1, h, part, mask, idx, scale, jnp.transpose(router), w_cross_query, w_cross_out, ckeys, cvalues, exp_gate, exp_up, exp_down, groups)
    return h, jnp.transpose(k_out, (0, 4, 1, 2, 3)), jnp.transpose(v_out, (0, 4, 1, 2, 3))


def solution(mesh):
    batch = ('dp', 'ep')
    row_spec = P(batch, None)
    vec_spec = P(batch)
    cache_spec = P(None, batch, 'tp', None, None)
    col_spec = P(None, None, 'tp')
    out_rows = P(None, 'tp', None)
    in_specs = (row_spec, vec_spec, row_spec, vec_spec, cache_spec, cache_spec, cache_spec, cache_spec, P('tp', None), P(), col_spec, col_spec, col_spec, out_rows, col_spec, out_rows, P(None, 'tp'), P(None, 'tp'), P('tp', None), P(), P('ep', None, 'tp'), P('ep', None, 'tp'), P('ep', 'tp', None))
    out_specs = (row_spec, cache_spec, cache_spec)
    body = functools.partial(decode_body, mesh.shape['ep'])
    return jax.shard_map(body, mesh=mesh, in_specs=in_specs, out_specs=out_specs, check_vma=False)
```

```python
import functools

import jax
import jax.numpy as jnp
from jax import lax
from jax.experimental import pallas as pl
from jax.experimental.pallas import tpu as pltpu
from jax.sharding import PartitionSpec as P

EPS = 1e-6
NEG_BIG = -1e9
MESH = pl.DeviceIdType.MESH
BF16 = jnp.bfloat16
F32 = jnp.float32
MIB = 1024 * 1024
GATE_SLOTS = 7
DOWN_SLOTS = 7
KEPT = 1
LAST_VMEM = int(53.5 * MIB)


def rms_norm(h_float, scale):
    inv_rms = lax.rsqrt(jnp.mean(h_float * h_float, axis=-1, keepdims=True) + EPS)
    return (h_float * inv_rms * scale).astype(BF16)


def dot(a, b):
    return jnp.dot(a, b, preferred_element_type=F32)


def dot_t(a, b):
    return lax.dot_general(a, b, (((0,), (0,)), ((), ())), preferred_element_type=F32)


def dot_nt(a, b):
    return lax.dot_general(a, b, (((1,), (1,)), ((), ())), preferred_element_type=F32)


def fold_rows(prod):
    parts = [prod[i * 8:(i + 1) * 8] for i in range(prod.shape[0] // 8)]
    while len(parts) > 1:
        parts = [a + b for a, b in zip(parts[::2], parts[1::2])]
    return parts[0]


def score_head(q_head, keys, head, acc_ref, merge=None):
    for slot in range(acc_ref.shape[1] // 8):
        k_slot = keys(head, slot) if callable(keys) else keys[head, slot]
        if merge is not None:
            pos_b, k_new, merged = merge
            k_slot = jnp.where(pos_b == jnp.asarray(slot, BF16), k_new, k_slot)
            merged[head, slot] = k_slot
        acc_ref[head, slot * 8:(slot + 1) * 8, :] = fold_rows(k_slot.astype(F32) * q_head)


def gather_scores(acc_ref, head, slots):
    total = acc_ref[head, pl.ds(0, slots, stride=8), :]
    for i in range(1, 8):
        total = total + acc_ref[head, pl.ds(i, slots, stride=8), :]
    return total


def softmax_rows(scores):
    top = jnp.max(scores, axis=0, keepdims=True)
    e = jnp.exp(scores - top)
    return (e / jnp.sum(e, axis=0, keepdims=True)).astype(BF16).astype(F32)


def context_head(p_ref, values, head, merge=None):
    total = None
    for slot in range(p_ref.shape[1]):
        v_slot = values(head, slot) if callable(values) else values[head, slot]
        if merge is not None:
            pos_b, v_new, merged = merge
            v_slot = jnp.where(pos_b == jnp.asarray(slot, BF16), v_new, v_slot)
            merged[head, slot] = v_slot
        term = v_slot.astype(F32) * p_ref[head, slot:slot + 1, :]
        total = term if total is None else total + term
    return total


def pinned(x):
    return pltpu.with_memory_space_constraint(x, pltpu.HBM)


def second_kernel(layer, h_ref, pos_ref, scale_ref, bias_ref, w_in, wo_ref, keys_in, values_in, keys_before, values_before,
                  part_ref, ko_hbm, vo_hbm,
                  keys, values, q_t, k_t, v_t, acc_ref, p_ref, ctx_t, ko_sem, vo_sem, before_sem):
    before = [pltpu.make_async_copy(s, d.at[layer - 1], before_sem.at[i])
              for i, (s, d) in enumerate(((keys_before, ko_hbm), (values_before, vo_hbm)))]
    for c in before:
        c.start()
    self_part(layer, h_ref, pos_ref, scale_ref, bias_ref, w_in, [None] * 3, wo_ref, None,
              keys_in, values_in, None, None, keys, values,
              part_ref, ko_hbm, vo_hbm, q_t, k_t, v_t, acc_ref, p_ref, ctx_t, ko_sem, vo_sem)
    for c in before:
        c.wait()


def self_part(layer, h_ref, pos_ref, scale_ref, bias_ref, w_in, w_waits, wo_ref, wo_wait,
              keys_in, values_in, k_wait, v_wait, keys, values,
              part_ref, ko_hbm, vo_hbm, q_t, k_t, v_t, acc_ref, p_ref, ctx_t, ko_sem, vo_sem):
    heads, slots, head_dim, tokens = keys.shape

    def k_out(head):
        return pltpu.make_async_copy(keys.at[head], ko_hbm.at[layer, head], ko_sem.at[head])

    def v_out(head):
        return pltpu.make_async_copy(values.at[head], vo_hbm.at[layer, head], vo_sem.at[head])

    x = rms_norm(h_ref[...].astype(F32), scale_ref[0, layer:layer + 1, :])
    pos = pos_ref[...]
    valid = pos >= lax.broadcasted_iota(jnp.int32, (slots, tokens), 0)
    pos_b = jnp.broadcast_to(pos.astype(F32), (head_dim, tokens)).astype(BF16)

    for i, target in enumerate((q_t, k_t, v_t)):
        if w_waits[i] is not None:
            w_waits[i]()
        proj = dot(x, w_in[i]).astype(BF16).astype(F32)
        target[...] = jnp.transpose(proj).reshape(target.shape).astype(target.dtype)

    def score_step(head, carry):
        if k_wait is not None:
            k_wait(head)
        score_head(q_t[head], keys_in, head, acc_ref, (pos_b, k_t[head], keys))
        if ko_hbm is not None:
            k_out(head).start()
        return carry

    lax.fori_loop(0, heads, score_step, 0)
    for head in range(heads):
        scores = jnp.where(valid, gather_scores(acc_ref, head, slots) + bias_ref[head], NEG_BIG)
        p_ref[head] = softmax_rows(scores)

    def context_step(head, carry):
        if v_wait is not None:
            v_wait(head)
        ctx_t[head] = context_head(p_ref, values_in, head, (pos_b, v_t[head], values))
        if vo_hbm is not None:
            v_out(head).start()
        return carry

    lax.fori_loop(0, heads, context_step, 0)
    ctx = jnp.transpose(ctx_t[...].reshape(heads * head_dim, tokens)).astype(BF16)
    if wo_wait is not None:
        wo_wait()
    part_ref[...] = dot(ctx, wo_ref[...]).astype(BF16)
    if ko_hbm is not None:
        for head in range(heads):
            k_out(head).wait()
            v_out(head).wait()


def attention_scratch(heads, slots, head_dim, tokens):
    return [
        pltpu.VMEM((heads, slots, head_dim, tokens), BF16),
        pltpu.VMEM((heads, slots, head_dim, tokens), BF16),
        pltpu.VMEM((heads, head_dim, tokens), F32),
        pltpu.VMEM((heads, head_dim, tokens), BF16),
        pltpu.VMEM((heads, head_dim, tokens), BF16),
        pltpu.VMEM((heads, slots * 8, tokens), F32),
        pltpu.VMEM((heads, slots, tokens), F32),
        pltpu.VMEM((heads, head_dim, tokens), F32),
    ]


def self_second(layer, h, pos, scale, bias, w_in, w_out, keys_in, values_in, keys_before, values_before):
    heads, slots, head_dim, tokens = keys_in.shape
    vmem = pl.BlockSpec(memory_space=pltpu.VMEM)
    hbm = pl.BlockSpec(memory_space=pltpu.HBM)
    dma = pltpu.SemaphoreType.DMA
    cache = pltpu.HBM((layer + 1,) + keys_in.shape, BF16)
    return pl.pallas_call(
        functools.partial(second_kernel, layer),
        out_shape=[pltpu.VMEM(h.shape, BF16), cache, cache],
        in_specs=[vmem] * 10,
        out_specs=[vmem, hbm, hbm],
        scratch_shapes=attention_scratch(heads, slots, head_dim, tokens) + [dma((heads,)), dma((heads,)), dma((2,))],
        compiler_params=pltpu.CompilerParams(vmem_limit_bytes=11 * MIB),
        name="self_second",
    )(h, pos, scale, bias, w_in, w_out, keys_in, values_in, keys_before, values_before)


def tp_exchange(src, dst, send_sem, recv_sem):
    rows = src.shape[0] // 2
    return [pltpu.make_async_remote_copy(
        src_ref=src.at[i * rows:(i + 1) * rows], dst_ref=dst.at[i * rows:(i + 1) * rows],
        send_sem=send_sem.at[i], recv_sem=recv_sem.at[i],
        device_id={"tp": 1 - lax.axis_index("tp")}, device_id_type=MESH) for i in range(2)]


def halves(ref):
    rows = ref.shape[0] // 2
    return [ref[i * rows:(i + 1) * rows] for i in range(2)]


def send_projected(ctx, wo_ref, mine_ref, copies):
    rows = ctx.shape[0] // 2
    for i, copy in enumerate(copies):
        mine_ref[i * rows:(i + 1) * rows] = dot(ctx[i * rows:(i + 1) * rows], wo_ref[...]).astype(BF16)
        copy.start()


def receive_sum(h_parts, mine_ref, other_ref, copies):
    rows = mine_ref.shape[0] // 2
    for i, copy in enumerate(copies):
        copy.wait()
        part = slice(i * rows, (i + 1) * rows)
        yield add_parts(h_parts[i], mine_ref[part], other_ref[part])


def add_parts(h_float, mine, other):
    delta = (mine.astype(F32) + other.astype(F32)).astype(BF16)
    return (h_float + delta.astype(F32)).astype(BF16).astype(F32)


def cross_context(x, mask, wq_copy, wq_ref, k_wait, keys, v_wait, values, q_t, acc_ref, p_ref, send_head, unrolled=False):
    heads, head_dim, tokens = q_t.shape
    slots = p_ref.shape[1]
    wq_copy.wait()
    proj = dot(x, wq_ref[...]).astype(BF16).astype(F32)
    q_t[...] = jnp.transpose(proj).reshape(heads, head_dim, tokens)

    def score_step(head, carry):
        k_wait(head)
        score_head(q_t[head], keys, head, acc_ref)
        return carry

    def context_step(head, carry):
        v_wait(head)
        send_head(head, context_head(p_ref, values, head))
        return carry

    def for_heads(step):
        if unrolled:
            for head in range(heads):
                step(head, 0)
        else:
            lax.fori_loop(0, heads, step, 0)

    for_heads(score_step)
    valid = mask > 0
    for head in range(heads):
        p_ref[head] = softmax_rows(jnp.where(valid, gather_scores(acc_ref, head, slots), NEG_BIG))
    for_heads(context_step)


def head_copy(ctx_ref, head, send_sem, recv_sem):
    tp = lax.axis_index("tp")
    return pltpu.make_async_remote_copy(
        src_ref=ctx_ref.at[tp, head], dst_ref=ctx_ref.at[tp, head], send_sem=send_sem.at[head], recv_sem=recv_sem.at[head],
        device_id={"tp": 1 - tp}, device_id_type=MESH)


def project_half(ctx_ref, full_ref, half):
    _, heads, head_dim, tokens = ctx_ref.shape
    ctx = jnp.transpose(ctx_ref[half].astype(F32).reshape(heads * head_dim, tokens)).astype(BF16)
    return dot(ctx, full_ref[half].reshape(heads * head_dim, full_ref.shape[-1]))


def add_heads(h_float, mine, ctx_ref, full_ref, send_sem, recv_sem):
    for head in range(ctx_ref.shape[1]):
        head_copy(ctx_ref, head, send_sem, recv_sem).wait()
    delta = (mine + project_half(ctx_ref, full_ref, 1 - lax.axis_index("tp"))).astype(BF16)
    return (h_float + delta.astype(F32)).astype(BF16).astype(F32)


def weight_copy(full_ref, sems):
    tp, ep = lax.axis_index("tp"), lax.axis_index("ep")
    return pltpu.make_async_remote_copy(
        src_ref=full_ref.at[tp, ep], dst_ref=full_ref.at[tp, ep], send_sem=sems.at[0], recv_sem=sems.at[1],
        device_id={"tp": 1 - tp}, device_id_type=MESH)


def weight_forward(full_ref, offset, sems):
    tp, ep = lax.axis_index("tp"), lax.axis_index("ep")
    return pltpu.make_async_remote_copy(
        src_ref=full_ref.at[1 - tp, ep], dst_ref=full_ref.at[1 - tp, ep], send_sem=sems.at[2 * offset], recv_sem=sems.at[2 * offset + 1],
        device_id={"ep": lax.rem(ep + offset, full_ref.shape[1])}, device_id_type=MESH)


def fill_bias(dist, rel_ref, bias_ref):
    heads, slots, tokens = bias_ref.shape
    bias = [jnp.zeros((slots, tokens), F32)] * heads
    for d in range(slots):
        hit = dist == d
        bias = [jnp.where(hit, rel_ref[head, d], b) for head, b in enumerate(bias)]
    for head in range(heads):
        bias_ref[head] = bias[head]


def middle_kernel(layer, h_hbm, mask_hbm, scale_hbm, pos_hbm, rel_hbm, sq_hbm, sk_hbm, sv_hbm, so_hbm, skeys_hbm, svalues_hbm,
                  wq_hbm, wo_hbm, wf_hbm, k_hbm, v_hbm, dg_hbm, du_hbm, dd_hbm, eg_hbm, eu_hbm, ed_hbm,
                  out_ref, pos_ref, scale_ref, bias_ref, nw_ref, nwo_ref, nkeys_ref, nvalues_ref, skeys, svalues, next_full, lg_ref, lu_ref, ld_ref,
                  h_ref, mask_ref, rel_ref, sw_ref, so_ref, wq_ref, wo_ref, keys, values, dg_ref, du_ref, dd_ref,
                  q_t, k_t, v_t, acc_ref, p_ref, ctx_t, part_ref, mine_ref, other_ref, prod_ref,
                  w_sem, k_sem, v_sem, send_sem, recv_sem, s_sem, n_sem, sw_sem, sk_sem, sv_sem, next_sem, l_sem):
    heads, slots, tokens = bias_ref.shape
    small = [pltpu.make_async_copy(s, d, s_sem.at[i]) for i, (s, d) in enumerate(
        ((h_hbm, h_ref), (scale_hbm, scale_ref), (pos_hbm, pos_ref), (rel_hbm, rel_ref), (mask_hbm, mask_ref)))]
    following = [pltpu.make_async_copy(s.at[layer + 1], d, n_sem.at[i]) for i, (s, d) in enumerate(
        ((sq_hbm, nw_ref.at[0]), (sk_hbm, nw_ref.at[1]), (sv_hbm, nw_ref.at[2]),
         (so_hbm, nwo_ref), (skeys_hbm, nkeys_ref), (svalues_hbm, nvalues_ref)))]
    own = [pltpu.make_async_copy(s.at[layer], d, sw_sem.at[i]) for i, (s, d) in enumerate(
        ((sq_hbm, sw_ref.at[0]), (sk_hbm, sw_ref.at[1]), (sv_hbm, sw_ref.at[2]), (so_hbm, so_ref)))]

    def sk_in(head):
        return pltpu.make_async_copy(skeys_hbm.at[layer, head], skeys.at[head], sk_sem.at[head])

    def sv_in(head):
        return pltpu.make_async_copy(svalues_hbm.at[layer, head], svalues.at[head], sv_sem.at[head])

    def k_in(head):
        return pltpu.make_async_copy(k_hbm.at[layer, head], keys.at[head], k_sem.at[head])

    def v_in(head):
        return pltpu.make_async_copy(v_hbm.at[layer, head], values.at[head], v_sem.at[head])

    wq_copy = pltpu.make_async_copy(wq_hbm.at[layer], wq_ref, w_sem.at[0])
    tp, ep = lax.axis_index("tp"), lax.axis_index("ep")
    groups = next_full.shape[1]
    wo_copy = pltpu.make_async_copy(wo_hbm.at[layer], wo_ref, w_sem.at[1])
    next_copy = pltpu.make_async_copy(wf_hbm.at[layer + 1], next_full.at[tp], w_sem.at[5])
    dense = [pltpu.make_async_copy(s, d, w_sem.at[2 + i]) for i, (s, d) in enumerate(((dg_hbm, dg_ref), (du_hbm, du_ref), (dd_hbm, dd_ref)))]

    kept = lg_ref.shape[0]
    first_kept = eg_hbm.shape[0] - kept
    late = [pltpu.make_async_copy(s.at[first_kept + i], d.at[i], l_sem.at[i, j])
            for i in range(kept) for j, (s, d) in enumerate(((eg_hbm, lg_ref), (eu_hbm, lu_ref), (ed_hbm, ld_ref)))]

    for c in small + own[:3]:
        c.start()
    barrier = pltpu.get_barrier_semaphore()
    pl.semaphore_signal(barrier, inc=1, device_id={"tp": 1 - tp}, device_id_type=MESH)
    for offset in range(1, groups):
        pl.semaphore_signal(barrier, inc=1, device_id={"ep": lax.rem(ep + offset, groups)}, device_id_type=MESH)
    next_copy.start()
    for head in range(heads):
        sk_in(head).start()
    for head in range(heads):
        sv_in(head).start()
    own[3].start()
    wq_copy.start(priority=1)
    for head in range(heads):
        k_in(head).start(priority=1)
    for head in range(heads):
        v_in(head).start(priority=1)
    wo_copy.start(priority=1)
    for c in dense + following + late:
        c.start(priority=1)

    small[2].wait()
    small[3].wait()
    fill_bias(pos_ref[...] - lax.broadcasted_iota(jnp.int32, (slots, tokens), 0), rel_ref, bias_ref)
    for i in (0, 1, 4):
        small[i].wait()
    next_copy.wait()
    pl.semaphore_wait(barrier, groups)
    weight_copy(next_full, next_sem).start()
    self_part(layer, h_ref, pos_ref, scale_ref, bias_ref, sw_ref, [c.wait for c in own[:3]], so_ref, own[3].wait,
              skeys, svalues, lambda head: sk_in(head).wait(), lambda head: sv_in(head).wait(), skeys, svalues,
              part_ref, None, None, q_t, k_t, v_t, acc_ref, p_ref, ctx_t, None, None)

    copies = [tp_exchange(part_ref if i == 0 else mine_ref.at[i - 1], other_ref.at[i], send_sem.at[i], recv_sem.at[i]) for i in range(3)]
    for c in copies[0]:
        c.start()
    weight_copy(next_full, next_sem).wait_recv()
    for offset in range(1, groups):
        weight_forward(next_full, offset, next_sem).start()
    h_parts = [h.astype(F32) for h in halves(h_ref)]
    h_new, x_new = [], []
    for h in receive_sum(h_parts, part_ref, other_ref.at[0], copies[0]):
        h_new.append(h)
        x_new.append(rms_norm(h, scale_ref[1, layer:layer + 1, :]))
    x = jnp.concatenate(x_new, axis=0)

    def keep_head(head, ctx):
        ctx_t[head] = ctx

    cross_context(x, mask_ref[...], wq_copy, wq_ref, lambda head: k_in(head).wait(), keys, lambda head: v_in(head).wait(), values, q_t, acc_ref, p_ref, keep_head)
    ctx = jnp.transpose(ctx_t[...].reshape(wo_ref.shape[0], tokens)).astype(BF16)
    wo_copy.wait()
    send_projected(ctx, wo_ref, mine_ref.at[0], copies[1])

    for c in dense:
        c.wait()
    width = dg_ref.shape[1]
    step = 512
    rows = ctx.shape[0] // 2
    h_last = []
    for i, h in enumerate(receive_sum(h_new, mine_ref.at[0], other_ref.at[1], copies[1])):
        h_last.append(h)
        x = rms_norm(h, scale_ref[2, layer:layer + 1, :])
        for c in range(0, width, step):
            gate_in = dot(x, dg_ref[:, c:c + step])
            lin_in = dot(x, du_ref[:, c:c + step])
            prod_ref[i * rows:(i + 1) * rows, c:c + step] = (jax.nn.gelu(gate_in) * lin_in).astype(BF16)
        mine_ref[1, i * rows:(i + 1) * rows] = dot(prod_ref[i * rows:(i + 1) * rows], dd_ref[...]).astype(BF16)
        copies[2][i].start()
    for i, h in enumerate(receive_sum(h_last, mine_ref.at[1], other_ref.at[2], copies[2])):
        out_ref[i * rows:(i + 1) * rows] = h.astype(BF16)
    for c in following + late:
        c.wait()
    weight_copy(next_full, next_sem).wait_send()
    for offset in range(1, groups):
        weight_forward(next_full, offset, next_sem).wait()


def middle(layer, h, mask, scale, pos, rel, w_self, keys_self, values_self, w_query, w_out, w_full, keys, values, dense_gate, dense_up, dense_down, experts):
    _, heads, slots, head_dim, tokens = keys.shape
    width, model = w_self[3].shape[1:]
    full = (2,) + w_full.shape[1:]
    ff = dense_gate.shape[1]
    vmem = pl.BlockSpec(memory_space=pltpu.VMEM)
    hbm = pl.BlockSpec(memory_space=pltpu.HBM)
    dma = pltpu.SemaphoreType.DMA
    cache = pltpu.VMEM((heads, slots, head_dim, tokens), BF16)
    ins = (h, mask, scale, pos, rel) + w_self + (keys_self, values_self, w_query, w_out, w_full, keys, values, dense_gate, dense_up, dense_down) + experts
    outs = [
        pltpu.VMEM((tokens, model), BF16), pltpu.VMEM(pos.shape, pos.dtype), pltpu.VMEM(scale.shape, F32), pltpu.VMEM((heads, slots, tokens), F32),
        pltpu.VMEM((3, model, width), BF16), pltpu.VMEM((width, model), BF16), cache, cache, cache, cache, pltpu.VMEM(full, BF16),
        pltpu.VMEM((KEPT, model, ff), BF16), pltpu.VMEM((KEPT, model, ff), BF16), pltpu.VMEM((KEPT, ff, model), BF16),
    ]
    return pl.pallas_call(
        functools.partial(middle_kernel, layer),
        out_shape=outs,
        in_specs=[hbm] * len(ins),
        out_specs=[vmem] * len(outs),
        scratch_shapes=[
            pltpu.VMEM((tokens, model), BF16),
            pltpu.VMEM(mask.shape, mask.dtype),
            pltpu.SMEM(rel.shape, F32),
            pltpu.VMEM((3, model, width), BF16),
            pltpu.VMEM((width, model), BF16),
            pltpu.VMEM((model, width), BF16),
            pltpu.VMEM((width, model), BF16),
            pltpu.VMEM((heads, slots, head_dim, tokens), BF16),
            pltpu.VMEM((heads, slots, head_dim, tokens), BF16),
            pltpu.VMEM((model, ff), BF16),
            pltpu.VMEM((model, ff), BF16),
            pltpu.VMEM((ff, model), BF16),
        ] + attention_scratch(heads, slots, head_dim, tokens)[2:] + [
            pltpu.VMEM((tokens, model), BF16),
            pltpu.VMEM((2, tokens, model), BF16),
            pltpu.VMEM((3, tokens, model), BF16),
            pltpu.VMEM((tokens, ff), BF16),
            dma((6,)), dma((heads,)), dma((heads,)), dma((3, 2)), dma((3, 2)), dma((5,)), dma((6,)), dma((4,)), dma((heads,)), dma((heads,)), dma((2 * full[1],)), dma((KEPT, 3)),
        ],
        compiler_params=pltpu.CompilerParams(vmem_limit_bytes=22 * MIB, collective_id=0, has_side_effects=True),
        name="middle",
    )(*map(pinned, ins))


def last_kernel(layer, h_ref, part_ref, full_ref, lg_ref, lu_ref, ld_ref, mask_hbm, idx_hbm, scale_hbm, router_hbm, wq_hbm, k_hbm, v_hbm, eg_hbm, eu_hbm, ed_hbm,
                out_ref,
                mask_ref, idx_ref, scale_ref, router_ref, wq_ref, eg_ref, eu_ref, ed_ref, q_t, acc_ref, p_ref, ctx_ref, other_ref,
                place_ref, send_x, recv_x, product_ref, send_y, recv_y, comb_ref, gate_ref,
                w_sem, k_sem, v_sem, g_sem, d_sem, tp_send, tp_recv, x_send, x_recv, y_send, y_recv, s_sem, c_send, c_recv):
    heads, head_dim, _ = q_t.shape
    slots = p_ref.shape[1]
    tokens, model = h_ref.shape
    experts = router_ref.shape[0]
    local, groups, capacity, _ = recv_x.shape
    rows = groups * capacity
    g_slots, d_slots = eg_ref.shape[0], ed_ref.shape[0]
    tp = lax.axis_index("tp")
    ep = lax.axis_index("ep")
    me = tp * groups + ep

    def peer_ep(offset):
        return lax.rem(ep + offset, groups)

    def peer_tp(offset):
        return lax.rem(tp + offset, 2)

    regions = (eg_ref.at[g_slots - 1], eu_ref.at[g_slots - 1], ed_ref.at[d_slots - 1])
    places = []
    for region in range(3):
        height, wide = regions[region].shape
        places += [(region, w, r) for w in range(wide // tokens) for r in range(height // head_dim)]

    def block(number):
        region, w, r = places[number]
        return regions[region].at[r * head_dim:(r + 1) * head_dim, w * tokens:(w + 1) * tokens]

    def cache_in(source, head, first, sems):
        out, slot = [], 0
        while slot < slots:
            region, w, r = places[first + slot]
            count = 1
            while slot + count < slots and places[first + slot + count][:2] == (region, w):
                count += 1
            dst = regions[region].at[r * head_dim:(r + count) * head_dim, w * tokens:(w + 1) * tokens]
            out.append(pltpu.make_async_copy(source.at[layer, head, slot * head_dim:(slot + count) * head_dim], dst, sems.at[head, len(out)]))
            slot += count
        return out

    def k_in(head):
        return cache_in(k_hbm, head, head * slots, k_sem)

    def v_in(head):
        return cache_in(v_hbm, head, (heads + head) * slots, v_sem)

    def wait_all(copies):
        for c in copies:
            c.wait()

    def gate_up_in(expert):
        slot = lax.rem(expert, g_slots)
        return [pltpu.make_async_copy(s.at[expert], d.at[slot], g_sem.at[slot, i]) for i, (s, d) in enumerate(((eg_hbm, eg_ref), (eu_hbm, eu_ref)))]

    def down_in(expert):
        slot = lax.rem(expert, d_slots)
        return pltpu.make_async_copy(ed_hbm.at[expert], ed_ref.at[slot], d_sem.at[slot])

    small = [pltpu.make_async_copy(s, d, s_sem.at[i]) for i, (s, d) in enumerate(
        ((mask_hbm, mask_ref), (idx_hbm, idx_ref), (scale_hbm, scale_ref), (router_hbm, router_ref)))]
    wq_copy = pltpu.make_async_copy(wq_hbm.at[layer], wq_ref, w_sem.at[0])

    others = [(dt, de) for dt in range(2) for de in range(groups) if dt or de]
    barrier = pltpu.get_barrier_semaphore()
    for dt, de in others:
        pl.semaphore_signal(barrier, inc=1, device_id={"tp": peer_tp(dt), "ep": peer_ep(de)}, device_id_type=MESH)
    for c in small:
        c.start()
    wq_copy.start()
    for head in range(heads):
        for c in k_in(head):
            c.start()
    for head in range(heads):
        for c in v_in(head):
            c.start()
    for expert in range(max(g_slots, d_slots) - 1):
        for c in (gate_up_in(expert) if expert < g_slots - 1 else []) + ([down_in(expert)] if expert < d_slots - 1 else []):
            c.start(priority=1)
    pl.semaphore_wait(barrier, len(others))

    copies = tp_exchange(part_ref, other_ref, tp_send, tp_recv)
    for c in copies:
        c.start()

    for c in small:
        c.wait()
    idx = idx_ref[...]
    onehot = (lax.broadcasted_iota(jnp.int32, (experts, tokens), 0) == idx).astype(F32)
    earlier = (lax.broadcasted_iota(jnp.int32, (tokens, tokens), 0) < lax.broadcasted_iota(jnp.int32, (tokens, tokens), 1)).astype(F32)
    counts = dot(onehot.astype(BF16), earlier.astype(BF16))
    slot_of = jnp.sum(counts * onehot, axis=0, keepdims=True).astype(jnp.int32)
    row_of = jnp.where(slot_of < capacity, lax.rem(idx, local) * rows + lax.div(idx, local) * capacity + slot_of, -1)
    place_ref[...] = (lax.broadcasted_iota(jnp.int32, (experts * capacity, tokens), 0) == row_of).astype(F32).astype(BF16)

    h_parts = [h.astype(F32) for h in halves(h_ref)]
    h_new, x_new = [], []
    for h in receive_sum(h_parts, part_ref, other_ref, copies):
        h_new.append(h)
        x_new.append(rms_norm(h, scale_ref[1, layer:layer + 1, :]))
    x = jnp.concatenate(x_new, axis=0)

    def send_head(head, ctx):
        ctx_ref[tp, head] = ctx.astype(BF16)
        head_copy(ctx_ref, head, c_send, c_recv).start()

    cross_context(
        x, mask_ref[...], wq_copy, wq_ref,
        lambda head: wait_all(k_in(head)), lambda head, slot: block(head * slots + slot)[...],
        lambda head: wait_all(v_in(head)), lambda head, slot: block((heads + head) * slots + slot)[...],
        q_t, acc_ref, p_ref, send_head, True)
    for c in gate_up_in(g_slots - 1) + [down_in(d_slots - 1)]:
        c.start(priority=1)
    mine = project_half(ctx_ref, full_ref, tp)
    h_float = add_heads(jnp.concatenate(h_new, axis=0), mine, ctx_ref, full_ref, c_send, c_recv)
    x = rms_norm(h_float, scale_ref[2, layer:layer + 1, :])

    def x_copy(expert, offset):
        return pltpu.make_async_remote_copy(
            src_ref=send_x.at[expert, peer_ep(offset)], dst_ref=recv_x.at[expert, ep],
            send_sem=x_send.at[expert], recv_sem=x_recv.at[expert],
            device_id={"ep": peer_ep(offset)}, device_id_type=MESH)

    def x_all(expert):
        return pltpu.make_async_remote_copy(
            src_ref=send_x.at[expert, 0:groups - 1], dst_ref=recv_x.at[expert, 0:groups - 1],
            send_sem=x_send.at[expert], recv_sem=x_recv.at[expert],
            device_id={"ep": peer_ep(1)}, device_id_type=MESH)

    def y_copy(expert, number):
        dt, de = others[number]
        return pltpu.make_async_remote_copy(
            src_ref=send_y.at[expert, peer_ep(de)], dst_ref=recv_y.at[expert, me],
            send_sem=y_send.at[expert], recv_sem=y_recv.at[expert],
            device_id={"tp": peer_tp(dt), "ep": peer_ep(de)}, device_id_type=MESH)

    def y_all(expert):
        return pltpu.make_async_remote_copy(
            src_ref=recv_y.at[expert, 0:2 * groups - 1], dst_ref=recv_y.at[expert, 0:2 * groups - 1],
            send_sem=y_send.at[expert], recv_sem=y_recv.at[expert],
            device_id={"ep": peer_ep(1)}, device_id_type=MESH)

    buffers = dot(place_ref[...], x).astype(BF16)
    for expert in range(local):
        for g in range(groups):
            first = expert * rows + g * capacity
            send_x[expert, g] = buffers[first:first + capacity]
        for offset in range(1, groups):
            x_copy(expert, offset).start()
    recv_x[:, ep] = send_x[:, ep]

    router = router_ref[...]
    high = router.astype(BF16)
    rest = router - high.astype(F32)
    mid = rest.astype(BF16)
    low = (rest - mid.astype(F32)).astype(BF16)
    logits = dot_nt(high, x) + (dot_nt(mid, x) + dot_nt(low, x))
    logits_exp = jnp.exp(logits - jnp.max(logits, axis=0, keepdims=True))
    gate = jnp.sum(logits_exp * onehot, axis=0, keepdims=True) / jnp.sum(logits_exp, axis=0, keepdims=True)
    gate_ref[...] = jnp.transpose(jnp.broadcast_to(gate, (tokens, tokens)))

    def gate_up(expert, gate_ref, up_ref):
        x_rows = jnp.concatenate([recv_x[expert, g].astype(F32) for g in range(groups)], axis=0).astype(BF16)
        return (jax.nn.gelu(dot(x_rows, gate_ref[...])) * dot(x_rows, up_ref[...])).astype(BF16)

    def send_result(expert, y):
        for g in range(groups):
            send_y[expert, g] = y[g * capacity:(g + 1) * capacity]
        for number in range(len(others)):
            y_copy(expert, number).start()
        recv_y[expert, me] = send_y[expert, ep]

    streamed = local - lg_ref.shape[0]

    def wait_gate_up(expert):
        x_all(expert).wait_recv()
        for c in gate_up_in(expert):
            c.wait()

    def streamed_gate_up(expert):
        slot = lax.rem(expert, g_slots)
        product_ref[lax.rem(expert, 2)] = gate_up(expert, eg_ref.at[slot], eu_ref.at[slot])

    def streamed_down(expert):
        return dot(product_ref[lax.rem(expert, 2)], ed_ref[lax.rem(expert, d_slots)]).astype(BF16)

    def collect(expert):
        y_all(expert).wait_recv()
        blocks = [recv_y[expert, g].astype(F32) + recv_y[expert, groups + g].astype(F32) for g in range(groups)]
        comb_ref[pl.ds(pl.multiple_of(expert * rows, rows), rows), :] = jnp.concatenate(blocks, axis=0).astype(BF16)

    wait_gate_up(0)
    streamed_gate_up(0)
    for c in gate_up_in(g_slots):
        c.start(priority=1)
    lag = 4
    turn = g_slots

    def refill(expert):
        @pl.when(expert + g_slots < streamed)
        def _():
            for c in gate_up_in(expert + g_slots):
                c.start(priority=1)

    def refill_down(expert):
        @pl.when(expert + d_slots < streamed)
        def _():
            down_in(expert + d_slots).start(priority=1)

    def expert_step(expert, carry):
        wait_gate_up(expert)
        down_in(expert - 1).wait()
        y = streamed_down(expert - 1)
        streamed_gate_up(expert)
        send_result(expert - 1, y)
        refill(expert)
        refill_down(expert - 1)

        @pl.when(jnp.logical_and(expert >= lag, expert < turn))
        def _():
            collect(expert - lag)

        @pl.when(expert >= turn + lag)
        def _():
            collect(expert - lag)
        return carry

    lax.fori_loop(1, turn, expert_step, 0)
    down_in(turn - 1).wait()
    y = streamed_down(turn - 1)
    before = turn - 1
    for i in range(local - streamed):
        x_all(streamed + i).wait_recv()
        product_ref[2] = gate_up(streamed + i, lg_ref.at[i], lu_ref.at[i])
        send_result(before, y)
        if i == 0:
            refill_down(turn - 1)
        y = dot(product_ref[2], ld_ref[i]).astype(BF16)
        before = streamed + i
    wait_gate_up(turn)
    streamed_gate_up(turn)
    send_result(before, y)
    refill(turn)
    lax.fori_loop(turn + 1, streamed, expert_step, 0)
    down_in(streamed - 1).wait()
    send_result(streamed - 1, streamed_down(streamed - 1))
    for expert in list(range(turn - lag, turn)) + list(range(streamed, local)) + list(range(streamed - lag, streamed)):
        collect(expert)
    combined = dot_t(place_ref[...], comb_ref[...])
    gate_col = gate_ref[...]
    for c in range(0, model, tokens):
        delta = gate_col * combined[:, c:c + tokens]
        out_ref[:, c:c + tokens] = (h_float[:, c:c + tokens] + delta).astype(BF16)
    for expert in range(local):
        x_all(expert).wait_send()
        y_all(expert).wait_send()


def last(layer, h, part, full, kept, mask, idx, scale, router, w_query, keys, values, exp_gate, exp_up, exp_down, groups):
    _, heads, slots, head_dim, tokens = keys.shape
    flat = keys.shape[:2] + (slots * head_dim, tokens)
    model, width = w_query.shape[1:]
    local, _, ff = exp_gate.shape
    experts = router.shape[0]
    capacity = (2 * tokens + experts - 1) // experts
    vmem = pl.BlockSpec(memory_space=pltpu.VMEM)
    hbm = pl.BlockSpec(memory_space=pltpu.HBM)
    dma = pltpu.SemaphoreType.DMA
    on_chip = functools.partial(pltpu.with_memory_space_constraint, memory_space=pltpu.VMEM)
    return pl.pallas_call(
        functools.partial(last_kernel, layer),
        out_shape=pltpu.VMEM((tokens, model), BF16),
        in_specs=[vmem] * 6 + [hbm] * 10,
        out_specs=vmem,
        scratch_shapes=[
            pltpu.VMEM(mask.shape, mask.dtype),
            pltpu.VMEM(idx.shape, idx.dtype),
            pltpu.VMEM(scale.shape, F32),
            pltpu.VMEM(router.shape, F32),
            pltpu.VMEM((model, width), BF16),
            pltpu.VMEM((GATE_SLOTS, model, ff), BF16),
            pltpu.VMEM((GATE_SLOTS, model, ff), BF16),
            pltpu.VMEM((DOWN_SLOTS, ff, model), BF16),
            pltpu.VMEM((heads, head_dim, tokens), F32),
            pltpu.VMEM((heads, slots * 8, tokens), F32),
            pltpu.VMEM((heads, slots, tokens), F32),
            pltpu.VMEM((2, heads, head_dim, tokens), BF16),
            pltpu.VMEM((tokens, model), BF16),
            pltpu.VMEM((experts * capacity, tokens), BF16),
            pltpu.VMEM((local, groups, capacity, model), BF16),
            pltpu.VMEM((local, groups, capacity, model), BF16),
            pltpu.VMEM((3, groups * capacity, ff), BF16),
            pltpu.VMEM((local, groups, capacity, model), BF16),
            pltpu.VMEM((local, 2 * groups, capacity, model), BF16),
            pltpu.VMEM((experts * capacity, model), BF16),
            pltpu.VMEM((tokens, tokens), F32),
            dma((1,)), dma((heads, 4)), dma((heads, 4)), dma((GATE_SLOTS, 2)), dma((DOWN_SLOTS,)), dma((2,)), dma((2,)),
            dma((local,)), dma((local,)), dma((local,)), dma((local,)), dma((4,)), dma((heads,)), dma((heads,)),
        ],
        compiler_params=pltpu.CompilerParams(vmem_limit_bytes=LAST_VMEM, collective_id=1, has_side_effects=True),
        name="last",
    )(*map(on_chip, (h, part, full, *kept)), *map(pinned, (mask, idx, scale, router, w_query, keys.reshape(flat), values.reshape(flat), exp_gate, exp_up, exp_down)))


def decode_body(groups, hidden, write_pos, enc_mask, expert_idx, self_keys, self_values, cross_keys, cross_values, rel_bias, norm_scale, w_query, w_key, w_value, w_out, w_cross_query, w_cross_out, dense_gate, dense_up, dense_down, router, exp_gate, exp_up, exp_down):
    def lanes(cache):
        return jnp.transpose(cache, (0, 2, 3, 4, 1))

    pos = write_pos.reshape(1, -1)
    idx = expert_idx.reshape(1, -1)
    mask = jnp.transpose(enc_mask)
    scale = jnp.transpose(norm_scale, (1, 0, 2))
    keys, values, ckeys, cvalues = map(lanes, (self_keys, self_values, cross_keys, cross_values))
    w_full = w_cross_out.reshape(w_cross_out.shape[0], groups, -1, w_cross_out.shape[2])
    h, pos, scale_in, bias, w_in, w_o, keys, values, k_first, v_first, full, *kept = middle(
        0, hidden, mask, scale, pos, rel_bias, (w_query, w_key, w_value, w_out), keys, values,
        w_cross_query, w_cross_out, w_full, ckeys, cvalues, dense_gate, dense_up, dense_down, (exp_gate, exp_up, exp_down))
    part, k_out, v_out = self_second(1, h, pos, scale_in, bias, w_in, w_o, keys, values, k_first, v_first)
    h = last(1, h, part, full, kept, mask, idx, scale, jnp.transpose(router), w_cross_query, ckeys, cvalues, exp_gate, exp_up, exp_down, groups)
    return h, jnp.transpose(k_out, (0, 4, 1, 2, 3)), jnp.transpose(v_out, (0, 4, 1, 2, 3))


def solution(mesh):
    batch = ('dp', 'ep')
    row_spec = P(batch, None)
    vec_spec = P(batch)
    cache_spec = P(None, batch, 'tp', None, None)
    col_spec = P(None, None, 'tp')
    out_rows = P(None, 'tp', None)
    in_specs = (row_spec, vec_spec, row_spec, vec_spec, cache_spec, cache_spec, cache_spec, cache_spec, P('tp', None), P(), col_spec, col_spec, col_spec, out_rows, col_spec, out_rows, P(None, 'tp'), P(None, 'tp'), P('tp', None), P(), P('ep', None, 'tp'), P('ep', None, 'tp'), P('ep', 'tp', None))
    out_specs = (row_spec, cache_spec, cache_spec)
    body = functools.partial(decode_body, mesh.shape['ep'])
    return jax.shard_map(body, mesh=mesh, in_specs=in_specs, out_specs=out_specs, check_vma=False)
```

```python
import functools

import jax
import jax.numpy as jnp
from jax import lax
from jax.experimental import pallas as pl
from jax.experimental.pallas import tpu as pltpu
from jax.sharding import PartitionSpec as P

EPS = 1e-6
NEG_BIG = -1e9
MESH = pl.DeviceIdType.MESH
BF16 = jnp.bfloat16
F32 = jnp.float32
MIB = 1024 * 1024
GATE_SLOTS = 7
DOWN_SLOTS = 7
KEPT = 1
LAST_VMEM = int(53.5 * MIB)


def rms_norm(h_float, scale):
    inv_rms = lax.rsqrt(jnp.mean(h_float * h_float, axis=-1, keepdims=True) + EPS)
    return (h_float * inv_rms * scale).astype(BF16)


def dot(a, b):
    return jnp.dot(a, b, preferred_element_type=F32)


def dot_t(a, b):
    return lax.dot_general(a, b, (((0,), (0,)), ((), ())), preferred_element_type=F32)


def dot_nt(a, b):
    return lax.dot_general(a, b, (((1,), (1,)), ((), ())), preferred_element_type=F32)


def fold_rows(prod):
    parts = [prod[i * 8:(i + 1) * 8] for i in range(prod.shape[0] // 8)]
    while len(parts) > 1:
        parts = [a + b for a, b in zip(parts[::2], parts[1::2])]
    return parts[0]


def score_head(q_head, keys, head, acc_ref, merge=None):
    for slot in range(acc_ref.shape[1] // 8):
        k_slot = keys(head, slot) if callable(keys) else keys[head, slot]
        if merge is not None:
            pos_b, k_new, merged = merge
            k_slot = jnp.where(pos_b == jnp.asarray(slot, BF16), k_new, k_slot)
            merged[head, slot] = k_slot
        acc_ref[head, slot * 8:(slot + 1) * 8, :] = fold_rows(k_slot.astype(F32) * q_head)


def gather_scores(acc_ref, head, slots):
    total = acc_ref[head, pl.ds(0, slots, stride=8), :]
    for i in range(1, 8):
        total = total + acc_ref[head, pl.ds(i, slots, stride=8), :]
    return total


def softmax_rows(scores):
    top = jnp.max(scores, axis=0, keepdims=True)
    e = jnp.exp(scores - top)
    return (e / jnp.sum(e, axis=0, keepdims=True)).astype(BF16).astype(F32)


def context_head(p_ref, values, head, merge=None):
    total = None
    for slot in range(p_ref.shape[1]):
        v_slot = values(head, slot) if callable(values) else values[head, slot]
        if merge is not None:
            pos_b, v_new, merged = merge
            v_slot = jnp.where(pos_b == jnp.asarray(slot, BF16), v_new, v_slot)
            merged[head, slot] = v_slot
        term = v_slot.astype(F32) * p_ref[head, slot:slot + 1, :]
        total = term if total is None else total + term
    return total


def pinned(x):
    return pltpu.with_memory_space_constraint(x, pltpu.HBM)


def second_kernel(layer, h_ref, pos_ref, scale_ref, bias_ref, w_in, wo_ref, keys_in, values_in, keys_before, values_before,
                  part_ref, ko_hbm, vo_hbm,
                  keys, values, q_t, k_t, v_t, acc_ref, p_ref, ctx_t, ko_sem, vo_sem, before_sem):
    before = [pltpu.make_async_copy(s, d.at[layer - 1], before_sem.at[i])
              for i, (s, d) in enumerate(((keys_before, ko_hbm), (values_before, vo_hbm)))]
    for c in before:
        c.start()
    self_part(layer, h_ref, pos_ref, scale_ref, bias_ref, w_in, [None] * 3, wo_ref, None,
              keys_in, values_in, None, None, keys, values,
              part_ref, ko_hbm, vo_hbm, q_t, k_t, v_t, acc_ref, p_ref, ctx_t, ko_sem, vo_sem)
    for c in before:
        c.wait()


def self_part(layer, h_ref, pos_ref, scale_ref, bias_ref, w_in, w_waits, wo_ref, wo_wait,
              keys_in, values_in, k_wait, v_wait, keys, values,
              part_ref, ko_hbm, vo_hbm, q_t, k_t, v_t, acc_ref, p_ref, ctx_t, ko_sem, vo_sem):
    heads, slots, head_dim, tokens = keys.shape

    def k_out(head):
        return pltpu.make_async_copy(keys.at[head], ko_hbm.at[layer, head], ko_sem.at[head])

    def v_out(head):
        return pltpu.make_async_copy(values.at[head], vo_hbm.at[layer, head], vo_sem.at[head])

    x = rms_norm(h_ref[...].astype(F32), scale_ref[0, layer:layer + 1, :])
    pos = pos_ref[...]
    valid = pos >= lax.broadcasted_iota(jnp.int32, (slots, tokens), 0)
    pos_b = jnp.broadcast_to(pos.astype(F32), (head_dim, tokens)).astype(BF16)

    for i, target in enumerate((q_t, k_t, v_t)):
        if w_waits[i] is not None:
            w_waits[i]()
        proj = dot(x, w_in[i]).astype(BF16).astype(F32)
        target[...] = jnp.transpose(proj).reshape(target.shape).astype(target.dtype)

    def score_step(head, carry):
        if k_wait is not None:
            k_wait(head)
        score_head(q_t[head], keys_in, head, acc_ref, (pos_b, k_t[head], keys))
        if ko_hbm is not None:
            k_out(head).start()
        return carry

    lax.fori_loop(0, heads, score_step, 0)
    for head in range(heads):
        scores = jnp.where(valid, gather_scores(acc_ref, head, slots) + bias_ref[head], NEG_BIG)
        p_ref[head] = softmax_rows(scores)

    def context_step(head, carry):
        if v_wait is not None:
            v_wait(head)
        ctx_t[head] = context_head(p_ref, values_in, head, (pos_b, v_t[head], values))
        if vo_hbm is not None:
            v_out(head).start()
        return carry

    lax.fori_loop(0, heads, context_step, 0)
    ctx = jnp.transpose(ctx_t[...].reshape(heads * head_dim, tokens)).astype(BF16)
    if wo_wait is not None:
        wo_wait()
    part_ref[...] = dot(ctx, wo_ref[...]).astype(BF16)
    if ko_hbm is not None:
        for head in range(heads):
            k_out(head).wait()
            v_out(head).wait()


def attention_scratch(heads, slots, head_dim, tokens):
    return [
        pltpu.VMEM((heads, slots, head_dim, tokens), BF16),
        pltpu.VMEM((heads, slots, head_dim, tokens), BF16),
        pltpu.VMEM((heads, head_dim, tokens), F32),
        pltpu.VMEM((heads, head_dim, tokens), BF16),
        pltpu.VMEM((heads, head_dim, tokens), BF16),
        pltpu.VMEM((heads, slots * 8, tokens), F32),
        pltpu.VMEM((heads, slots, tokens), F32),
        pltpu.VMEM((heads, head_dim, tokens), F32),
    ]


def self_second(layer, h, pos, scale, bias, w_in, w_out, keys_in, values_in, keys_before, values_before):
    heads, slots, head_dim, tokens = keys_in.shape
    vmem = pl.BlockSpec(memory_space=pltpu.VMEM)
    hbm = pl.BlockSpec(memory_space=pltpu.HBM)
    dma = pltpu.SemaphoreType.DMA
    cache = pltpu.HBM((layer + 1,) + keys_in.shape, BF16)
    return pl.pallas_call(
        functools.partial(second_kernel, layer),
        out_shape=[pltpu.VMEM(h.shape, BF16), cache, cache],
        in_specs=[vmem] * 10,
        out_specs=[vmem, hbm, hbm],
        scratch_shapes=attention_scratch(heads, slots, head_dim, tokens) + [dma((heads,)), dma((heads,)), dma((2,))],
        compiler_params=pltpu.CompilerParams(vmem_limit_bytes=11 * MIB),
        name="self_second",
    )(h, pos, scale, bias, w_in, w_out, keys_in, values_in, keys_before, values_before)


def tp_exchange(src, dst, send_sem, recv_sem):
    rows = src.shape[0] // 2
    return [pltpu.make_async_remote_copy(
        src_ref=src.at[i * rows:(i + 1) * rows], dst_ref=dst.at[i * rows:(i + 1) * rows],
        send_sem=send_sem.at[i], recv_sem=recv_sem.at[i],
        device_id={"tp": 1 - lax.axis_index("tp")}, device_id_type=MESH) for i in range(2)]


def halves(ref):
    rows = ref.shape[0] // 2
    return [ref[i * rows:(i + 1) * rows] for i in range(2)]


def send_projected(ctx, wo_ref, mine_ref, copies):
    rows = ctx.shape[0] // 2
    for i, copy in enumerate(copies):
        mine_ref[i * rows:(i + 1) * rows] = dot(ctx[i * rows:(i + 1) * rows], wo_ref[...]).astype(BF16)
        copy.start()


def receive_sum(h_parts, mine_ref, other_ref, copies):
    rows = mine_ref.shape[0] // 2
    for i, copy in enumerate(copies):
        copy.wait()
        part = slice(i * rows, (i + 1) * rows)
        yield add_parts(h_parts[i], mine_ref[part], other_ref[part])


def add_parts(h_float, mine, other):
    delta = (mine.astype(F32) + other.astype(F32)).astype(BF16)
    return (h_float + delta.astype(F32)).astype(BF16).astype(F32)


def cross_context(x, mask, wq_copy, wq_ref, k_wait, keys, v_wait, values, q_t, acc_ref, p_ref, send_head, unrolled=False):
    heads, head_dim, tokens = q_t.shape
    slots = p_ref.shape[1]
    wq_copy.wait()
    proj = dot(x, wq_ref[...]).astype(BF16).astype(F32)
    q_t[...] = jnp.transpose(proj).reshape(heads, head_dim, tokens)

    def score_step(head, carry):
        k_wait(head)
        score_head(q_t[head], keys, head, acc_ref)
        return carry

    def context_step(head, carry):
        v_wait(head)
        send_head(head, context_head(p_ref, values, head))
        return carry

    def for_heads(step):
        if unrolled:
            for head in range(heads):
                step(head, 0)
        else:
            lax.fori_loop(0, heads, step, 0)

    for_heads(score_step)
    valid = mask > 0
    for head in range(heads):
        p_ref[head] = softmax_rows(jnp.where(valid, gather_scores(acc_ref, head, slots), NEG_BIG))
    for_heads(context_step)


def head_copy(ctx_ref, head, send_sem, recv_sem):
    tp = lax.axis_index("tp")
    return pltpu.make_async_remote_copy(
        src_ref=ctx_ref.at[tp, head], dst_ref=ctx_ref.at[tp, head], send_sem=send_sem.at[head], recv_sem=recv_sem.at[head],
        device_id={"tp": 1 - tp}, device_id_type=MESH)


def project_half(ctx_ref, full_ref, half):
    _, heads, head_dim, tokens = ctx_ref.shape
    ctx = jnp.transpose(ctx_ref[half].astype(F32).reshape(heads * head_dim, tokens)).astype(BF16)
    return dot(ctx, full_ref[half].reshape(heads * head_dim, full_ref.shape[-1]))


def add_heads(h_float, mine, ctx_ref, full_ref, send_sem, recv_sem):
    for head in range(ctx_ref.shape[1]):
        head_copy(ctx_ref, head, send_sem, recv_sem).wait()
    delta = (mine + project_half(ctx_ref, full_ref, 1 - lax.axis_index("tp"))).astype(BF16)
    return (h_float + delta.astype(F32)).astype(BF16).astype(F32)


def weight_copy(full_ref, sems):
    tp, ep = lax.axis_index("tp"), lax.axis_index("ep")
    return pltpu.make_async_remote_copy(
        src_ref=full_ref.at[tp, ep], dst_ref=full_ref.at[tp, ep], send_sem=sems.at[0], recv_sem=sems.at[1],
        device_id={"tp": 1 - tp}, device_id_type=MESH)


def weight_forward(full_ref, offset, sems):
    tp, ep = lax.axis_index("tp"), lax.axis_index("ep")
    return pltpu.make_async_remote_copy(
        src_ref=full_ref.at[1 - tp, ep], dst_ref=full_ref.at[1 - tp, ep], send_sem=sems.at[2 * offset], recv_sem=sems.at[2 * offset + 1],
        device_id={"ep": lax.rem(ep + offset, full_ref.shape[1])}, device_id_type=MESH)


def fill_bias(dist, rel_ref, bias_ref):
    heads, slots, tokens = bias_ref.shape
    bias = [jnp.zeros((slots, tokens), F32)] * heads
    for d in range(slots):
        hit = dist == d
        bias = [jnp.where(hit, rel_ref[head, d], b) for head, b in enumerate(bias)]
    for head in range(heads):
        bias_ref[head] = bias[head]


def middle_kernel(layer, h_hbm, mask_hbm, scale_hbm, pos_hbm, rel_hbm, sq_hbm, sk_hbm, sv_hbm, so_hbm, skeys_hbm, svalues_hbm,
                  wq_hbm, wo_hbm, wf_hbm, k_hbm, v_hbm, dg_hbm, du_hbm, dd_hbm, eg_hbm, eu_hbm, ed_hbm,
                  out_ref, pos_ref, scale_ref, bias_ref, nw_ref, nwo_ref, nkeys_ref, nvalues_ref, skeys, svalues, next_full, lg_ref, lu_ref, ld_ref,
                  h_ref, mask_ref, rel_ref, sw_ref, so_ref, wq_ref, wo_ref, keys, values, dg_ref, du_ref, dd_ref,
                  q_t, k_t, v_t, acc_ref, p_ref, ctx_t, part_ref, mine_ref, other_ref, prod_ref,
                  w_sem, k_sem, v_sem, send_sem, recv_sem, s_sem, n_sem, sw_sem, sk_sem, sv_sem, next_sem, l_sem):
    heads, slots, tokens = bias_ref.shape
    small = [pltpu.make_async_copy(s, d, s_sem.at[i]) for i, (s, d) in enumerate(
        ((h_hbm, h_ref), (scale_hbm, scale_ref), (pos_hbm, pos_ref), (rel_hbm, rel_ref), (mask_hbm, mask_ref)))]
    following = [pltpu.make_async_copy(s.at[layer + 1], d, n_sem.at[i]) for i, (s, d) in enumerate(
        ((sq_hbm, nw_ref.at[0]), (sk_hbm, nw_ref.at[1]), (sv_hbm, nw_ref.at[2]),
         (so_hbm, nwo_ref), (skeys_hbm, nkeys_ref), (svalues_hbm, nvalues_ref)))]
    own = [pltpu.make_async_copy(s.at[layer], d, sw_sem.at[i]) for i, (s, d) in enumerate(
        ((sq_hbm, sw_ref.at[0]), (sk_hbm, sw_ref.at[1]), (sv_hbm, sw_ref.at[2]), (so_hbm, so_ref)))]

    def sk_in(head):
        return pltpu.make_async_copy(skeys_hbm.at[layer, head], skeys.at[head], sk_sem.at[head])

    def sv_in(head):
        return pltpu.make_async_copy(svalues_hbm.at[layer, head], svalues.at[head], sv_sem.at[head])

    def k_in(head):
        return pltpu.make_async_copy(k_hbm.at[layer, head], keys.at[head], k_sem.at[head])

    def v_in(head):
        return pltpu.make_async_copy(v_hbm.at[layer, head], values.at[head], v_sem.at[head])

    wq_copy = pltpu.make_async_copy(wq_hbm.at[layer], wq_ref, w_sem.at[0])
    tp, ep = lax.axis_index("tp"), lax.axis_index("ep")
    groups = next_full.shape[1]
    wo_copy = pltpu.make_async_copy(wo_hbm.at[layer], wo_ref, w_sem.at[1])
    next_copy = pltpu.make_async_copy(wf_hbm.at[layer + 1], next_full.at[tp], w_sem.at[5])
    dense = [pltpu.make_async_copy(s, d, w_sem.at[2 + i]) for i, (s, d) in enumerate(((dg_hbm, dg_ref), (du_hbm, du_ref), (dd_hbm, dd_ref)))]

    kept = lg_ref.shape[0]
    first_kept = eg_hbm.shape[0] - kept
    late = [pltpu.make_async_copy(s.at[first_kept + i], d.at[i], l_sem.at[i, j])
            for i in range(kept) for j, (s, d) in enumerate(((eg_hbm, lg_ref), (eu_hbm, lu_ref), (ed_hbm, ld_ref)))]

    next_copy.start()
    for c in small + own[:3]:
        c.start()
    barrier = pltpu.get_barrier_semaphore()
    pl.semaphore_signal(barrier, inc=1, device_id={"tp": 1 - tp}, device_id_type=MESH)
    for offset in range(1, groups):
        pl.semaphore_signal(barrier, inc=1, device_id={"ep": lax.rem(ep + offset, groups)}, device_id_type=MESH)
    for head in range(heads):
        sk_in(head).start()
    for head in range(heads):
        sv_in(head).start()
    own[3].start()
    wq_copy.start(priority=1)
    for head in range(heads):
        k_in(head).start(priority=1)
    for head in range(heads):
        v_in(head).start(priority=1)
    wo_copy.start(priority=1)
    for c in dense + following + late:
        c.start(priority=1)

    small[2].wait()
    small[3].wait()
    fill_bias(pos_ref[...] - lax.broadcasted_iota(jnp.int32, (slots, tokens), 0), rel_ref, bias_ref)
    for i in (0, 1, 4):
        small[i].wait()
    next_copy.wait()
    pl.semaphore_wait(barrier, groups)
    weight_copy(next_full, next_sem).start()
    self_part(layer, h_ref, pos_ref, scale_ref, bias_ref, sw_ref, [c.wait for c in own[:3]], so_ref, own[3].wait,
              skeys, svalues, lambda head: sk_in(head).wait(), lambda head: sv_in(head).wait(), skeys, svalues,
              part_ref, None, None, q_t, k_t, v_t, acc_ref, p_ref, ctx_t, None, None)

    copies = [tp_exchange(part_ref if i == 0 else mine_ref.at[i - 1], other_ref.at[i], send_sem.at[i], recv_sem.at[i]) for i in range(3)]
    for c in copies[0]:
        c.start()
    weight_copy(next_full, next_sem).wait_recv()
    for offset in range(1, groups):
        weight_forward(next_full, offset, next_sem).start()
    h_parts = [h.astype(F32) for h in halves(h_ref)]
    h_new, x_new = [], []
    for h in receive_sum(h_parts, part_ref, other_ref.at[0], copies[0]):
        h_new.append(h)
        x_new.append(rms_norm(h, scale_ref[1, layer:layer + 1, :]))
    x = jnp.concatenate(x_new, axis=0)

    def keep_head(head, ctx):
        ctx_t[head] = ctx

    cross_context(x, mask_ref[...], wq_copy, wq_ref, lambda head: k_in(head).wait(), keys, lambda head: v_in(head).wait(), values, q_t, acc_ref, p_ref, keep_head)
    ctx = jnp.transpose(ctx_t[...].reshape(wo_ref.shape[0], tokens)).astype(BF16)
    wo_copy.wait()
    send_projected(ctx, wo_ref, mine_ref.at[0], copies[1])

    for c in dense:
        c.wait()
    width = dg_ref.shape[1]
    step = 512
    rows = ctx.shape[0] // 2
    h_last = []
    for i, h in enumerate(receive_sum(h_new, mine_ref.at[0], other_ref.at[1], copies[1])):
        h_last.append(h)
        x = rms_norm(h, scale_ref[2, layer:layer + 1, :])
        for c in range(0, width, step):
            gate_in = dot(x, dg_ref[:, c:c + step])
            lin_in = dot(x, du_ref[:, c:c + step])
            prod_ref[i * rows:(i + 1) * rows, c:c + step] = (jax.nn.gelu(gate_in) * lin_in).astype(BF16)
        mine_ref[1, i * rows:(i + 1) * rows] = dot(prod_ref[i * rows:(i + 1) * rows], dd_ref[...]).astype(BF16)
        copies[2][i].start()
    for i, h in enumerate(receive_sum(h_last, mine_ref.at[1], other_ref.at[2], copies[2])):
        out_ref[i * rows:(i + 1) * rows] = h.astype(BF16)
    for c in following + late:
        c.wait()
    weight_copy(next_full, next_sem).wait_send()
    for offset in range(1, groups):
        weight_forward(next_full, offset, next_sem).wait()


def middle(layer, h, mask, scale, pos, rel, w_self, keys_self, values_self, w_query, w_out, w_full, keys, values, dense_gate, dense_up, dense_down, experts):
    _, heads, slots, head_dim, tokens = keys.shape
    width, model = w_self[3].shape[1:]
    full = (2,) + w_full.shape[1:]
    ff = dense_gate.shape[1]
    vmem = pl.BlockSpec(memory_space=pltpu.VMEM)
    hbm = pl.BlockSpec(memory_space=pltpu.HBM)
    dma = pltpu.SemaphoreType.DMA
    cache = pltpu.VMEM((heads, slots, head_dim, tokens), BF16)
    ins = (h, mask, scale, pos, rel) + w_self + (keys_self, values_self, w_query, w_out, w_full, keys, values, dense_gate, dense_up, dense_down) + experts
    outs = [
        pltpu.VMEM((tokens, model), BF16), pltpu.VMEM(pos.shape, pos.dtype), pltpu.VMEM(scale.shape, F32), pltpu.VMEM((heads, slots, tokens), F32),
        pltpu.VMEM((3, model, width), BF16), pltpu.VMEM((width, model), BF16), cache, cache, cache, cache, pltpu.VMEM(full, BF16),
        pltpu.VMEM((KEPT, model, ff), BF16), pltpu.VMEM((KEPT, model, ff), BF16), pltpu.VMEM((KEPT, ff, model), BF16),
    ]
    return pl.pallas_call(
        functools.partial(middle_kernel, layer),
        out_shape=outs,
        in_specs=[hbm] * len(ins),
        out_specs=[vmem] * len(outs),
        scratch_shapes=[
            pltpu.VMEM((tokens, model), BF16),
            pltpu.VMEM(mask.shape, mask.dtype),
            pltpu.SMEM(rel.shape, F32),
            pltpu.VMEM((3, model, width), BF16),
            pltpu.VMEM((width, model), BF16),
            pltpu.VMEM((model, width), BF16),
            pltpu.VMEM((width, model), BF16),
            pltpu.VMEM((heads, slots, head_dim, tokens), BF16),
            pltpu.VMEM((heads, slots, head_dim, tokens), BF16),
            pltpu.VMEM((model, ff), BF16),
            pltpu.VMEM((model, ff), BF16),
            pltpu.VMEM((ff, model), BF16),
        ] + attention_scratch(heads, slots, head_dim, tokens)[2:] + [
            pltpu.VMEM((tokens, model), BF16),
            pltpu.VMEM((2, tokens, model), BF16),
            pltpu.VMEM((3, tokens, model), BF16),
            pltpu.VMEM((tokens, ff), BF16),
            dma((6,)), dma((heads,)), dma((heads,)), dma((3, 2)), dma((3, 2)), dma((5,)), dma((6,)), dma((4,)), dma((heads,)), dma((heads,)), dma((2 * full[1],)), dma((KEPT, 3)),
        ],
        compiler_params=pltpu.CompilerParams(vmem_limit_bytes=22 * MIB, collective_id=0, has_side_effects=True),
        name="middle",
    )(*map(pinned, ins))


def last_kernel(layer, h_ref, part_ref, full_ref, lg_ref, lu_ref, ld_ref, mask_hbm, idx_hbm, scale_hbm, router_hbm, wq_hbm, k_hbm, v_hbm, eg_hbm, eu_hbm, ed_hbm,
                out_ref,
                mask_ref, idx_ref, scale_ref, router_ref, wq_ref, eg_ref, eu_ref, ed_ref, q_t, acc_ref, p_ref, ctx_ref, other_ref,
                place_ref, send_x, recv_x, product_ref, send_y, recv_y, comb_ref, gate_ref,
                w_sem, k_sem, v_sem, g_sem, d_sem, tp_send, tp_recv, x_send, x_recv, y_send, y_recv, s_sem, c_send, c_recv):
    heads, head_dim, _ = q_t.shape
    slots = p_ref.shape[1]
    tokens, model = h_ref.shape
    experts = router_ref.shape[0]
    local, groups, capacity, _ = recv_x.shape
    rows = groups * capacity
    g_slots, d_slots = eg_ref.shape[0], ed_ref.shape[0]
    tp = lax.axis_index("tp")
    ep = lax.axis_index("ep")
    me = tp * groups + ep

    def peer_ep(offset):
        return lax.rem(ep + offset, groups)

    def peer_tp(offset):
        return lax.rem(tp + offset, 2)

    regions = (eg_ref.at[g_slots - 1], eu_ref.at[g_slots - 1], ed_ref.at[d_slots - 1])
    places = []
    for region in range(3):
        height, wide = regions[region].shape
        places += [(region, w, r) for w in range(wide // tokens) for r in range(height // head_dim)]

    def block(number):
        region, w, r = places[number]
        return regions[region].at[r * head_dim:(r + 1) * head_dim, w * tokens:(w + 1) * tokens]

    def cache_in(source, head, first, sems):
        out, slot = [], 0
        while slot < slots:
            region, w, r = places[first + slot]
            count = 1
            while slot + count < slots and places[first + slot + count][:2] == (region, w):
                count += 1
            dst = regions[region].at[r * head_dim:(r + count) * head_dim, w * tokens:(w + 1) * tokens]
            out.append(pltpu.make_async_copy(source.at[layer, head, slot * head_dim:(slot + count) * head_dim], dst, sems.at[head, len(out)]))
            slot += count
        return out

    def k_in(head):
        return cache_in(k_hbm, head, head * slots, k_sem)

    def v_in(head):
        return cache_in(v_hbm, head, (heads + head) * slots, v_sem)

    def wait_all(copies):
        for c in copies:
            c.wait()

    def gate_up_in(expert):
        slot = lax.rem(expert, g_slots)
        return [pltpu.make_async_copy(s.at[expert], d.at[slot], g_sem.at[slot, i]) for i, (s, d) in enumerate(((eg_hbm, eg_ref), (eu_hbm, eu_ref)))]

    def down_in(expert):
        slot = lax.rem(expert, d_slots)
        return pltpu.make_async_copy(ed_hbm.at[expert], ed_ref.at[slot], d_sem.at[slot])

    small = [pltpu.make_async_copy(s, d, s_sem.at[i]) for i, (s, d) in enumerate(
        ((mask_hbm, mask_ref), (idx_hbm, idx_ref), (scale_hbm, scale_ref), (router_hbm, router_ref)))]
    wq_copy = pltpu.make_async_copy(wq_hbm.at[layer], wq_ref, w_sem.at[0])

    others = [(dt, de) for dt in range(2) for de in range(groups) if dt or de]
    barrier = pltpu.get_barrier_semaphore()
    for dt, de in others:
        pl.semaphore_signal(barrier, inc=1, device_id={"tp": peer_tp(dt), "ep": peer_ep(de)}, device_id_type=MESH)
    for c in small:
        c.start()
    wq_copy.start()
    for head in range(heads):
        for c in k_in(head):
            c.start()
    for head in range(heads):
        for c in v_in(head):
            c.start()
    for expert in range(max(g_slots, d_slots) - 1):
        for c in (gate_up_in(expert) if expert < g_slots - 1 else []) + ([down_in(expert)] if expert < d_slots - 1 else []):
            c.start(priority=1)
    pl.semaphore_wait(barrier, len(others))

    copies = tp_exchange(part_ref, other_ref, tp_send, tp_recv)
    for c in copies:
        c.start()

    for c in small:
        c.wait()
    idx = idx_ref[...]
    onehot = (lax.broadcasted_iota(jnp.int32, (experts, tokens), 0) == idx).astype(F32)
    earlier = (lax.broadcasted_iota(jnp.int32, (tokens, tokens), 0) < lax.broadcasted_iota(jnp.int32, (tokens, tokens), 1)).astype(F32)
    counts = dot(onehot.astype(BF16), earlier.astype(BF16))
    slot_of = jnp.sum(counts * onehot, axis=0, keepdims=True).astype(jnp.int32)
    row_of = jnp.where(slot_of < capacity, lax.rem(idx, local) * rows + lax.div(idx, local) * capacity + slot_of, -1)
    place_ref[...] = (lax.broadcasted_iota(jnp.int32, (experts * capacity, tokens), 0) == row_of).astype(F32).astype(BF16)

    h_parts = [h.astype(F32) for h in halves(h_ref)]
    h_new, x_new = [], []
    for h in receive_sum(h_parts, part_ref, other_ref, copies):
        h_new.append(h)
        x_new.append(rms_norm(h, scale_ref[1, layer:layer + 1, :]))
    x = jnp.concatenate(x_new, axis=0)

    def send_head(head, ctx):
        ctx_ref[tp, head] = ctx.astype(BF16)
        head_copy(ctx_ref, head, c_send, c_recv).start()

    cross_context(
        x, mask_ref[...], wq_copy, wq_ref,
        lambda head: wait_all(k_in(head)), lambda head, slot: block(head * slots + slot)[...],
        lambda head: wait_all(v_in(head)), lambda head, slot: block((heads + head) * slots + slot)[...],
        q_t, acc_ref, p_ref, send_head, True)
    for c in gate_up_in(g_slots - 1) + [down_in(d_slots - 1)]:
        c.start(priority=1)
    mine = project_half(ctx_ref, full_ref, tp)
    h_float = add_heads(jnp.concatenate(h_new, axis=0), mine, ctx_ref, full_ref, c_send, c_recv)
    x = rms_norm(h_float, scale_ref[2, layer:layer + 1, :])

    def x_copy(expert, offset):
        return pltpu.make_async_remote_copy(
            src_ref=send_x.at[expert, peer_ep(offset)], dst_ref=recv_x.at[expert, ep],
            send_sem=x_send.at[expert], recv_sem=x_recv.at[expert],
            device_id={"ep": peer_ep(offset)}, device_id_type=MESH)

    def x_all(expert):
        return pltpu.make_async_remote_copy(
            src_ref=send_x.at[expert, 0:groups - 1], dst_ref=recv_x.at[expert, 0:groups - 1],
            send_sem=x_send.at[expert], recv_sem=x_recv.at[expert],
            device_id={"ep": peer_ep(1)}, device_id_type=MESH)

    def y_copy(expert, number):
        dt, de = others[number]
        return pltpu.make_async_remote_copy(
            src_ref=send_y.at[expert, peer_ep(de)], dst_ref=recv_y.at[expert, me],
            send_sem=y_send.at[expert], recv_sem=y_recv.at[expert],
            device_id={"tp": peer_tp(dt), "ep": peer_ep(de)}, device_id_type=MESH)

    def y_all(expert):
        return pltpu.make_async_remote_copy(
            src_ref=recv_y.at[expert, 0:2 * groups - 1], dst_ref=recv_y.at[expert, 0:2 * groups - 1],
            send_sem=y_send.at[expert], recv_sem=y_recv.at[expert],
            device_id={"ep": peer_ep(1)}, device_id_type=MESH)

    buffers = dot(place_ref[...], x).astype(BF16)
    for expert in range(local):
        for g in range(groups):
            first = expert * rows + g * capacity
            send_x[expert, g] = buffers[first:first + capacity]
        for offset in range(1, groups):
            x_copy(expert, offset).start()
    recv_x[:, ep] = send_x[:, ep]

    router = router_ref[...]
    high = router.astype(BF16)
    rest = router - high.astype(F32)
    mid = rest.astype(BF16)
    low = (rest - mid.astype(F32)).astype(BF16)
    logits = dot_nt(high, x) + (dot_nt(mid, x) + dot_nt(low, x))
    logits_exp = jnp.exp(logits - jnp.max(logits, axis=0, keepdims=True))
    gate = jnp.sum(logits_exp * onehot, axis=0, keepdims=True) / jnp.sum(logits_exp, axis=0, keepdims=True)
    gate_ref[...] = jnp.transpose(jnp.broadcast_to(gate, (tokens, tokens)))

    def gate_up(expert, gate_ref, up_ref):
        x_rows = jnp.concatenate([recv_x[expert, g].astype(F32) for g in range(groups)], axis=0).astype(BF16)
        return (jax.nn.gelu(dot(x_rows, gate_ref[...])) * dot(x_rows, up_ref[...])).astype(BF16)

    def send_result(expert, y):
        for g in range(groups):
            send_y[expert, g] = y[g * capacity:(g + 1) * capacity]
        for number in range(len(others)):
            y_copy(expert, number).start()
        recv_y[expert, me] = send_y[expert, ep]

    streamed = local - lg_ref.shape[0]

    def wait_gate_up(expert):
        x_all(expert).wait_recv()
        for c in gate_up_in(expert):
            c.wait()

    def streamed_gate_up(expert):
        slot = lax.rem(expert, g_slots)
        product_ref[lax.rem(expert, 2)] = gate_up(expert, eg_ref.at[slot], eu_ref.at[slot])

    def streamed_down(expert):
        return dot(product_ref[lax.rem(expert, 2)], ed_ref[lax.rem(expert, d_slots)]).astype(BF16)

    def collect(expert):
        y_all(expert).wait_recv()
        blocks = [recv_y[expert, g].astype(F32) + recv_y[expert, groups + g].astype(F32) for g in range(groups)]
        comb_ref[pl.ds(pl.multiple_of(expert * rows, rows), rows), :] = jnp.concatenate(blocks, axis=0).astype(BF16)

    wait_gate_up(0)
    streamed_gate_up(0)
    for c in gate_up_in(g_slots):
        c.start(priority=1)
    lag = 5
    turn = g_slots

    def refill(expert):
        @pl.when(expert + g_slots < streamed)
        def _():
            for c in gate_up_in(expert + g_slots):
                c.start(priority=1)

    def refill_down(expert):
        @pl.when(expert + d_slots < streamed)
        def _():
            down_in(expert + d_slots).start(priority=1)

    def expert_step(expert, carry):
        wait_gate_up(expert)
        down_in(expert - 1).wait()
        y = streamed_down(expert - 1)
        streamed_gate_up(expert)
        send_result(expert - 1, y)
        refill(expert)
        refill_down(expert - 1)

        @pl.when(jnp.logical_and(expert >= lag, expert < turn))
        def _():
            collect(expert - lag)

        @pl.when(expert >= turn + lag)
        def _():
            collect(expert - lag)
        return carry

    lax.fori_loop(1, turn, expert_step, 0)
    down_in(turn - 1).wait()
    y = streamed_down(turn - 1)
    before = turn - 1
    for i in range(local - streamed):
        x_all(streamed + i).wait_recv()
        product_ref[2] = gate_up(streamed + i, lg_ref.at[i], lu_ref.at[i])
        send_result(before, y)
        if i == 0:
            refill_down(turn - 1)
        y = dot(product_ref[2], ld_ref[i]).astype(BF16)
        before = streamed + i
    wait_gate_up(turn)
    streamed_gate_up(turn)
    send_result(before, y)
    refill(turn)
    lax.fori_loop(turn + 1, streamed, expert_step, 0)
    down_in(streamed - 1).wait()
    send_result(streamed - 1, streamed_down(streamed - 1))
    for expert in list(range(turn - lag, turn)) + list(range(streamed, local)) + list(range(streamed - lag, streamed)):
        collect(expert)
    combined = dot_t(place_ref[...], comb_ref[...])
    gate_col = gate_ref[...]
    for c in range(0, model, tokens):
        delta = gate_col * combined[:, c:c + tokens]
        out_ref[:, c:c + tokens] = (h_float[:, c:c + tokens] + delta).astype(BF16)
    for expert in range(local):
        x_all(expert).wait_send()
        y_all(expert).wait_send()


def last(layer, h, part, full, kept, mask, idx, scale, router, w_query, keys, values, exp_gate, exp_up, exp_down, groups):
    _, heads, slots, head_dim, tokens = keys.shape
    flat = keys.shape[:2] + (slots * head_dim, tokens)
    model, width = w_query.shape[1:]
    local, _, ff = exp_gate.shape
    experts = router.shape[0]
    capacity = (2 * tokens + experts - 1) // experts
    vmem = pl.BlockSpec(memory_space=pltpu.VMEM)
    hbm = pl.BlockSpec(memory_space=pltpu.HBM)
    dma = pltpu.SemaphoreType.DMA
    on_chip = functools.partial(pltpu.with_memory_space_constraint, memory_space=pltpu.VMEM)
    return pl.pallas_call(
        functools.partial(last_kernel, layer),
        out_shape=pltpu.VMEM((tokens, model), BF16),
        in_specs=[vmem] * 6 + [hbm] * 10,
        out_specs=vmem,
        scratch_shapes=[
            pltpu.VMEM(mask.shape, mask.dtype),
            pltpu.VMEM(idx.shape, idx.dtype),
            pltpu.VMEM(scale.shape, F32),
            pltpu.VMEM(router.shape, F32),
            pltpu.VMEM((model, width), BF16),
            pltpu.VMEM((GATE_SLOTS, model, ff), BF16),
            pltpu.VMEM((GATE_SLOTS, model, ff), BF16),
            pltpu.VMEM((DOWN_SLOTS, ff, model), BF16),
            pltpu.VMEM((heads, head_dim, tokens), F32),
            pltpu.VMEM((heads, slots * 8, tokens), F32),
            pltpu.VMEM((heads, slots, tokens), F32),
            pltpu.VMEM((2, heads, head_dim, tokens), BF16),
            pltpu.VMEM((tokens, model), BF16),
            pltpu.VMEM((experts * capacity, tokens), BF16),
            pltpu.VMEM((local, groups, capacity, model), BF16),
            pltpu.VMEM((local, groups, capacity, model), BF16),
            pltpu.VMEM((3, groups * capacity, ff), BF16),
            pltpu.VMEM((local, groups, capacity, model), BF16),
            pltpu.VMEM((local, 2 * groups, capacity, model), BF16),
            pltpu.VMEM((experts * capacity, model), BF16),
            pltpu.VMEM((tokens, tokens), F32),
            dma((1,)), dma((heads, 4)), dma((heads, 4)), dma((GATE_SLOTS, 2)), dma((DOWN_SLOTS,)), dma((2,)), dma((2,)),
            dma((local,)), dma((local,)), dma((local,)), dma((local,)), dma((4,)), dma((heads,)), dma((heads,)),
        ],
        compiler_params=pltpu.CompilerParams(vmem_limit_bytes=LAST_VMEM, collective_id=1, has_side_effects=True),
        name="last",
    )(*map(on_chip, (h, part, full, *kept)), *map(pinned, (mask, idx, scale, router, w_query, keys.reshape(flat), values.reshape(flat), exp_gate, exp_up, exp_down)))


def decode_body(groups, hidden, write_pos, enc_mask, expert_idx, self_keys, self_values, cross_keys, cross_values, rel_bias, norm_scale, w_query, w_key, w_value, w_out, w_cross_query, w_cross_out, dense_gate, dense_up, dense_down, router, exp_gate, exp_up, exp_down):
    def lanes(cache):
        return jnp.transpose(cache, (0, 2, 3, 4, 1))

    pos = write_pos.reshape(1, -1)
    idx = expert_idx.reshape(1, -1)
    mask = jnp.transpose(enc_mask)
    scale = jnp.transpose(norm_scale, (1, 0, 2))
    keys, values, ckeys, cvalues = map(lanes, (self_keys, self_values, cross_keys, cross_values))
    w_full = w_cross_out.reshape(w_cross_out.shape[0], groups, -1, w_cross_out.shape[2])
    h, pos, scale_in, bias, w_in, w_o, keys, values, k_first, v_first, full, *kept = middle(
        0, hidden, mask, scale, pos, rel_bias, (w_query, w_key, w_value, w_out), keys, values,
        w_cross_query, w_cross_out, w_full, ckeys, cvalues, dense_gate, dense_up, dense_down, (exp_gate, exp_up, exp_down))
    part, k_out, v_out = self_second(1, h, pos, scale_in, bias, w_in, w_o, keys, values, k_first, v_first)
    h = last(1, h, part, full, kept, mask, idx, scale, jnp.transpose(router), w_cross_query, ckeys, cvalues, exp_gate, exp_up, exp_down, groups)
    return h, jnp.transpose(k_out, (0, 4, 1, 2, 3)), jnp.transpose(v_out, (0, 4, 1, 2, 3))


def solution(mesh):
    batch = ('dp', 'ep')
    row_spec = P(batch, None)
    vec_spec = P(batch)
    cache_spec = P(None, batch, 'tp', None, None)
    col_spec = P(None, None, 'tp')
    out_rows = P(None, 'tp', None)
    in_specs = (row_spec, vec_spec, row_spec, vec_spec, cache_spec, cache_spec, cache_spec, cache_spec, P('tp', None), P(), col_spec, col_spec, col_spec, out_rows, col_spec, out_rows, P(None, 'tp'), P(None, 'tp'), P('tp', None), P(), P('ep', None, 'tp'), P('ep', None, 'tp'), P('ep', 'tp', None))
    out_specs = (row_spec, cache_spec, cache_spec)
    body = functools.partial(decode_body, mesh.shape['ep'])
    return jax.shard_map(body, mesh=mesh, in_specs=in_specs, out_specs=out_specs, check_vma=False)
```
